32 devices in a mesh: dp: 1 (over z), fsdp: 4 (over y), tp: 8 (over x, core).
Axes of the slice: x: 4, y: 4, z: 1, core: 2. Of those that a mesh axis runs over, the one named last changes fastest.
The devices are a block of a 4x4x8 slice.
Arguments:
- hidden: bfloat16 [16384, 1024], P(('dp', 'fsdp', 'tp'))
- w_head: bfloat16 [1024, 50304], P('fsdp', 'tp')
- labels: int32 [16384], P(('dp', 'fsdp', 'tp'))
Outputs:
- output 1: float32 [1], P('dp')
- output 2: bfloat16 [16384, 1024], P(('dp', 'fsdp', 'tp'))
- output 3: bfloat16 [1024, 50304], P(('dp', 'fsdp'), 'tp')
All inputs are finite; a program needn't handle non-finite values.
Results may differ from the reference program's by a relative error of at most 0.001.
Values are sent between devices in bfloat16 or wider.
A program may use at most 768 MiB of HBM per device.

```python
import jax
import jax.numpy as jnp
from jax import lax

HIDDEN = 1024
VOCAB = 50304
TOKENS = 16384
ROW_BLOCK = 32
COL_ROWS = 256
VOCAB_SPLIT = 16


def setup_inputs(seed: int = 0, part: int = 0) -> dict:
    base_key = jax.random.key(seed)
    key_head, key_data = jax.random.split(base_key)
    part_key = jax.random.fold_in(key_data, part)
    key_hidden, key_labels = jax.random.split(part_key)
    hidden = jax.random.normal(key_hidden, (TOKENS, HIDDEN), jnp.float32)
    w_head = jax.random.normal(key_head, (HIDDEN, VOCAB), jnp.float32) * (2.0 * HIDDEN ** -0.5)
    labels = jax.random.randint(key_labels, (TOKENS,), 0, VOCAB, jnp.int32)
    labels = labels.at[0].set(VOCAB - 1).at[1].set(0)
    return {"hidden": hidden.astype(jnp.bfloat16), "w_head": w_head.astype(jnp.bfloat16), "labels": labels}


def reference(hidden, w_head, labels):
    inv_tokens = 1.0 / TOKENS
    vocab_ids = jnp.arange(VOCAB, dtype=jnp.int32)
    x_blocks = hidden.reshape(TOKENS // ROW_BLOCK, ROW_BLOCK, HIDDEN)
    lab_blocks = labels.reshape(TOKENS // ROW_BLOCK, ROW_BLOCK)

    def row_pass(block):
        x_block, lab_block = block
        logits = jnp.dot(x_block, w_head, preferred_element_type=jnp.float32)
        row_max = jnp.max(logits, axis=1)
        exp_rows = jnp.exp(logits - row_max[:, None])
        row_sum = jnp.sum(exp_rows, axis=1)
        onehot = vocab_ids[None, :] == lab_block[:, None]
        target = jnp.sum(jnp.where(onehot, logits, 0.0), axis=1)
        tok_loss = row_max + jnp.log(row_sum) - target
        prob_rows = exp_rows / row_sum[:, None]
        grad_logits = (jnp.where(onehot, prob_rows - 1.0, prob_rows) * inv_tokens).astype(jnp.bfloat16)
        d_rows = jnp.dot(grad_logits, w_head.T, preferred_element_type=jnp.float32).astype(jnp.bfloat16)
        return tok_loss, row_max, row_sum, d_rows

    tok_loss, row_max, row_sum, d_rows = lax.map(row_pass, (x_blocks, lab_blocks))
    mean_loss = jnp.mean(tok_loss).reshape(1)
    d_hidden = d_rows.reshape(TOKENS, HIDDEN)

    col_width = VOCAB // VOCAB_SPLIT
    row_count = TOKENS // COL_ROWS
    x_cols = hidden.reshape(row_count, COL_ROWS, HIDDEN)
    lab_cols = labels.reshape(row_count, COL_ROWS)
    max_cols = row_max.reshape(row_count, COL_ROWS)
    sum_cols = row_sum.reshape(row_count, COL_ROWS)
    col_ids = jnp.arange(col_width, dtype=jnp.int32)

    def col_pass(col_index):
        col_start = col_index * col_width
        w_cols = lax.dynamic_slice_in_dim(w_head, col_start, col_width, axis=1)

        def row_step(grad_acc, block):
            x_block, lab_block, max_block, sum_block = block
            logits = jnp.dot(x_block, w_cols, preferred_element_type=jnp.float32)
            onehot = (col_ids + col_start)[None, :] == lab_block[:, None]
            prob_rows = jnp.exp(logits - max_block[:, None]) / sum_block[:, None]
            grad_logits = (jnp.where(onehot, prob_rows - 1.0, prob_rows) * inv_tokens).astype(jnp.bfloat16)
            grad_acc = grad_acc + jnp.dot(x_block.T, grad_logits, preferred_element_type=jnp.float32)
            return grad_acc, None

        grad_init = jnp.zeros((HIDDEN, col_width), jnp.float32)
        grad_acc, unused_out = lax.scan(row_step, grad_init, (x_cols, lab_cols, max_cols, sum_cols))
        return grad_acc.astype(jnp.bfloat16)

    d_blocks = lax.map(col_pass, jnp.arange(VOCAB_SPLIT, dtype=jnp.int32))
    d_w_head = jnp.transpose(d_blocks, (1, 0, 2)).reshape(HIDDEN, VOCAB)
    return mean_loss, d_hidden, d_w_head
```

```python
import functools

import jax
import jax.numpy as jnp
from jax import lax
from jax.experimental import pallas as pl
from jax.experimental.pallas import tpu as pltpu
from jax.sharding import PartitionSpec as P

MESH = pl.DeviceIdType.MESH
F32 = jnp.float32
BF16 = jnp.bfloat16
NCH = 5
LOW = -1e30
ANY = pl.BlockSpec(memory_space=pl.ANY)


class Place:
    def __init__(self, nx, ny):
        tp = lax.axis_index("tp")
        self.nx, self.ny = nx, ny
        self.x, self.c, self.y = tp // 2, tp % 2, lax.axis_index("fsdp")
        up, down = (self.y + 1) % ny, (self.y + ny - 1) % ny
        even = (self.y + self.c) % 2 == 0
        self.up, self.down = up, down
        self.p = jnp.where(even, up, down)
        self.a = jnp.where(even, down, up)
        self.far = (self.y + 2) % ny
        self.half = ((self.y - self.c + ny) % ny) // 2

    def dev(self, x=None, y=None, c=None):
        x = self.x if x is None else x
        y = self.y if y is None else y
        c = self.c if c is None else c
        return {"fsdp": y, "tp": x * 2 + c}


def half_of(y, b, ny):
    return ((y - b + ny) % ny) // 2


def remote(src, dst, ssem, rsem, dev):
    return pltpu.make_async_remote_copy(
        src_ref=src, dst_ref=dst, send_sem=ssem, recv_sem=rsem, device_id=dev, device_id_type=MESH
    )


def gather_logits_kernel(
    nx, ny, vocab,
    x_hbm, w_hbm, lab_hbm, xg, wo, z, sta, laba,
    w, xown, ra, rb, xb, zb, bias, m, s, stm,
    xsend, xrecv, ysend, yrecv, wsend, wrecv, dsend, drecv, ssend, srecv, lsend, lrecv, loc, wloc, xsem, zsem,
):
    at = Place(nx, ny)
    x, y, c = at.x, at.y, at.c
    tr = xown.shape[0]
    hk = w_hbm.shape[0]
    sb = w.shape[2] // 2
    slot = NCH * sb
    left, right = (x + nx - 1) % nx, (x + 1) % nx
    far_x = (x + 2) % nx
    top, bot = pl.ds(0, tr // 2), pl.ds(tr // 2, tr // 2)

    barrier = pltpu.get_barrier_semaphore()
    for k in range(1, nx):
        pl.semaphore_signal(barrier, inc=1, device_id=at.dev(x=(x + k) % nx), device_id_type=MESH)
    for k in range(nx):
        pl.semaphore_signal(barrier, inc=1, device_id=at.dev(x=(x + k) % nx, y=at.far), device_id_type=MESH)
    pl.semaphore_signal(barrier, inc=1, device_id=at.dev(y=at.up), device_id_type=MESH)
    pl.semaphore_signal(barrier, inc=1, device_id=at.dev(y=at.down), device_id_type=MESH)
    pl.semaphore_signal(barrier, inc=1, device_id=at.dev(c=1 - c), device_id_type=MESH)
    load_x = pltpu.make_async_copy(x_hbm, xown, loc.at[0])
    load_x.start()
    pl.semaphore_wait(barrier, 2 * nx + 2)
    load_x.wait()

    def x_send(r, to_right):
        i = 0 if to_right else 1
        src = xown if r == 0 else xg.at[1, x]
        return remote(src, xg.at[r, x], xsend.at[r, i], xrecv.at[r, i], at.dev(x=right if to_right else left))

    def x_relay(r, to_right):
        if to_right:
            part = xg.at[r, left, top]
            return remote(part, part, xsend.at[r, 2], xrecv.at[r, 2], at.dev(x=right))
        part = xg.at[r, right, bot]
        return remote(part, part, xsend.at[r, 3], xrecv.at[r, 3], at.dev(x=left))

    y_up = remote(xown.at[top], ra, ysend.at[0], yrecv.at[0], at.dev(y=at.up))
    y_down = remote(xown.at[bot], rb, ysend.at[1], yrecv.at[1], at.dev(y=at.down))
    y_up2 = remote(ra, xg.at[1, x, top], ysend.at[2], yrecv.at[2], at.dev(y=at.up))
    y_down2 = remote(rb, xg.at[1, x, bot], ysend.at[3], yrecv.at[3], at.dev(y=at.down))
    keep_x = pltpu.make_async_copy(xown, xg.at[0, x], loc.at[1])

    def w_src(f, q):
        return w_hbm.at[:, pl.ds(pl.multiple_of(f * slot + q * sb, 128), sb)]

    def w_dst(k, q):
        return w.at[q, pl.ds(pl.multiple_of(k * hk, 16), hk), pl.ds(pl.multiple_of(c * sb, 128), sb)]

    def w_own(q):
        return remote(w_src(at.half, q), w_dst(y, q), wsend.at[0, q], wrecv.at[0, q], at.dev(y=at.p))

    def w_other(q):
        return remote(w_src(1 - at.half, q), w_dst(y, q), wsend.at[1, q], wrecv.at[1, q], at.dev(y=at.a))

    def w_fwd(q):
        return remote(w_dst(at.a, q), w_dst(at.a, q), wsend.at[2, q], wrecv.at[2, q], at.dev(y=at.p))

    def w_core(q):
        part = w.at[q, :, pl.ds(pl.multiple_of(c * sb, 128), sb)]
        return remote(part, part, dsend.at[q], drecv.at[q], at.dev(c=1 - c))

    def w_local(q):
        return pltpu.make_async_copy(w_src(at.half, q), w_dst(y, q), wloc.at[q])

    y_up.start()
    y_down.start()
    x_send(0, True).start()
    x_send(0, False).start()
    w_own(0).start()
    w_other(0).start()
    keep_x.start()
    for q in range(NCH):
        w_local(q).start()

    peers = [(0, k) for k in range(1, nx)] + [(1, k) for k in range(nx)]

    def lab_copy(i):
        sy, k = peers[i]
        return remote(
            lab_hbm, laba.at[sy, x], lsend.at[i], lrecv.at[sy, x],
            at.dev(x=(x + k) % nx, y=at.far if sy else y),
        )

    for i in range(len(peers)):
        lab_copy(i).start()
    lab_own = pltpu.make_async_copy(lab_hbm, laba.at[0, x], loc.at[2])
    lab_own.start()

    col = lax.broadcasted_iota(jnp.int32, bias.shape, 1)
    row = lax.broadcasted_iota(jnp.int32, bias.shape, 0)
    b = col // sb
    pos = row * sb + col - b * sb
    half_b = jnp.where(b == 0, half_of(y, 0, ny), half_of(y, 1, ny))
    bias[...] = jnp.where((half_b == 1) & (pos >= vocab - slot), LOW, 0.0)
    m[...] = jnp.full_like(m, -3e38)
    s[...] = jnp.zeros_like(s)

    y_up.wait_recv()
    y_up2.start()
    y_down.wait_recv()
    y_down2.start()
    for q in range(1, NCH):
        w_own(q).start()
        w_other(q).start()
    w_other(0).wait_recv()
    w_fwd(0).start()
    x_send(0, True).wait_recv()
    x_relay(0, True).start()
    x_send(0, False).wait_recv()
    x_relay(0, False).start()
    y_up2.wait_recv()
    y_down2.wait_recv()
    x_send(1, True).start()
    x_send(1, False).start()
    keep_x.wait()
    x_relay(0, True).wait_recv()
    x_relay(0, False).wait_recv()

    n_steps = 2 * nx * NCH

    def place_of(i):
        g = i // nx
        r = g // NCH
        k = i - g * nx
        return r, g - r * NCH, k

    def xcp(i, u):
        r, j, k = place_of(i)
        return pltpu.make_async_copy(xg.at[r, k], xb.at[u], xsem.at[u])

    def zcp(i, u):
        r, j, k = place_of(i)
        return pltpu.make_async_copy(zb.at[u], z.at[j, r, k], zsem.at[u])

    def step(i, u):
        r, j, k = place_of(i)
        run = r * nx + k
        c0 = 0
        for width in (sb * 4 // 5, 2 * sb - sb * 4 // 5) if sb % 640 == 0 else (2 * sb,):
            cols = slice(c0, c0 + width)
            zz = jnp.dot(xb[u], w[j, :, cols], preferred_element_type=F32) + bias[pl.ds(j, 1), cols]
            zb[u, :, cols] = zz
            blk = min(64, tr)
            for o in range(0, tr, blk):
                rows = slice(o, o + blk)
                m_old = m[run, rows, :]
                parts = [zz[rows, 128 * e : 128 * e + 128] for e in range(width // 128)]
                mx = m_old
                for part in parts:
                    mx = jnp.maximum(mx, part)
                acc = s[run, rows, :] * jnp.exp(m_old - mx)
                for part in parts:
                    acc = acc + jnp.exp(part - mx)
                m[run, rows, :] = mx
                s[run, rows, :] = acc
            c0 += width

    def stat_copy(r, i):
        sy, k = peers[i]
        rr = 1 - r if sy else r
        return remote(
            stm.at[r], sta.at[sy, x, rr], ssend.at[r, i], srecv.at[sy, x, rr],
            at.dev(x=(x + k) % nx, y=at.far if sy else y),
        )

    def stat_own(r):
        return pltpu.make_async_copy(stm.at[r], sta.at[0, x, r], loc.at[3 + r])

    def finish_stats(r):
        def one(d, _):
            run = r * nx + d
            mm = m[run]
            top_m = jnp.max(mm, axis=1, keepdims=True)
            tot = jnp.sum(s[run] * jnp.exp(mm - top_m), axis=1, keepdims=True)
            lane = lax.broadcasted_iota(jnp.int32, mm.shape, 1)
            blk = jnp.where(lane == 0, top_m, jnp.where(lane == 1, tot, 0.0))
            stm[r, d] = blk.T[0:8, :]
            return 0

        lax.fori_loop(0, nx, one, 0)
        for i in range(len(peers)):
            stat_copy(r, i).start()
        stat_own(r).start()

    def body(t, _):
        @pl.when((t < 2 * NCH) & (t % 2 == 0))
        def _():
            j = t // 2
            w_local(j).wait()
            w_own(j).wait_recv()
            w_fwd(j).wait_recv()
            w_core(j).start()

            @pl.when(j + 1 < NCH)
            def _():
                w_other(j + 1).wait_recv()
                w_fwd(j + 1).start()

            w_core(j).wait_recv()

        @pl.when(t == 6)
        def _():
            x_send(1, True).wait_recv()
            x_relay(1, True).start()
            x_send(1, False).wait_recv()
            x_relay(1, False).start()

        @pl.when(t == 2 * NCH - 1)
        def _():
            pltpu.make_async_copy(w, wo, loc.at[5]).start()
            x_relay(1, True).wait_recv()
            x_relay(1, False).wait_recv()

        @pl.when(t == 2 * NCH)
        def _():
            finish_stats(0)

        for u in range(2):
            xcp(2 * t + u, u).wait()

        @pl.when(t > 0)
        def _():
            for u in range(2):
                zcp(2 * t - 2 + u, u).wait()

        for u in range(2):
            step(2 * t + u, u)
        for u in range(2):
            zcp(2 * t + u, u).start()

        @pl.when(2 * t + 2 < n_steps)
        def _():
            for u in range(2):
                xcp(2 * t + 2 + u, u).start()

        return 0

    for u in range(2):
        xcp(u, u).start()
    lax.fori_loop(0, n_steps // 2, body, 0)
    finish_stats(1)
    for u in range(2):
        zcp(n_steps - 2 + u, u).wait()
    pltpu.make_async_copy(w, wo, loc.at[5]).wait()
    lab_own.wait()
    stat_own(0).wait()
    stat_own(1).wait()
    for r in range(2):
        for right_way in (True, False):
            x_send(r, right_way).wait_send()
            x_relay(r, right_way).wait_send()
    for cp in (y_up, y_down, y_up2, y_down2):
        cp.wait_send()
    for q in range(NCH):
        w_own(q).wait_send()
        w_other(q).wait_send()
        w_fwd(q).wait_send()
        w_core(q).wait_send()
    for i in range(len(peers)):
        lab_copy(i).wait_send()
        stat_copy(0, i).wait_send()
        stat_copy(1, i).wait_send()
    for sy in range(2):
        for k in range(nx):
            def arrived():
                remote(lab_hbm, laba.at[sy, k], lsend.at[0], lrecv.at[sy, k], at.dev(c=1 - c)).wait_recv()
                for rr in range(2):
                    remote(stm.at[rr], sta.at[sy, k, rr], ssend.at[0, 0], srecv.at[sy, k, rr], at.dev(c=1 - c)).wait_recv()

            if sy == 0:
                pl.when(k != x)(arrived)
            else:
                arrived()


def gather_logits(nx, ny, vocab, x, w, lab):
    tr, h = x.shape
    hk, vp = w.shape
    ch = vp // NCH
    shape = jax.ShapeDtypeStruct
    dma = pltpu.SemaphoreType.DMA
    vm = pltpu.VMEM
    flops = 2 * 2 * nx * tr * h * vp
    return pl.pallas_call(
        functools.partial(gather_logits_kernel, nx, ny, vocab),
        out_shape=(
            shape((2, nx, tr, h), BF16),
            shape((NCH, h, ch), BF16),
            shape((NCH, 2, nx, tr, ch), F32),
            shape((2, nx, 2, nx, 8, tr), F32),
            shape((2, nx) + lab.shape, jnp.int32),
        ),
        in_specs=[ANY] * 3,
        out_specs=(ANY,) * 5,
        scratch_shapes=[
            vm((NCH, h, ch), BF16), vm((tr, h), BF16), vm((tr // 2, h), BF16), vm((tr // 2, h), BF16),
            vm((2, tr, h), BF16), vm((2, tr, ch), F32), vm((8, ch), F32),
            vm((2 * nx, tr, 128), F32), vm((2 * nx, tr, 128), F32), vm((2, nx, 8, tr), F32),
            dma((2, 4)), dma((2, 4)), dma((4,)), dma((4,)), dma((3, NCH)), dma((3, NCH)), dma((NCH,)), dma((NCH,)),
            dma((2, 2 * nx - 1)), dma((2, nx, 2)), dma((2 * nx - 1,)), dma((2, nx)),
            dma((6,)), dma((NCH,)), dma((2,)), dma((2,)),
        ],
        compiler_params=pltpu.CompilerParams(
            collective_id=0, has_side_effects=True, vmem_limit_bytes=60 * 2**20
        ),
        cost_estimate=pl.CostEstimate(flops=flops, bytes_accessed=4 * 2 * nx * tr * vp, transcendentals=0),
        name="gather_logits",
    )(x, w, lab)


def grads_kernel(nx, inv, z, w_hbm, xg, st8, dxp, dwp, loss, w, xt, zb, gb, acc, dx, st, lacc, zsem, sem, osem):
    tr, h = xg.shape[2], xg.shape[3]
    ch = zb.shape[2]
    pltpu.make_async_copy(w_hbm, w, sem.at[0]).start()

    def prep(run, _):
        cp = pltpu.make_async_copy(xg.at[run // nx, run % nx], gb.at[:, pl.ds(0, h)], sem.at[1])
        cp.start()
        one = st8[run // nx, run % nx]
        st[run] = jnp.concatenate([one] * 16, axis=0).T
        cp.wait()
        xt[run] = gb[:, 0:h].T
        return 0

    lax.fori_loop(0, 2 * nx, prep, 0)
    lacc[...] = jnp.zeros_like(lacc)
    pltpu.make_async_copy(w_hbm, w, sem.at[0]).wait()
    n_each = 2 * nx * NCH

    def place_of(i):
        first = i < n_each
        k = jnp.where(first, i, i - n_each)
        j = jnp.where(first, k % NCH, k // (2 * nx))
        run = jnp.where(first, k // NCH, k % (2 * nx))
        return j, run

    def zcp(i, u):
        j, run = place_of(i)
        return pltpu.make_async_copy(z.at[j, run // nx, run % nx], zb.at[u], zsem.at[u])

    def make_g(i, u, want_loss):
        j, run = place_of(i)
        blk = min(64, tr)
        for o in range(0, tr, blk):
            rows = slice(o, o + blk)
            t = st[run, rows, :]
            top = jnp.broadcast_to(t[:, 0:1], (blk, 128))
            scale = jnp.broadcast_to(t[:, 1:2], (blk, 128))
            lab = jnp.broadcast_to(t[:, 2:3], (blk, 128)).astype(jnp.int32) - j * ch
            lane = lax.broadcasted_iota(jnp.int32, (blk, 128), 1)
            add = jnp.zeros((blk, 128), F32)
            for e in range(ch // 128):
                cols = slice(128 * e, 128 * e + 128)
                d = zb[u, rows, cols] - top
                g = jnp.exp(d) * scale
                hit = lab - 128 * e == lane
                if want_loss:
                    add = add + jnp.where(hit, d, 0.0)
                gb[rows, cols] = jnp.where(hit, g - inv, g).astype(BF16)
            if want_loss:
                lacc[rows, :] += add

    def dx_body(t, _):
        for u in range(2):
            i = 2 * t + u
            zcp(i, u).wait()
            zcp(i + 1, 1 - u).start()
            j, run = place_of(i)
            make_g(i, u, True)
            part = lax.dot_general(gb[...], w[j], (((1,), (1,)), ((), ())), preferred_element_type=F32)

            @pl.when(j == 0)
            def _():
                dx[...] = part

            @pl.when(j > 0)
            def _():
                dx[...] += part

            @pl.when(j == NCH - 1)
            def _():
                cp = pltpu.make_async_copy(dx, dxp.at[run // nx, run % nx], osem.at[0])
                cp.start()
                cp.wait()

        return 0

    def dw_body(t, _):
        for u in range(2):
            i = n_each + 2 * t + u
            zcp(i, u).wait()

            @pl.when(i + 1 < 2 * n_each)
            def _():
                zcp(i + 1, 1 - u).start()

            j, run = place_of(i)
            make_g(i, u, False)
            part = jnp.dot(xt[run], gb[...], preferred_element_type=F32)

            @pl.when(run == 0)
            def _():
                acc[...] = part

            @pl.when(run > 0)
            def _():
                acc[...] += part

            @pl.when(run == 2 * nx - 1)
            def _():
                cp = pltpu.make_async_copy(acc, dwp.at[j], osem.at[0])
                cp.start()
                cp.wait()

        return 0

    zcp(0, 0).start()
    lax.fori_loop(0, n_each // 2, dx_body, 0)
    lax.fori_loop(0, n_each // 2, dw_body, 0)
    loss[...] = jnp.sum(lacc[...].reshape(tr // 8, 8, 128), axis=0)


def grads(nx, inv, z, w, xg, st8):
    tr, h = xg.shape[2:]
    ch = w.shape[2]
    shape = jax.ShapeDtypeStruct
    dma = pltpu.SemaphoreType.DMA
    vm = pltpu.VMEM
    vspec = pl.BlockSpec(memory_space=pltpu.VMEM)
    return pl.pallas_call(
        functools.partial(grads_kernel, nx, inv),
        out_shape=(shape((2, nx, tr, h), F32), shape((NCH, h, ch), F32), shape((8, 128), F32)),
        in_specs=[ANY, ANY, ANY, vspec],
        out_specs=(ANY, ANY, vspec),
        scratch_shapes=[
            vm((NCH, h, ch), BF16), vm((2 * nx, h, tr), BF16), vm((2, tr, ch), F32), vm((tr, ch), BF16),
            vm((h, ch), F32), vm((tr, h), F32), vm((2 * nx, tr, 128), F32), vm((tr, 128), F32),
            dma((2,)), dma((2,)), dma((1,)),
        ],
        compiler_params=pltpu.CompilerParams(vmem_limit_bytes=63 * 2**20),
        name="grads",
    )(z, w, xg, st8)


def solution(mesh):
    ny = mesh.shape["fsdp"]
    tp_size = mesh.shape["tp"]
    nx = tp_size // 2
    token_spec = P(("dp", "fsdp", "tp"), None)
    label_spec = P(("dp", "fsdp", "tp"))

    def local_step(hidden, w_head, labels):
        tr, h = hidden.shape
        hk, vocab = w_head.shape
        inv = 1.0 / (tr * tp_size * ny)
        vp = -(-vocab // (256 * NCH)) * (256 * NCH)
        ch = vp // NCH
        sb = ch // 2
        slot = NCH * sb
        tp = lax.axis_index("tp")
        x, c, y = tp // 2, tp % 2, lax.axis_index("fsdp")
        w_pad = jnp.pad(w_head, ((0, 0), (0, vp - vocab)))
        lab8 = jnp.pad(labels.reshape(-1, 128), ((0, 8 - tr // 128), (0, 0)))
        xg, wg, z, sta, laba = gather_logits(nx, ny, vocab, hidden, w_pad, lab8)

        ms = sta[..., 0, :].reshape(2 * nx, 2, nx, tr)
        ss = sta[..., 1, :].reshape(2 * nx, 2, nx, tr)
        top = jnp.max(ms, axis=0)
        tot = jnp.sum(ss * jnp.exp(ms - top), axis=0)
        lab = laba[:, :, 0 : tr // 128, :].reshape(2, nx, tr)
        shard, off = lab // vocab, lab % vocab
        b, f = shard % 2, off // slot
        pos = off - f * slot
        mine = (shard // 2 == x) & (half_of(y, b, ny) == f)
        col = jnp.where(mine, (pos // sb) * ch + b * sb + pos % sb, -1)
        rows = [top, inv / tot, col.astype(F32)]
        st8 = jnp.stack(rows + [jnp.zeros_like(top)] * 5, axis=2)
        dxp, dwp, lpart = grads(nx, inv, z, wg, xg, st8)

        log_own = jnp.sum(jnp.log(lax.dynamic_index_in_dim(tot[0], x, keepdims=False)))
        mean_loss = lax.psum(log_own - jnp.sum(lpart), ("fsdp", "tp")) * inv

        groups = [[2 * k + e for k in range(nx)] for e in range(2)]
        own = lax.psum_scatter(dxp[0], "tp", scatter_dimension=0, tiled=False, axis_index_groups=groups)
        oth = lax.psum_scatter(dxp[1], "tp", scatter_dimension=0, tiled=False, axis_index_groups=groups)
        oth = lax.ppermute(oth, "fsdp", [(k, (k + 2) % ny) for k in range(ny)])
        d_hidden = (own + oth).astype(BF16)

        dw = jnp.transpose(dwp.reshape(NCH, h, 2, sb), (2, 1, 0, 3)).reshape(2, h, slot)
        dw = dw + lax.ppermute(dw, "tp", [(k, k ^ 1) for k in range(tp_size)])
        mesh_axes = ("fsdp", "tp")

        def par(yy, bb):
            return (yy + 1) % ny if (yy + bb) % 2 == 0 else (yy - 1) % ny

        def adj(yy, bb):
            return (yy - 1) % ny if (yy + bb) % 2 == 0 else (yy + 1) % ny

        outs = []
        for bb in range(2):
            perm = [(yy * tp_size + t, par(yy, bb) * tp_size + t) for yy in range(ny) for t in range(tp_size)]
            outs.append(dw[bb] + lax.ppermute(dw[bb], mesh_axes, perm))
        mine_dw = jnp.where(c == 0, outs[0], outs[1])
        adj_perm = [
            (yy * tp_size + t, adj(yy, t % 2) * tp_size + t) for yy in range(ny) for t in range(tp_size)
        ]
        even = (y + c) % 2 == 0
        adj_row = jnp.where(even, (y + ny - 1) % ny, (y + 1) % ny)
        keep = lax.dynamic_slice_in_dim(mine_dw, y * hk, hk, axis=0)
        give = lax.dynamic_slice_in_dim(mine_dw, adj_row * hk, hk, axis=0)
        got = lax.ppermute(give, mesh_axes, adj_perm)
        hh = half_of(y, c, ny)
        first = jnp.where(hh == 0, keep, got)
        second = jnp.where(hh == 0, got, keep)
        d_w = jnp.concatenate([first, second], axis=1)[:, :vocab].astype(BF16)
        return mean_loss.reshape(1), d_hidden, d_w

    return jax.shard_map(
        local_step,
        mesh=mesh,
        in_specs=(token_spec, P("fsdp", "tp"), label_spec),
        out_specs=(P("dp"), token_spec, P(("dp", "fsdp"), "tp")),
        check_vma=False,
    )
```

```python
import functools

import jax
import jax.numpy as jnp
from jax import lax
from jax.experimental import pallas as pl
from jax.experimental.pallas import tpu as pltpu
from jax.sharding import PartitionSpec as P

MESH = pl.DeviceIdType.MESH
F32 = jnp.float32
BF16 = jnp.bfloat16
NCH = 5
LOW = -1e30
ANY = pl.BlockSpec(memory_space=pl.ANY)


class Place:
    def __init__(self, nx, ny):
        tp = lax.axis_index("tp")
        self.nx, self.ny = nx, ny
        self.x, self.c, self.y = tp // 2, tp % 2, lax.axis_index("fsdp")
        up, down = (self.y + 1) % ny, (self.y + ny - 1) % ny
        even = (self.y + self.c) % 2 == 0
        self.up, self.down = up, down
        self.p = jnp.where(even, up, down)
        self.a = jnp.where(even, down, up)
        self.far = (self.y + 2) % ny
        self.half = ((self.y - self.c + ny) % ny) // 2

    def dev(self, x=None, y=None, c=None):
        x = self.x if x is None else x
        y = self.y if y is None else y
        c = self.c if c is None else c
        return {"fsdp": y, "tp": x * 2 + c}


def half_of(y, b, ny):
    return ((y - b + ny) % ny) // 2


def pick(n, table):
    out = 0
    for i, v in enumerate(table):
        if v:
            out = out + jnp.where(n == i, v, 0)
    return out


def remote(src, dst, ssem, rsem, dev):
    return pltpu.make_async_remote_copy(
        src_ref=src, dst_ref=dst, send_sem=ssem, recv_sem=rsem, device_id=dev, device_id_type=MESH
    )


def gather_logits_kernel(
    nx, ny, vocab,
    x_hbm, w_hbm, lab_hbm, xg, wo, z, sta, laba, xt,
    w, xown, xb, zb, bias, m, s, stm, xtb,
    xsend, xrecv, ysend, yrecv, wsend, wrecv, dsend, drecv, ssend, srecv, lsend, lrecv, loc, wloc, xsem, zsem, tsem,
):
    at = Place(nx, ny)
    x, y, c = at.x, at.y, at.c
    tr = xown.shape[0]
    hk = w_hbm.shape[0]
    sb = w.shape[2] // 2
    slot = NCH * sb
    left, right = (x + nx - 1) % nx, (x + 1) % nx
    top, bot = pl.ds(0, tr // 2), pl.ds(tr // 2, tr // 2)

    barrier = pltpu.get_barrier_semaphore()
    for k in range(1, nx):
        pl.semaphore_signal(barrier, inc=1, device_id=at.dev(x=(x + k) % nx), device_id_type=MESH)
    for k in range(nx):
        pl.semaphore_signal(barrier, inc=1, device_id=at.dev(x=(x + k) % nx, y=at.far), device_id_type=MESH)
    pl.semaphore_signal(barrier, inc=1, device_id=at.dev(y=at.up), device_id_type=MESH)
    pl.semaphore_signal(barrier, inc=1, device_id=at.dev(y=at.down), device_id_type=MESH)
    pl.semaphore_signal(barrier, inc=1, device_id=at.dev(c=1 - c), device_id_type=MESH)
    load_x = pltpu.make_async_copy(x_hbm, xown, loc.at[0])
    load_x.start()
    pl.semaphore_wait(barrier, 2 * nx + 2)
    load_x.wait()

    def x_send(r, to_right):
        i = 0 if to_right else 1
        src = xown if r == 0 else xg.at[1, x]
        return remote(src, xg.at[r, x], xsend.at[r, i], xrecv.at[r, i], at.dev(x=right if to_right else left))

    def x_relay(r, to_right):
        if to_right:
            part = xg.at[r, left, top]
            return remote(part, part, xsend.at[r, 2], xrecv.at[r, 2], at.dev(x=right))
        part = xg.at[r, right, bot]
        return remote(part, part, xsend.at[r, 3], xrecv.at[r, 3], at.dev(x=left))

    x_far = remote(xown, xg.at[1, x], ysend, yrecv, at.dev(y=at.far))
    keep_x = pltpu.make_async_copy(xown, xg.at[0, x], loc.at[1])

    def w_src(f, q):
        return w_hbm.at[:, pl.ds(pl.multiple_of(f * slot + q * sb, 128), sb)]

    def w_dst(k, q):
        return w.at[q, pl.ds(pl.multiple_of(k * hk, 16), hk), pl.ds(pl.multiple_of(c * sb, 128), sb)]

    def w_own(q):
        return remote(w_src(at.half, q), w_dst(y, q), wsend.at[0, q], wrecv.at[0, q], at.dev(y=at.p))

    def w_other(q):
        return remote(w_src(1 - at.half, q), w_dst(y, q), wsend.at[1, q], wrecv.at[1, q], at.dev(y=at.a))

    def w_fwd(q):
        return remote(w_dst(at.a, q), w_dst(at.a, q), wsend.at[2, q], wrecv.at[2, q], at.dev(y=at.p))

    def w_core(q):
        part = w.at[q, :, pl.ds(pl.multiple_of(c * sb, 128), sb)]
        return remote(part, part, dsend.at[q], drecv.at[q], at.dev(c=1 - c))

    def w_local(q):
        return pltpu.make_async_copy(w_src(at.half, q), w_dst(y, q), wloc.at[q])

    def w_out(q):
        w_own(q).start()
        w_other(q).start()

    w_out(0)
    x_send(0, True).start()
    x_send(0, False).start()
    keep_x.start()
    for q in range(NCH):
        w_local(q).start()

    peers = [(0, k) for k in range(1, nx)] + [(1, k) for k in range(nx)]

    def lab_copy(i):
        sy, k = peers[i]
        return remote(
            lab_hbm, laba.at[sy, x], lsend.at[i], lrecv.at[sy, x],
            at.dev(x=(x + k) % nx, y=at.far if sy else y),
        )

    for i in range(len(peers)):
        lab_copy(i).start()
    lab_own = pltpu.make_async_copy(lab_hbm, laba.at[0, x], loc.at[2])
    lab_own.start()

    col = lax.broadcasted_iota(jnp.int32, bias.shape, 1)
    row = lax.broadcasted_iota(jnp.int32, bias.shape, 0)
    b = col // sb
    pos = row * sb + col - b * sb
    half_b = jnp.where(b == 0, half_of(y, 0, ny), half_of(y, 1, ny))
    bias[...] = jnp.where((half_b == 1) & (pos >= vocab - slot), LOW, 0.0)
    m[...] = jnp.full_like(m, -3e38)
    s[...] = jnp.zeros_like(s)

    def xt_out(run, u):
        return pltpu.make_async_copy(
            xtb.at[u], xt.at[run // 2, :, pl.ds(pl.multiple_of((run % 2) * tr, 128), tr)], tsem.at[u]
        )

    w_other(0).wait_recv()
    w_fwd(0).start()
    w_out(1)
    w_other(1).wait_recv()
    w_fwd(1).start()
    w_out(2)
    keep_x.wait()
    x_send(0, True).wait_recv()
    x_relay(0, True).start()
    x_send(0, False).wait_recv()
    x_relay(0, False).start()

    n_steps = 2 * nx * NCH

    order = [(0, k, j) for k in (0, 3, 1, 2) for j in range(2)]
    order += [(0, k, 2) for k in (0, 3, 1, 2)]
    order += [(1, 0, 0), (1, 0, 1)]
    order += [(0, k, 3) for k in (0, 3, 1, 2)]
    order += [(1, 0, 2), (1, 0, 3)]
    order += [(0, k, 4) for k in (0, 3, 1, 2)]
    order += [(1, 0, 4)] + [(1, k, j) for k in (3, 1, 2) for j in range(NCH)]

    def place_of(i):
        code = pick(i, [(r * 4 + k) * 8 + j for r, k, j in order])
        run = code // 8
        return run // 4, code % 8, (x + run % 4) % nx

    def xcp(i, u):
        r, j, k = place_of(i)
        return pltpu.make_async_copy(xg.at[r, k], xb.at[u], xsem.at[u])

    def zcp(i, u):
        r, j, k = place_of(i)
        return pltpu.make_async_copy(zb.at[u], z.at[j, r, k], zsem.at[u])

    def step(i, u):
        r, j, k = place_of(i)
        run = r * nx + k
        c0 = 0
        for width in (sb * 4 // 5, 2 * sb - sb * 4 // 5) if sb % 640 == 0 else (2 * sb,):
            cols = slice(c0, c0 + width)
            zz = jnp.dot(xb[u], w[j, :, cols], preferred_element_type=F32) + bias[pl.ds(j, 1), cols]
            zb[u, :, cols] = zz
            blk = min(64, tr)
            for o in range(0, tr, blk):
                rows = slice(o, o + blk)
                m_old = m[run, rows, :]
                parts = [zz[rows, 128 * e : 128 * e + 128] for e in range(width // 128)]
                mx = m_old
                for part in parts:
                    mx = jnp.maximum(mx, part)
                acc = s[run, rows, :] * jnp.exp(m_old - mx)
                for part in parts:
                    acc = acc + jnp.exp(part - mx)
                m[run, rows, :] = mx
                s[run, rows, :] = acc
            c0 += width

    def stat_copy(r, i):
        sy, k = peers[i]
        rr = 1 - r if sy else r
        return remote(
            stm.at[r], sta.at[sy, x, rr], ssend.at[r, i], srecv.at[sy, x, rr],
            at.dev(x=(x + k) % nx, y=at.far if sy else y),
        )

    def stat_own(r):
        return pltpu.make_async_copy(stm.at[r], sta.at[0, x, r], loc.at[3 + r])

    def finish_stats(r):
        def one(d, _):
            run = r * nx + d
            mm = m[run]
            top_m = jnp.max(mm, axis=1, keepdims=True)
            tot = jnp.sum(s[run] * jnp.exp(mm - top_m), axis=1, keepdims=True)
            lane = lax.broadcasted_iota(jnp.int32, mm.shape, 1)
            blk = jnp.where(lane == 0, top_m, jnp.where(lane == 1, tot, 0.0))
            stm[r, d] = blk.T[0:8, :]
            return 0

        lax.fori_loop(0, nx, one, 0)
        for i in range(len(peers)):
            stat_copy(r, i).start()
        stat_own(r).start()

    def w_ready(j):
        w_local(j).wait()
        w_own(j).wait_recv()
        w_fwd(j).wait_recv()
        w_core(j).start()
        w_core(j).wait_recv()

    def body(t, _):
        @pl.when(t == 0)
        def _():
            for k in range(2):
                xcp(k, k).start()
            w_ready(0)
            w_ready(1)

        @pl.when(t == 2)
        def _():
            w_other(2).wait_recv()
            w_fwd(2).start()
            x_far.start()
            w_out(3)
            x_relay(0, True).wait_recv()
            x_relay(0, False).wait_recv()

        @pl.when(t == 4)
        def _():
            w_ready(2)

        @pl.when(t == 6)
        def _():
            x_far.wait_recv()
            x_send(1, True).start()
            x_send(1, False).start()
            for u in range(2):
                xcp(2 * t + u, u).start()

        @pl.when(t == 7)
        def _():
            w_other(3).wait_recv()
            w_fwd(3).start()
            w_out(4)
            w_ready(3)

        @pl.when(t == 8)
        def _():
            w_other(4).wait_recv()
            w_fwd(4).start()

        @pl.when(t == 10)
        def _():
            w_ready(4)
            pltpu.make_async_copy(w, wo, loc.at[5]).start()

        @pl.when(t == 11)
        def _():
            x_send(1, True).wait_recv()
            x_relay(1, True).start()
            x_send(1, False).wait_recv()
            x_relay(1, False).start()

        @pl.when(t == 12)
        def _():
            finish_stats(0)

        @pl.when(t == 16)
        def _():
            x_relay(1, True).wait_recv()
            x_relay(1, False).wait_recv()

        base = (t % 2) * 2
        for u in range(2):
            xcp(2 * t + u, base + u).wait()

        for u in range(2):
            r, j, k = place_of(2 * t + u)

            @pl.when(j == 0)
            def _():
                cp = xt_out(r * nx + k, u)
                xtb[u] = xb[base + u].T
                cp.start()

        @pl.when((2 * t + 2 < n_steps) & (t != 5))
        def _():
            for u in range(2):
                xcp(2 * t + 2 + u, 2 - base + u).start()

        @pl.when(t > 1)
        def _():
            for u in range(2):
                zcp(2 * t - 4 + u, base + u).wait()

        for u in range(2):
            step(2 * t + u, base + u)
        for u in range(2):
            zcp(2 * t + u, base + u).start()
            r, j, k = place_of(2 * t + u)

            @pl.when(j == 0)
            def _():
                xt_out(r * nx + k, u).wait()

        return 0

    lax.fori_loop(0, n_steps // 2, body, 0)
    finish_stats(1)
    for u in range(4):
        zcp(n_steps - 4 + u, u).wait()
    pltpu.make_async_copy(w, wo, loc.at[5]).wait()
    lab_own.wait()
    stat_own(0).wait()
    stat_own(1).wait()
    for r in range(2):
        for right_way in (True, False):
            x_send(r, right_way).wait_send()
            x_relay(r, right_way).wait_send()
    x_far.wait_send()
    for q in range(NCH):
        w_own(q).wait_send()
        w_other(q).wait_send()
        w_fwd(q).wait_send()
        w_core(q).wait_send()
    for i in range(len(peers)):
        lab_copy(i).wait_send()
        stat_copy(0, i).wait_send()
        stat_copy(1, i).wait_send()
    for sy in range(2):
        for k in range(nx):
            def arrived():
                remote(lab_hbm, laba.at[sy, k], lsend.at[0], lrecv.at[sy, k], at.dev(c=1 - c)).wait_recv()
                for rr in range(2):
                    remote(stm.at[rr], sta.at[sy, k, rr], ssend.at[0, 0], srecv.at[sy, k, rr], at.dev(c=1 - c)).wait_recv()

            if sy == 0:
                pl.when(k != x)(arrived)
            else:
                arrived()


def gather_logits(nx, ny, vocab, x, w, lab):
    tr, h = x.shape
    hk, vp = w.shape
    ch = vp // NCH
    shape = jax.ShapeDtypeStruct
    dma = pltpu.SemaphoreType.DMA
    vm = pltpu.VMEM
    flops = 2 * 2 * nx * tr * h * vp
    return pl.pallas_call(
        functools.partial(gather_logits_kernel, nx, ny, vocab),
        out_shape=(
            shape((2, nx, tr, h), BF16),
            shape((NCH, h, ch), BF16),
            shape((NCH, 2, nx, tr, ch), F32),
            shape((2, nx, 2, nx, 8, tr), F32),
            shape((2, nx) + lab.shape, jnp.int32),
            shape((nx, h, 2 * tr), BF16),
        ),
        in_specs=[ANY] * 3,
        out_specs=(ANY,) * 6,
        scratch_shapes=[
            vm((NCH, h, ch), BF16), vm((tr, h), BF16),
            vm((4, tr, h), BF16), vm((4, tr, ch), F32), vm((8, ch), F32),
            vm((2 * nx, tr, 128), F32), vm((2 * nx, tr, 128), F32), vm((2, nx, 8, tr), F32), vm((2, h, tr), BF16),
            dma((2, 4)), dma((2, 4)), dma, dma, dma((3, NCH)), dma((3, NCH)), dma((NCH,)), dma((NCH,)),
            dma((2, 2 * nx - 1)), dma((2, nx, 2)), dma((2 * nx - 1,)), dma((2, nx)),
            dma((6,)), dma((NCH,)), dma((4,)), dma((4,)), dma((2,)),
        ],
        compiler_params=pltpu.CompilerParams(
            collective_id=0, has_side_effects=True, vmem_limit_bytes=60 * 2**20
        ),
        cost_estimate=pl.CostEstimate(flops=flops, bytes_accessed=4 * 2 * nx * tr * vp, transcendentals=0),
        name="gather_logits",
    )(x, w, lab)


def grads_kernel(
    nx, ny, inv, z, w_hbm, xt_hbm, st8, dxo, dwo, loss, rx, fx, dd, rr,
    w, xt, zb, gb, acc, dx, st, lacc, tmpa, tmpb, keep, fin, fdx, lbuf,
    wsem, tsem, zsem, xsend, xrecv, fsend, frecv, dsend, drecv, rsend, rrecv, osend, orecv, asem, bsem, lsend, lrecv,
    out_sem,
):
    at = Place(nx, ny)
    x, y, c = at.x, at.y, at.c
    tr, h = dxo.shape
    ch = zb.shape[2]
    sb = ch // 2
    slot = NCH * sb
    hk = dwo.shape[0]
    nq = rx.shape[2]
    qr = tr // nq
    left, right = (x + nx - 1) % nx, (x + 1) % nx

    def par(yy, b):
        return jnp.where((yy + b) % 2 == 0, (yy + 1) % ny, (yy + ny - 1) % ny)

    def adj(yy, b):
        return jnp.where((yy + b) % 2 == 0, (yy + ny - 1) % ny, (yy + 1) % ny)

    for j in range(NCH):
        pltpu.make_async_copy(w_hbm.at[j], w.at[j], wsem.at[j]).start()
    barrier = pltpu.get_barrier_semaphore()
    for k in range(1, nx):
        pl.semaphore_signal(barrier, inc=1, device_id=at.dev(x=(x + k) % nx), device_id_type=MESH)
    for k in range(1, ny):
        pl.semaphore_signal(barrier, inc=1, device_id=at.dev(y=(y + k) % ny), device_id_type=MESH)
        pl.semaphore_signal(barrier, inc=1, device_id=at.dev(y=(y + k) % ny, c=1 - c), device_id_type=MESH)
    pl.semaphore_signal(barrier, inc=1, device_id=at.dev(c=1 - c), device_id_type=MESH)

    segments = ["x0", "w0", "w1", "x1", "w2", "w3", "x2", "w4", "x3"]
    bodies = []
    for seg in segments:
        for k in range(NCH if seg[0] == "x" else nx):
            bodies.append((0 if seg[0] == "x" else 1, int(seg[1]), k))
    n_body = len(bodies)
    first = {seg: bodies.index((0 if seg[0] == "x" else 1, int(seg[1]), 0)) for seg in segments}
    after = {seg: first[seg] + (NCH if seg[0] == "x" else nx) for seg in segments}

    def body_at(n):
        return pick(n, [b[0] for b in bodies]), pick(n, [b[1] for b in bodies]), pick(n, [b[2] for b in bodies])

    def tile(n, u):
        kind, i, k = body_at(n)
        mine = jnp.where(u == 0, (x + 2 * nx - 1 - i) % nx, (x + 1 + i) % nx)
        run = 2 * k + u
        is_x = kind == 0
        return jnp.where(is_x, k, i), jnp.where(is_x, u, run // nx), jnp.where(is_x, mine, run % nx)

    def zcp(n, u, buf):
        j, r, d = tile(n, u)
        return pltpu.make_async_copy(z.at[j, r, d], zb.at[buf], zsem.at[buf])

    for u in range(2):
        zcp(0, u, u).start()
    pltpu.make_async_copy(xt_hbm, xt, tsem).start()

    def spread(run, _):
        st[run] = jnp.concatenate([st8[run // nx, run % nx]] * 16, axis=0).T
        return 0

    lax.fori_loop(0, 2 * nx, spread, 0)
    lacc[...] = jnp.zeros_like(lacc)
    pl.semaphore_wait(barrier, nx - 1 + 2 * (ny - 1) + 1)

    def x_copy(s, dr, q):
        return remote(
            dx.at[s % 2, dr, pl.ds(pl.multiple_of(q * qr, 8), qr)], rx.at[s, dr, q],
            xsend.at[s, dr, q], xrecv.at[s, dr, q], at.dev(x=left if dr else right),
        )

    def far_copy(q):
        return remote(
            dx.at[1, 1, pl.ds(pl.multiple_of(q * qr, 8), qr)], fx.at[q], fsend.at[q], frecv.at[q], at.dev(y=at.far)
        )

    def a_load(s, q, dr):
        return pltpu.make_async_copy(rx.at[s - 1, dr, q], tmpa.at[q % 2, dr], asem.at[q % 2, dr])

    def a_pre(s, q):
        for dr in range(2):
            x_copy(s - 1, dr, q).wait_recv()
            a_load(s, q, dr).start()

    def a_use(s, q):
        rows = pl.ds(pl.multiple_of(q * qr, 8), qr)
        for dr in range(2):
            a_load(s, q, dr).wait()
            dx[s % 2, dr, rows, :] += tmpa[q % 2, dr]

        @pl.when(s < nx - 1)
        def _():
            for dr in range(2):
                x_copy(s, dr, q).start()

        @pl.when(s == nx - 1)
        def _():
            far_copy(q).start()

    def f_load(q):
        return pltpu.make_async_copy(fx.at[q], tmpa.at[q % 2, 0], asem.at[q % 2, 0])

    def f_out(q):
        return pltpu.make_async_copy(fdx.at[q % 2], dxo.at[pl.ds(pl.multiple_of(q * qr, 16), qr)], out_sem.at[q])

    def f_pre(q):
        far_copy(q).wait_recv()
        f_load(q).start()

    def f_use(q):
        f_load(q).wait()

        @pl.when(q > 1)
        def _():
            f_out(q - 2).wait()

        rows = pl.ds(pl.multiple_of(q * qr, 8), qr)
        fdx[q % 2] = (dx[1, 0, rows, :] + tmpa[q % 2, 0]).astype(BF16)
        f_out(q).start()

    def lot(b):
        q = (c + b) % 2
        slices = [(b + 2 * q) % ny, (b + 1 + 2 * q) % ny]
        other = [(b + 2 * (1 - q)) % ny, (b + 1 + 2 * (1 - q)) % ny]
        home = half_of(y, b, ny) == q
        kt = jnp.where(home, y, adj(y, b))
        it = jnp.where(slices[0] == kt, 0, 1)
        return slices, other, kt, it, home

    def rows_of(k):
        return pl.ds(pl.multiple_of(k * hk, 16), hk)

    def d_copy(j, b, i):
        other = lot(b)[1]
        return remote(
            acc.at[j % 2, rows_of(other[i]), pl.ds(b * sb, sb)], dd.at[j, b, i],
            dsend.at[j, b, i], drecv.at[j, b, i], at.dev(c=1 - c),
        )

    def d_send(j):
        for b in range(2):
            for i in range(2):
                d_copy(j, b, i).start()

    def r_load(j, b, i):
        return pltpu.make_async_copy(dd.at[j, b, i], tmpb.at[b, i], bsem.at[b, i])

    def r_pre(j):
        for b in range(2):
            for i in range(2):
                d_copy(j, b, i).wait_recv()
                r_load(j, b, i).start()

    def r_copy(j, b):
        slices, _, _, it, _ = lot(b)
        kg = jnp.where(it == 0, slices[1], slices[0])
        src = acc.at[j % 2, rows_of(kg), pl.ds(b * sb, sb)]
        return remote(src, rr.at[j, b], rsend.at[j, b], rrecv.at[j, b], at.dev(y=par(y, b)))

    def r_use(j):
        for b in range(2):
            slices, _, kt, it, _ = lot(b)
            kg = jnp.where(it == 0, slices[1], slices[0])
            for i in range(2):
                r_load(j, b, i).wait()

            acc[j % 2, rows_of(kg), pl.ds(b * sb, sb)] += tmpb[b, 1 - it]
            r_copy(j, b).start()
            keep[j % 2, b] = acc[j % 2, rows_of(kt), pl.ds(b * sb, sb)] + tmpb[b, it]

    def s_load(j, b):
        return pltpu.make_async_copy(rr.at[j, b], tmpb.at[b, 0], bsem.at[b, 0])

    def s_pre(j):
        for b in range(2):
            r_copy(j, b).wait_recv()
            s_load(j, b).start()

    def o_copy(j, b):
        kt = lot(b)[2]
        f = half_of(y, b, ny)
        dst = dwo.at[:, pl.ds(pl.multiple_of(f * slot + j * sb, 128), sb)]
        return remote(fin.at[b], dst, osend.at[j, b], orecv.at[f, j], at.dev(y=kt, c=b))

    def o_here(j, b):
        f = half_of(y, b, ny)
        dst = dwo.at[:, pl.ds(pl.multiple_of(f * slot + j * sb, 128), sb)]
        return pltpu.make_async_copy(fin.at[b], dst, orecv.at[f, j])

    def is_here(b):
        return lot(b)[4] & (c == b)

    def s_use(j):
        for b in range(2):
            s_load(j, b).wait()

            @pl.when((j > 0) & jnp.logical_not(is_here(b)))
            def _():
                o_copy(j - 1, b).wait_send()

            @pl.when((j > 0) & is_here(b))
            def _():
                o_here(j - 1, b).wait()

            fin[b] = (keep[j % 2, b] + tmpb[b, 0]).astype(BF16)

            @pl.when(is_here(b))
            def _():
                o_here(j, b).start()

            @pl.when(jnp.logical_not(is_here(b)))
            def _():
                o_copy(j, b).start()

    def l_copy(stage, k):
        if stage == 0:
            return remote(lbuf.at[0, x], lbuf.at[0, x], lsend.at[0, k], lrecv.at[0, x], at.dev(x=(x + k) % nx))
        if stage == 1:
            return remote(lbuf.at[1, y], lbuf.at[1, y], lsend.at[1, k], lrecv.at[1, y], at.dev(y=(y + k) % ny))
        return remote(lbuf.at[2, c], lbuf.at[2, c], lsend.at[2, 0], lrecv.at[2, c], at.dev(c=1 - c))

    def l_sum(stage, size, me):
        for k in range(size):
            @pl.when(k != me)
            def _():
                remote(
                    lbuf.at[stage, k], lbuf.at[stage, k], lsend.at[stage, 0], lrecv.at[stage, k], at.dev(c=1 - c)
                ).wait_recv()

        total = lbuf[stage, 0]
        for k in range(1, size):
            total = total + lbuf[stage, k]
        return total

    def l_start():
        mine = -jnp.sum(lacc[...].reshape(-1, 8, 128), axis=0)
        logs = st8[0, x, 3:4, :]
        for o in range(tr // 128):
            mine = mine + jnp.concatenate([logs[:, 128 * o : 128 * o + 128], jnp.zeros((7, 128), F32)], axis=0)
        lbuf[0, x] = mine
        for k in range(1, nx):
            l_copy(0, k).start()

    def l_mid():
        lbuf[1, y] = l_sum(0, nx, x)
        for k in range(1, ny):
            l_copy(1, k).start()

    def l_late():
        lbuf[2, c] = l_sum(1, ny, y)
        l_copy(2, 0).start()

    def make_g(n, u, buf, c0, c1, want_loss):
        j, r, d = tile(n, u)
        run = r * nx + d
        blk = min(64, tr)
        for o in range(0, tr, blk):
            rows = slice(o, o + blk)
            t = st[run, rows, :]
            top = jnp.broadcast_to(t[:, 0:1], (blk, 128))
            scale = jnp.broadcast_to(t[:, 1:2], (blk, 128))
            lab = jnp.broadcast_to(t[:, 2:3], (blk, 128)).astype(jnp.int32) - j * ch
            lane = lax.broadcasted_iota(jnp.int32, (blk, 128), 1)
            add = jnp.zeros((blk, 128), F32)
            for e in range(c0 // 128, c1 // 128):
                cols = slice(128 * e, 128 * e + 128)
                dist = zb[buf, rows, cols] - top
                g = jnp.exp(dist) * scale
                hit = lab - 128 * e == lane
                if want_loss:
                    add = add + jnp.where(hit, dist, 0.0)
                gb[u, rows, cols] = jnp.where(hit, g - inv, g).astype(BF16)
            if want_loss:
                lacc[...] += add

    x_cuts = [(0, ch * 2 // 5), (ch * 2 // 5, ch)] if ch % 640 == 0 else [(0, ch)]
    w_cuts = [(0, ch // 5), (ch // 5, ch * 3 // 5), (ch * 3 // 5, ch)] if ch % 1280 == 0 else [(0, ch)]

    def x_body(n, base):
        _, s, j = body_at(n)
        half = s % 2

        @pl.when(j == 0)
        def _():
            dx[half] = jnp.zeros(dx.shape[1:], F32)

        for u in range(2):
            for c0, c1 in x_cuts:
                make_g(n, u, base + u, c0, c1, True)
                dx[half, u] += lax.dot_general(
                    gb[u, :, c0:c1], w[j, :, c0:c1], (((1,), (1,)), ((), ())), preferred_element_type=F32
                )

    def w_body(n, base):
        _, j, k = body_at(n)
        half = j % 2

        @pl.when(k == 0)
        def _():
            acc[half] = jnp.zeros(acc.shape[1:], F32)

        for c0, c1 in w_cuts:
            for u in range(2):
                make_g(n, u, base + u, c0, c1, False)
            acc[half, :, c0:c1] += jnp.dot(
                xt[k], gb[:, :, c0:c1].reshape(2 * tr, c1 - c0), preferred_element_type=F32
            )

    last = n_body
    plan_a = [(after["x1"] + q, 1, q) for q in range(nq)] + [(after["x2"] + q, 2, q) for q in range(nq)]
    plan_a += [(last + q, 3, q) for q in range(nq)]
    plan_r = [(11, 12, 0), (15, 17, 1), (24, 25, 2), (28, 30, 3), (37, 38, 4)]
    plan_s = [(18, 19, 0), (22, 23, 1), (31, 32, 2), (35, 36, 3), (last + 1, last + 2, 4)]
    plan_f = [(last + nq + q, q) for q in range(nq)]
    n_all = last + 2 * nq

    def when(n, table, fn):
        table = [(e[0], e[1:]) for e in table]
        hit = functools.reduce(lambda p, q: p | q, [n == e for e, _ in table])

        @pl.when(hit)
        def _():
            args = []
            for i in range(len(table[0][1])):
                val = 0
                for e, vals in table:
                    if vals[i]:
                        val = val + jnp.where(n == e, vals[i], 0)
                args.append(val + jnp.int32(0))
            fn(*args)

    def body(n, _):
        @pl.when(n < NCH)
        def _():
            pltpu.make_async_copy(w_hbm.at[n], w.at[n], wsem.at[n]).wait()

        @pl.when(n == first["w0"])
        def _():
            pltpu.make_async_copy(xt_hbm, xt, tsem).wait()
            for q in range(nq):
                for dr in range(2):
                    x_copy(0, dr, q).start()

        when(n, [(after["w%d" % j], j) for j in range(NCH)], d_send)
        when(n, plan_a, a_use)
        when(n, plan_f, f_use)
        when(n, [(e[1], e[2]) for e in plan_r], r_use)
        when(n, [(e[1], e[2]) for e in plan_s], s_use)
        when(n, [(e[0] - 1,) + e[1:] for e in plan_a], a_pre)
        when(n, [(e[0] - 1,) + e[1:] for e in plan_f], f_pre)
        when(n, [(e[0], e[2]) for e in plan_r], r_pre)
        when(n, [(e[0], e[2]) for e in plan_s], s_pre)

        @pl.when(n == last)
        def _():
            l_start()

        @pl.when(n == last + 2)
        def _():
            l_mid()

        @pl.when(n == last + nq + 1)
        def _():
            l_late()

        @pl.when((n == first["x2"]) | (n == first["x3"]))
        def _():
            s = jnp.where(n == first["x2"], 0, 1)
            for q in range(nq):
                for dr in range(2):
                    x_copy(s, dr, q).wait_send()

        for j in range(2, NCH):
            @pl.when(n == first["w%d" % j])
            def _():
                for b in range(2):
                    r_copy(j - 2, b).wait_send()
                    for i in range(2):
                        d_copy(j - 2, b, i).wait_send()

        base = (n % 2) * 2

        @pl.when(n < n_body)
        def _():
            for u in range(2):
                zcp(n, u, base + u).wait()

            @pl.when(n + 1 < n_body)
            def _():
                for u in range(2):
                    zcp(n + 1, u, 2 - base + u).start()

            kind = body_at(n)[0]

            @pl.when(kind == 0)
            def _():
                x_body(n, base)

            @pl.when(kind == 1)
            def _():
                w_body(n, base)

        return 0

    lax.fori_loop(0, n_all, body, 0)
    loss[...] = l_sum(2, 2, c)

    for q in range(nq):
        if q >= nq - 2:
            f_out(q).wait()
        far_copy(q).wait_send()
        for dr in range(2):
            x_copy(2, dr, q).wait_send()
    for b in range(2):
        for j in range(NCH - 2, NCH):
            for i in range(2):
                d_copy(j, b, i).wait_send()
            r_copy(j, b).wait_send()

        @pl.when(is_here(b))
        def _():
            o_here(NCH - 1, b).wait()

        @pl.when(jnp.logical_not(is_here(b)))
        def _():
            o_copy(NCH - 1, b).wait_send()

    q0 = half_of(y, c, ny)
    for f in range(2):
        local = (f == q0) & ((q0 + c) % 2 == c)

        @pl.when(jnp.logical_not(local))
        def _():
            for j in range(NCH):
                dst = dwo.at[:, pl.ds(f * slot + j * sb, sb)]
                remote(fin.at[0], dst, osend.at[j, 0], orecv.at[f, j], at.dev(c=1 - c)).wait_recv()

    for k in range(1, nx):
        l_copy(0, k).wait_send()
    for k in range(1, ny):
        l_copy(1, k).wait_send()
    l_copy(2, 0).wait_send()


def grads(nx, ny, inv, z, w, xt, st8, hk):
    h = w.shape[1]
    ch = w.shape[2]
    tr = z.shape[3]
    nq = 4
    shape = jax.ShapeDtypeStruct
    dma = pltpu.SemaphoreType.DMA
    vm = pltpu.VMEM
    vspec = pl.BlockSpec(memory_space=pltpu.VMEM)
    sb, qr = ch // 2, tr // nq
    return pl.pallas_call(
        functools.partial(grads_kernel, nx, ny, inv),
        out_shape=(
            shape((tr, h), BF16), shape((hk, NCH * ch), BF16), shape((8, 128), F32),
            shape((nx - 1, 2, nq, qr, h), F32), shape((nq, qr, h), F32),
            shape((NCH, 2, 2, hk, sb), F32), shape((NCH, 2, hk, sb), F32),
        ),
        in_specs=[ANY, ANY, ANY, vspec],
        out_specs=(ANY, ANY, vspec, ANY, ANY, ANY, ANY),
        scratch_shapes=[
            vm((NCH, h, ch), BF16), vm((nx, h, 2 * tr), BF16), vm((4, tr, ch), F32), vm((2, tr, ch), BF16),
            vm((2, h, ch), F32), vm((2, 2, tr, h), F32), vm((2 * nx, tr, 128), F32), vm((min(64, tr), 128), F32),
            vm((2, 2, qr, h), F32), vm((2, 2, hk, sb), F32), vm((2, 2, hk, sb), F32),
            vm((2, hk, sb), BF16), vm((2, qr, h), BF16), vm((3, max(nx, ny), 8, 128), F32),
            dma((NCH,)), dma, dma((4,)), dma((nx - 1, 2, nq)), dma((nx - 1, 2, nq)), dma((nq,)), dma((nq,)),
            dma((NCH, 2, 2)), dma((NCH, 2, 2)), dma((NCH, 2)), dma((NCH, 2)), dma((NCH, 2)), dma((2, NCH)),
            dma((2, 2)), dma((2, 2)), dma((3, max(nx, ny))), dma((3, max(nx, ny))), dma((nq,)),
        ],
        compiler_params=pltpu.CompilerParams(
            collective_id=1, has_side_effects=True, vmem_limit_bytes=67_000_000
        ),
        name="grads",
    )(z, w, xt, st8)


def solution(mesh):
    ny = mesh.shape["fsdp"]
    tp_size = mesh.shape["tp"]
    nx = tp_size // 2
    token_spec = P(("dp", "fsdp", "tp"), None)
    label_spec = P(("dp", "fsdp", "tp"))

    def local_step(hidden, w_head, labels):
        tr, h = hidden.shape
        hk, vocab = w_head.shape
        inv = 1.0 / (tr * tp_size * ny)
        vp = -(-vocab // (256 * NCH)) * (256 * NCH)
        ch = vp // NCH
        sb = ch // 2
        slot = NCH * sb
        tp = lax.axis_index("tp")
        x, y = tp // 2, lax.axis_index("fsdp")
        w_pad = jnp.pad(w_head, ((0, 0), (0, vp - vocab)))
        lab8 = jnp.pad(labels.reshape(-1, 128), ((0, 8 - tr // 128), (0, 0)))
        xg, wg, z, sta, laba, xt = gather_logits(nx, ny, vocab, hidden, w_pad, lab8)

        ms = sta[..., 0, :].reshape(2 * nx, 2, nx, tr)
        ss = sta[..., 1, :].reshape(2 * nx, 2, nx, tr)
        top = jnp.max(ms, axis=0)
        tot = jnp.sum(ss * jnp.exp(ms - top), axis=0)
        lab = laba[:, :, 0 : tr // 128, :].reshape(2, nx, tr)
        shard, off = lab // vocab, lab % vocab
        b, f = shard % 2, off // slot
        pos = off - f * slot
        mine = (shard // 2 == x) & (half_of(y, b, ny) == f)
        col = jnp.where(mine, (pos // sb) * ch + b * sb + pos % sb, -1)
        rows = [top, inv / tot, col.astype(F32), jnp.log(tot)]
        st8 = jnp.stack(rows + [jnp.zeros_like(top)] * 4, axis=2)
        d_hidden, d_w, loss = grads(nx, ny, inv, z, wg, xt, st8, hk)[:3]
        mean_loss = jnp.sum(loss) * inv
        return mean_loss.reshape(1), d_hidden, d_w[:, :vocab]

    return jax.shard_map(
        local_step,
        mesh=mesh,
        in_specs=(token_spec, P("fsdp", "tp"), label_spec),
        out_specs=(P("dp"), token_spec, P(("dp", "fsdp"), "tp")),
        check_vma=False,
    )
```

```python
import functools

import jax
import jax.numpy as jnp
from jax import lax
from jax.experimental import pallas as pl
from jax.experimental.pallas import tpu as pltpu
from jax.sharding import PartitionSpec as P

MESH = pl.DeviceIdType.MESH
F32 = jnp.float32
BF16 = jnp.bfloat16
NCH = 5
LOW = -1e30
ANY = pl.BlockSpec(memory_space=pl.ANY)
LANES = 128
SUB = 8
TWO = 2
BOTH = range(TWO)
RIGHT, LEFT = True, False


class Place:
    def __init__(self, nx, ny):
        tp = lax.axis_index("tp")
        self.nx, self.ny = nx, ny
        self.x, self.c, self.y = tp // TWO, tp % TWO, lax.axis_index("fsdp")
        up, down = (self.y + 1) % ny, (self.y + ny - 1) % ny
        even = (self.y + self.c) % TWO == 0
        self.up, self.down = up, down
        self.pc = 1 - self.c
        self.p = jnp.where(even, up, down)
        self.a = jnp.where(even, down, up)
        self.far = (self.y + 2) % ny
        self.half = ((self.y - self.c + ny) % ny) // TWO

    def dev(self, x=None, y=None, c=None):
        x = self.x if x is None else x
        y = self.y if y is None else y
        c = self.c if c is None else c
        return {"fsdp": y, "tp": x * 2 + c}


def half_of(y, b, ny):
    return ((y - b + ny) % ny) // TWO


def pick(n, table):
    out = 0
    for i, v in enumerate(table):
        if v:
            out = out + jnp.where(n == i, v, 0)
    return out


def remote(src, dst, ssem, rsem, dev):
    return pltpu.make_async_remote_copy(
        src_ref=src, dst_ref=dst, send_sem=ssem, recv_sem=rsem, device_id=dev, device_id_type=MESH
    )


def local(src, dst, sem):
    return pltpu.make_async_copy(src, dst, sem)


def gather_logits_kernel(
    nx, ny, vocab,
    x_hbm, w_hbm, lab_hbm, xg, wo, z, sta, laba, xt,
    w, xown, xb, zb, bias, m, s, stm, xtb,
    xsend, xrecv, ysend, yrecv, wsend, wrecv, dsend, drecv, ssend, srecv, lsend, lrecv, loc, wloc, xsem, zsem, tsem,
):
    at = Place(nx, ny)
    x, y, c = at.x, at.y, at.c
    tr = xown.shape[0]
    hk = w_hbm.shape[0]
    sb = w.shape[2] // TWO
    slot = NCH * sb
    left, right = (x + nx - 1) % nx, (x + 1) % nx
    top, bot = pl.ds(0, tr // TWO), pl.ds(tr // TWO, tr // TWO)

    barrier = pltpu.get_barrier_semaphore()
    for k in range(1, nx):
        pl.semaphore_signal(barrier, inc=1, device_id=at.dev(x=(x + k) % nx), device_id_type=MESH)
    for k in range(nx):
        pl.semaphore_signal(barrier, inc=1, device_id=at.dev(x=(x + k) % nx, y=at.far), device_id_type=MESH)
    pl.semaphore_signal(barrier, inc=1, device_id=at.dev(y=at.up), device_id_type=MESH)
    pl.semaphore_signal(barrier, inc=1, device_id=at.dev(y=at.down), device_id_type=MESH)
    pl.semaphore_signal(barrier, inc=1, device_id=at.dev(c=at.pc), device_id_type=MESH)
    load_x = local(x_hbm, xown, loc.at[0])
    load_x.start()
    pl.semaphore_wait(barrier, TWO * nx + 2)
    load_x.wait()

    def x_send(r, to_right):
        i = 0 if to_right else 1
        src = xown if r == 0 else xg.at[1, x]
        return remote(src, xg.at[r, x], xsend.at[r, i], xrecv.at[r, i], at.dev(x=right if to_right else left))

    def x_relay(r, to_right):
        if to_right:
            part = xg.at[r, left, top]
            return remote(part, part, xsend.at[r, 2], xrecv.at[r, 2], at.dev(x=right))
        part = xg.at[r, right, bot]
        return remote(part, part, xsend.at[r, 3], xrecv.at[r, 3], at.dev(x=left))

    x_far = remote(xown, xg.at[1, x], ysend, yrecv, at.dev(y=at.far))
    keep_x = local(xown, xg.at[0, x], loc.at[1])

    def w_src(f, q):
        return w_hbm.at[:, pl.ds(pl.multiple_of(f * slot + q * sb, LANES), sb)]

    def w_dst(k, q):
        return w.at[q, pl.ds(pl.multiple_of(k * hk, 16), hk), pl.ds(pl.multiple_of(c * sb, LANES), sb)]

    def w_own(q):
        return remote(w_src(at.half, q), w_dst(y, q), wsend.at[0, q], wrecv.at[0, q], at.dev(y=at.p))

    def w_other(q):
        return remote(w_src(1 - at.half, q), w_dst(y, q), wsend.at[1, q], wrecv.at[1, q], at.dev(y=at.a))

    def w_fwd(q):
        return remote(w_dst(at.a, q), w_dst(at.a, q), wsend.at[2, q], wrecv.at[2, q], at.dev(y=at.p))

    def w_core(q):
        part = w.at[q, :, pl.ds(pl.multiple_of(c * sb, LANES), sb)]
        return remote(part, part, dsend.at[q], drecv.at[q], at.dev(c=at.pc))

    def w_local(q):
        return local(w_src(at.half, q), w_dst(y, q), wloc.at[q])

    def w_out(q):
        w_own(q).start()
        w_other(q).start()

    w_out(0)
    x_send(0, RIGHT).start()
    x_send(0, LEFT).start()
    keep_x.start()
    for q in range(NCH):
        w_local(q).start()

    peers = [(0, k) for k in range(1, nx)] + [(1, k) for k in range(nx)]

    def lab_copy(i):
        sy, k = peers[i]
        return remote(
            lab_hbm, laba.at[sy, x], lsend.at[i], lrecv.at[sy, x],
            at.dev(x=(x + k) % nx, y=at.far if sy else y),
        )

    for i in range(len(peers)):
        lab_copy(i).start()
    lab_own = local(lab_hbm, laba.at[0, x], loc.at[2])
    lab_own.start()

    tail = lax.broadcasted_iota(jnp.int32, bias.shape[1:], 1)
    slot_of = tail // LANES
    pos = slot - LANES + tail - slot_of * LANES
    half_b = jnp.where(slot_of == 0, half_of(y, 0, ny), half_of(y, 1, ny))
    bias[...] = jnp.zeros_like(bias)
    bias[NCH - 1] = jnp.where((half_b == 1) & (pos >= vocab - slot), LOW, 0.0)
    m[...] = jnp.full_like(m, -3e38)
    s[...] = jnp.zeros_like(s)

    def xt_out(run, u):
        return local(
            xtb.at[u], xt.at[run // TWO, :, pl.ds(pl.multiple_of((run % TWO) * tr, LANES), tr)], tsem.at[u]
        )

    w_other(0).wait_recv()
    w_fwd(0).start()
    w_out(1)
    w_other(1).wait_recv()
    w_fwd(1).start()
    w_out(2)
    keep_x.wait()
    x_send(0, RIGHT).wait_recv()
    x_relay(0, RIGHT).start()
    x_send(0, LEFT).wait_recv()
    x_relay(0, LEFT).start()

    n_steps = TWO * nx * NCH

    order = [(0, k, j) for k in (0, 3, 1, TWO) for j in BOTH]
    order += [(0, k, TWO) for k in (0, 3, 1, TWO)]
    order += [(1, 0, 0), (1, 0, 1)]
    order += [(0, k, 3) for k in (0, 3, 1, TWO)]
    order += [(1, 0, TWO), (1, 0, 3)]
    order += [(0, k, 4) for k in (0, 3, 1, TWO)]
    order += [(1, 0, 4)] + [(1, k, j) for k in (3, 1, TWO) for j in range(NCH)]

    codes = [(r * 4 + k) * 8 + j for r, k, j in order]

    def code_of(t):
        return tuple(pick(t, codes[u::TWO]) for u in BOTH)

    def place_of(code):
        run = code // 8
        return run // 4, code % 8, (x + run % 4) % nx

    def xcp(i, u):
        r, j, k = place_of(i)
        return local(xg.at[r, k], xb.at[u], xsem.at[u])

    def zcp(i, u):
        r, j, k = place_of(i)
        return local(zb.at[u], z.at[j, r, k], zsem.at[u])

    def step(i, u):
        r, j, k = place_of(i)
        run = r * nx + k
        c0 = 0
        for width in (sb * 4 // 5, TWO * sb - sb * 4 // 5) if sb % 640 == 0 else (2 * sb,):
            cols = slice(c0, c0 + width)
            zz = jnp.dot(xb[u], w[j, :, cols], preferred_element_type=F32)
            zb[u, :, cols] = zz
            blk = min(64, tr)
            for o in range(0, tr, blk):
                rows = slice(o, o + blk)
                m_old = m[run, rows, :]
                parts = [zz[rows, LANES * e : LANES * e + LANES] for e in range(width // LANES)]
                for e in range(width // LANES):
                    at_e = slice(c0 + LANES * e, c0 + LANES * e + LANES)
                    if at_e.stop % sb == 0:
                        end = at_e.stop // sb
                        parts[e] = parts[e] + bias[j, 0:1, LANES * end - LANES : LANES * end]
                        zb[u, rows, at_e] = parts[e]
                mx = m_old
                for part in parts:
                    mx = jnp.maximum(mx, part)
                acc = s[run, rows, :] * jnp.exp(m_old - mx)
                for part in parts:
                    acc = acc + jnp.exp(part - mx)
                m[run, rows, :] = mx
                s[run, rows, :] = acc
            c0 += width

    def stat_copy(r, i):
        sy, k = peers[i]
        rr = 1 - r if sy else r
        return remote(
            stm.at[r], sta.at[sy, x, rr], ssend.at[r, i], srecv.at[sy, x, rr],
            at.dev(x=(x + k) % nx, y=at.far if sy else y),
        )

    def stat_own(r):
        return local(stm.at[r], sta.at[0, x, r], loc.at[3 + r])

    def finish_stats(r):
        def one(d, _):
            run = r * nx + d
            mm = m[run]
            top_m = jnp.max(mm, axis=1, keepdims=True)
            tot = jnp.sum(s[run] * jnp.exp(mm - top_m), axis=1, keepdims=True)
            lane = lax.broadcasted_iota(jnp.int32, mm.shape, 1)
            blk = jnp.where(lane == 0, top_m, jnp.where(lane == 1, tot, 0.0))
            stm[r, d] = blk.T[0:SUB, :]
            return 0

        lax.fori_loop(0, nx, one, 0)
        for i in range(len(peers)):
            stat_copy(r, i).start()
        stat_own(r).start()

    def w_ready(j):
        w_local(j).wait()
        w_own(j).wait_recv()
        w_fwd(j).wait_recv()
        w_core(j).start()
        w_core(j).wait_recv()

    def body(t, held):
        older, old, now = held
        later = code_of(t + 1)

        @pl.when(t == 0)
        def _():
            for u in BOTH:
                xcp(now[u], u).start()
            w_ready(0)
            w_ready(1)

        @pl.when(t == 2)
        def _():
            w_other(2).wait_recv()
            w_fwd(2).start()
            x_far.start()
            w_out(3)
            x_relay(0, RIGHT).wait_recv()
            x_relay(0, LEFT).wait_recv()

        @pl.when(t == 4)
        def _():
            w_ready(2)

        @pl.when(t == 6)
        def _():
            x_far.wait_recv()
            x_send(1, RIGHT).start()
            x_send(1, LEFT).start()
            for u in BOTH:
                xcp(now[u], u).start()

        @pl.when(t == 7)
        def _():
            w_other(3).wait_recv()
            w_fwd(3).start()
            w_out(4)
            w_ready(3)

        @pl.when(t == 8)
        def _():
            w_other(4).wait_recv()
            w_fwd(4).start()

        @pl.when(t == 10)
        def _():
            w_ready(4)
            local(w, wo, loc.at[5]).start()

        @pl.when(t == 11)
        def _():
            x_send(1, RIGHT).wait_recv()
            x_relay(1, RIGHT).start()
            x_send(1, LEFT).wait_recv()
            x_relay(1, LEFT).start()

        @pl.when(t == 12)
        def _():
            finish_stats(0)

        @pl.when(t == 16)
        def _():
            x_relay(1, RIGHT).wait_recv()
            x_relay(1, LEFT).wait_recv()

        base = (t % TWO) * 2
        for u in BOTH:
            xcp(now[u], base + u).wait()

        for u in BOTH:
            r, j, k = place_of(now[u])

            @pl.when(j == 0)
            def _():
                cp = xt_out(r * nx + k, u)
                xtb[u] = xb[base + u].T
                cp.start()

        @pl.when((TWO * t + 2 < n_steps) & (t != 5))
        def _():
            for u in BOTH:
                xcp(later[u], 2 - base + u).start()

        @pl.when(t > 1)
        def _():
            for u in BOTH:
                zcp(older[u], base + u).wait()

        for u in BOTH:
            step(now[u], base + u)
        for u in BOTH:
            zcp(now[u], base + u).start()
            r, j, k = place_of(now[u])

            @pl.when(j == 0)
            def _():
                xt_out(r * nx + k, u).wait()

        return old, now, later

    none = (jnp.int32(0),) * TWO
    older, old, _ = lax.fori_loop(0, n_steps // TWO, body, (none, none, code_of(jnp.int32(0))))
    finish_stats(1)
    for u in BOTH:
        zcp(older[u], u).wait()
        zcp(old[u], TWO + u).wait()
    local(w, wo, loc.at[5]).wait()
    lab_own.wait()
    stat_own(0).wait()
    stat_own(1).wait()
    for r in BOTH:
        for right_way in (RIGHT, LEFT):
            x_send(r, right_way).wait_send()
            x_relay(r, right_way).wait_send()
    x_far.wait_send()
    for q in range(NCH):
        w_own(q).wait_send()
        w_other(q).wait_send()
        w_fwd(q).wait_send()
        w_core(q).wait_send()
    for i in range(len(peers)):
        lab_copy(i).wait_send()
        stat_copy(0, i).wait_send()
        stat_copy(1, i).wait_send()
    for sy in BOTH:
        for k in range(nx):
            def arrived():
                remote(lab_hbm, laba.at[sy, k], lsend.at[0], lrecv.at[sy, k], at.dev(c=at.pc)).wait_recv()
                for rr in BOTH:
                    remote(stm.at[rr], sta.at[sy, k, rr], ssend.at[0, 0], srecv.at[sy, k, rr], at.dev(c=at.pc)).wait_recv()

            if sy == 0:
                pl.when(k != x)(arrived)
            else:
                arrived()


def gather_logits(nx, ny, vocab, x, w, lab):
    tr, h = x.shape
    hk, vp = w.shape
    ch = vp // NCH
    shape = jax.ShapeDtypeStruct
    dma = pltpu.SemaphoreType.DMA
    vm = pltpu.VMEM
    flops = TWO * TWO * nx * tr * h * vp
    return pl.pallas_call(
        functools.partial(gather_logits_kernel, nx, ny, vocab),
        out_shape=(
            shape((TWO, nx, tr, h), BF16),
            shape((NCH, h, ch), BF16),
            shape((NCH, TWO, nx, tr, ch), F32),
            shape((TWO, nx, TWO, nx, SUB, tr), F32),
            shape((TWO, nx) + lab.shape, jnp.int32),
            shape((nx, h, TWO * tr), BF16),
        ),
        in_specs=[ANY] * 3,
        out_specs=(ANY,) * 6,
        scratch_shapes=[
            vm((NCH, h, ch), BF16), vm((tr, h), BF16),
            vm((4, tr, h), BF16), vm((4, tr, ch), F32), vm((NCH, SUB, TWO * LANES), F32),
            vm((TWO * nx, tr, LANES), F32), vm((TWO * nx, tr, LANES), F32), vm((TWO, nx, SUB, tr), F32), vm((TWO, h, tr), BF16),
            dma((TWO, 4)), dma((TWO, 4)), dma, dma, dma((3, NCH)), dma((3, NCH)), dma((NCH,)), dma((NCH,)),
            dma((TWO, TWO * nx - 1)), dma((TWO, nx, TWO)), dma((TWO * nx - 1,)), dma((TWO, nx)),
            dma((6,)), dma((NCH,)), dma((4,)), dma((4,)), dma((TWO,)),
        ],
        compiler_params=pltpu.CompilerParams(
            collective_id=0, has_side_effects=True, vmem_limit_bytes=60 * 2**20
        ),
        cost_estimate=pl.CostEstimate(flops=flops, bytes_accessed=4 * TWO * nx * tr * vp, transcendentals=0),
        name="gather_logits",
    )(x, w, lab)


def grads_kernel(
    nx, ny, inv, z, w_hbm, xt_hbm, st8, dxo, dwo, loss, rx, fx, dd, rr,
    w, xt, zb, gb, acc, dx, st, lacc, tmpa, tmpb, keep, fin, fdx, lbuf,
    wsem, tsem, zsem, xsend, xrecv, fsend, frecv, dsend, drecv, rsend, rrecv, osend, orecv, asem, bsem, lsend, lrecv,
    out_sem,
):
    at = Place(nx, ny)
    x, y, c = at.x, at.y, at.c
    tr, h = dxo.shape
    ch = zb.shape[2]
    sb = ch // TWO
    slot = NCH * sb
    hk = dwo.shape[0]
    nq = rx.shape[2]
    qr = tr // nq
    left, right = (x + nx - 1) % nx, (x + 1) % nx

    def par(yy, b):
        return jnp.where((yy + b) % TWO == 0, (yy + 1) % ny, (yy + ny - 1) % ny)

    def adj(yy, b):
        return jnp.where((yy + b) % TWO == 0, (yy + ny - 1) % ny, (yy + 1) % ny)

    for j in range(NCH):
        local(w_hbm.at[j], w.at[j], wsem.at[j]).start()
    barrier = pltpu.get_barrier_semaphore()
    for k in range(1, nx):
        pl.semaphore_signal(barrier, inc=1, device_id=at.dev(x=(x + k) % nx), device_id_type=MESH)
    for k in range(1, ny):
        pl.semaphore_signal(barrier, inc=1, device_id=at.dev(y=(y + k) % ny), device_id_type=MESH)
        pl.semaphore_signal(barrier, inc=1, device_id=at.dev(y=(y + k) % ny, c=at.pc), device_id_type=MESH)
    pl.semaphore_signal(barrier, inc=1, device_id=at.dev(c=at.pc), device_id_type=MESH)

    segments = ["x0", "w0", "w1", "x1", "w2", "w3", "x2", "w4", "x3"]
    segments += ["l%d" % j for j in range(NCH)]
    first, after, n_body = {}, {}, 0
    for seg in segments:
        first[seg] = n_body
        n_body += NCH if seg.startswith("x") else nx
        after[seg] = n_body

    def body_at(n):
        code, start = 0, 0
        for seg in segments[1:]:
            here = n >= first[seg]
            code = jnp.where(here, "xwl".index(seg[0]) * 8 + int(seg[-1]), code)
            start = jnp.where(here, first[seg], start)
        return code // 8, code % 8, n - start

    def tile(n, u):
        kind, i, k = body_at(n)
        mine = jnp.where(u == 0, (x + TWO * nx - 1 - i) % nx, (x + 1 + i) % nx)
        run = TWO * k + u
        is_x = kind == 0
        return jnp.where(is_x, k, i), jnp.where(is_x, u, run // nx), jnp.where(is_x, mine, run % nx)

    def zcp(n, u, buf):
        j, r, d = tile(n, u)
        return local(z.at[j, r, d], zb.at[buf], zsem.at[buf])

    for u in BOTH:
        zcp(0, u, u).start()
    local(xt_hbm, xt, tsem).start()

    def spread(run, _):
        st[run] = jnp.concatenate([st8[run // nx, run % nx]] * 16, axis=0).T
        return 0

    lax.fori_loop(0, TWO * nx, spread, 0)
    lacc[...] = jnp.zeros_like(lacc)
    pl.semaphore_wait(barrier, nx - 1 + TWO * (ny - 1) + 1)

    def x_copy(s, dr, q):
        return remote(
            dx.at[s % TWO, dr, pl.ds(pl.multiple_of(q * qr, SUB), qr)], rx.at[s, dr, q],
            xsend.at[s, dr, q], xrecv.at[s, dr, q], at.dev(x=left if dr else right),
        )

    def far_copy(q):
        return remote(
            dx.at[1, 1, pl.ds(pl.multiple_of(q * qr, SUB), qr)], fx.at[q], fsend.at[q], frecv.at[q], at.dev(y=at.far)
        )

    def a_load(s, q, dr):
        return local(rx.at[s - 1, dr, q], tmpa.at[q % TWO, dr], asem.at[q % TWO, dr])

    def a_pre(s, q):
        for dr in BOTH:
            x_copy(s - 1, dr, q).wait_recv()
            a_load(s, q, dr).start()

    def a_use(s, q):
        rows = pl.ds(pl.multiple_of(q * qr, SUB), qr)
        for dr in BOTH:
            a_load(s, q, dr).wait()
            dx[s % TWO, dr, rows, :] += tmpa[q % TWO, dr]

        @pl.when(s < nx - 1)
        def _():
            for dr in BOTH:
                x_copy(s, dr, q).start()

        @pl.when(s == nx - 1)
        def _():
            far_copy(q).start()

    def f_load(q):
        return local(fx.at[q], tmpa.at[q % TWO, 0], asem.at[q % TWO, 0])

    def f_out(q):
        return local(fdx.at[q % TWO], dxo.at[pl.ds(pl.multiple_of(q * qr, 16), qr)], out_sem.at[q])

    def f_pre(q):
        far_copy(q).wait_recv()
        f_load(q).start()

    def f_use(q):
        f_load(q).wait()

        @pl.when(q > 1)
        def _():
            f_out(q - 2).wait()

        rows = pl.ds(pl.multiple_of(q * qr, SUB), qr)
        fdx[q % TWO] = (dx[1, 0, rows] + tmpa[q % TWO, 0]).astype(BF16)
        f_out(q).start()

    def lot(b):
        q = (c + b) % TWO
        slices = [(b + TWO * q) % ny, (b + 1 + TWO * q) % ny]
        other = [(b + TWO * (1 - q)) % ny, (b + 1 + TWO * (1 - q)) % ny]
        home = half_of(y, b, ny) == q
        kt = jnp.where(home, y, adj(y, b))
        it = jnp.where(slices[0] == kt, 0, 1)
        return slices, other, kt, it, home

    def rows_of(k):
        return pl.ds(pl.multiple_of(k * hk, 16), hk)

    def d_copy(j, b, i):
        other = lot(b)[1]
        return remote(
            acc.at[j % TWO, rows_of(other[i]), pl.ds(b * sb, sb)], dd.at[j, b, i],
            dsend.at[j, b, i], drecv.at[j, b, i], at.dev(c=at.pc),
        )

    def d_send(j):
        for b in BOTH:
            for i in BOTH:
                d_copy(j, b, i).start()

    def r_load(j, b, i):
        return local(dd.at[j, b, i], tmpb.at[b, i], bsem.at[b, i])

    def r_pre(j):
        for b in BOTH:
            for i in BOTH:
                d_copy(j, b, i).wait_recv()
                r_load(j, b, i).start()

    def r_copy(j, b):
        slices, _, _, it, _ = lot(b)
        kg = jnp.where(it == 0, slices[1], slices[0])
        src = acc.at[j % TWO, rows_of(kg), pl.ds(b * sb, sb)]
        return remote(src, rr.at[j, b], rsend.at[j, b], rrecv.at[j, b], at.dev(y=par(y, b)))

    def r_use(j):
        for b in BOTH:
            slices, _, kt, it, _ = lot(b)
            kg = jnp.where(it == 0, slices[1], slices[0])
            for i in BOTH:
                r_load(j, b, i).wait()

            acc[j % TWO, rows_of(kg), pl.ds(b * sb, sb)] += tmpb[b, 1 - it]
            r_copy(j, b).start()
            keep[j % TWO, b] = acc[j % TWO, rows_of(kt), pl.ds(b * sb, sb)] + tmpb[b, it]

    def s_load(j, b):
        return local(rr.at[j, b], tmpb.at[b, 0], bsem.at[b, 0])

    def s_pre(j):
        for b in BOTH:
            r_copy(j, b).wait_recv()
            s_load(j, b).start()

    def o_copy(j, b):
        kt = lot(b)[2]
        f = half_of(y, b, ny)
        dst = dwo.at[:, pl.ds(pl.multiple_of(f * slot + j * sb, LANES), sb)]
        return remote(fin.at[b], dst, osend.at[j, b], orecv.at[f, j], at.dev(y=kt, c=b))

    def o_here(j, b):
        f = half_of(y, b, ny)
        dst = dwo.at[:, pl.ds(pl.multiple_of(f * slot + j * sb, LANES), sb)]
        return local(fin.at[b], dst, orecv.at[f, j])

    def is_here(b):
        return lot(b)[4] & (c == b)

    def s_use(j):
        for b in BOTH:
            s_load(j, b).wait()

            @pl.when((j > 0) & jnp.logical_not(is_here(b)))
            def _():
                o_copy(j - 1, b).wait_send()

            @pl.when((j > 0) & is_here(b))
            def _():
                o_here(j - 1, b).wait()

            fin[b] = (keep[j % TWO, b] + tmpb[b, 0]).astype(BF16)

            @pl.when(is_here(b))
            def _():
                o_here(j, b).start()

            @pl.when(jnp.logical_not(is_here(b)))
            def _():
                o_copy(j, b).start()

    def l_copy(stage, k):
        if stage == 0:
            return remote(lbuf.at[0, x], lbuf.at[0, x], lsend.at[0, k], lrecv.at[0, x], at.dev(x=(x + k) % nx))
        if stage == 1:
            return remote(lbuf.at[1, y], lbuf.at[1, y], lsend.at[1, k], lrecv.at[1, y], at.dev(y=(y + k) % ny))
        return remote(lbuf.at[2, c], lbuf.at[2, c], lsend.at[2, 0], lrecv.at[2, c], at.dev(c=at.pc))

    def l_sum(stage, size, me):
        for k in range(size):
            @pl.when(k != me)
            def _():
                remote(
                    lbuf.at[stage, k], lbuf.at[stage, k], lsend.at[stage, 0], lrecv.at[stage, k], at.dev(c=at.pc)
                ).wait_recv()

        total = lbuf[stage, 0]
        for k in range(1, size):
            total = total + lbuf[stage, k]
        return total

    def l_start():
        lbuf[0, x] = -lacc[...]
        for k in range(1, nx):
            l_copy(0, k).start()

    def l_mid():
        lbuf[1, y] = l_sum(0, nx, x)
        for k in range(1, ny):
            l_copy(1, k).start()

    def l_late():
        lbuf[2, c] = l_sum(1, ny, y)
        l_copy(2, 0).start()

    lane = lax.broadcasted_iota(jnp.int32, (min(64, tr), LANES), 1).astype(F32)

    def each_tile(n, u, buf, c0, c1, fn):
        j, r, d = tile(n, u)
        blk = min(64, tr)
        for o in range(0, tr, blk):
            rows = slice(o, o + blk)
            t = st[r * nx + d, rows, :]
            shift = jnp.broadcast_to(t[:, 0:1], (blk, LANES))
            lab = jnp.broadcast_to(t[:, 1:TWO], (blk, LANES)) - (j * ch).astype(F32)
            for e in range(c0 // LANES, c1 // LANES):
                cols = slice(LANES * e, LANES * e + LANES)
                fn(rows, cols, zb[buf, rows, cols] - shift, lane + float(LANES * e) == lab)

    def make_g(n, u, buf, c0, c1):
        def one(rows, cols, dist, hit):
            g = jnp.exp(dist)
            gb[u, rows, cols] = jnp.where(hit, g - inv, g).astype(BF16)

        each_tile(n, u, buf, c0, c1, one)

    def l_body(n, base):
        total = [jnp.zeros((SUB, LANES), F32)]

        def one(rows, cols, dist, hit):
            total[0] = total[0] + jnp.sum(jnp.where(hit, dist, 0.0).reshape(-1, SUB, LANES), axis=0)

        for u in BOTH:
            each_tile(n, u, base + u, 0, ch, one)
        lacc[...] += total[0]

    big = ch % (10 * LANES) == 0
    x_cuts = [(ch * e // 5, ch * (e + 1) // 5) for e in range(5)] if big else [(0, ch)]
    w_cuts = [(0, ch // 5), (ch // 5, ch * 3 // 5), (ch * 3 // 5, ch)] if big else [(0, ch)]

    def x_body(n, base):
        _, s, j = body_at(n)
        half = s % TWO

        @pl.when(j == 0)
        def _():
            dx[half] = jnp.zeros(dx.shape[1:], F32)

        for u in BOTH:
            for c0, c1 in x_cuts:
                make_g(n, u, base + u, c0, c1)
                dx[half, u] += lax.dot_general(
                    gb[u, :, c0:c1], w[j, :, c0:c1], (((1,), (1,)), ((), ())), preferred_element_type=F32
                )

    def w_body(n, base):
        _, j, k = body_at(n)
        half = j % TWO

        @pl.when(k == 0)
        def _():
            acc[half] = jnp.zeros(acc.shape[1:], F32)

        for c0, c1 in w_cuts:
            for u in BOTH:
                make_g(n, u, base + u, c0, c1)
            acc[half, :, c0:c1] += jnp.dot(
                xt[k], gb[:, :, c0:c1].reshape(TWO * tr, c1 - c0), preferred_element_type=F32
            )

    late = after["x3"]
    plan_a = [(after["x1"] + q, 1, q) for q in range(nq)] + [(after["x2"] + q, 2, q) for q in range(nq)]
    plan_a += [(late + 1 + 7 * q - q // 3 * 2, 3, q) for q in range(nq)]
    plan_r = [(11, 12, 0), (15, 17, 1), (24, 25, 2), (28, 30, 3), (37, 38, 4)]
    plan_s = [(18, 19, 0), (22, 23, 1), (31, 32, 2), (35, 36, 3), (late + 6, late + 7, 4)]
    pre_r, use_r = [(p, j) for p, _, j in plan_r], [(u, j) for _, u, j in plan_r]
    pre_s, use_s = [(p, j) for p, _, j in plan_s], [(u, j) for _, u, j in plan_s]
    plan_f = [(late + 11, 0), (late + 18, 1), (n_body + TWO, 2), (n_body + 4, 3)]
    n_all = n_body + 5

    def when(n, table, fn):
        table = [(e[0], e[1:]) for e in table]
        hit = functools.reduce(lambda p, q: p | q, [n == e for e, _ in table])

        @pl.when(hit)
        def _():
            args = []
            for i in range(len(table[0][1])):
                val = 0
                for e, vals in table:
                    if vals[i]:
                        val = val + jnp.where(n == e, vals[i], 0)
                args.append(val + jnp.int32(0))
            fn(*args)

    def body(n, _):
        @pl.when(n < NCH)
        def _():
            local(w_hbm.at[n], w.at[n], wsem.at[n]).wait()

        @pl.when(n == first["w0"])
        def _():
            local(xt_hbm, xt, tsem).wait()
            for q in range(nq):
                for dr in BOTH:
                    x_copy(0, dr, q).start()

        when(n, [(after["w%d" % j], j) for j in range(NCH)], d_send)
        when(n, plan_a, a_use)
        when(n, plan_f, f_use)
        when(n, use_r, r_use)
        when(n, use_s, s_use)
        when(n, [(e[0] - 1,) + e[1:] for e in plan_a], a_pre)
        when(n, [(e[0] - 1,) + e[1:] for e in plan_f], f_pre)
        when(n, pre_r, r_pre)
        when(n, pre_s, s_pre)

        for at_n, fn in ((n_body, l_start), (n_body + TWO, l_mid), (n_body + 4, l_late)):
            pl.when(n == at_n)(fn)

        @pl.when((n == first["x2"]) | (n == first["x3"]))
        def _():
            s = jnp.where(n == first["x2"], 0, 1)
            for q in range(nq):
                for dr in BOTH:
                    x_copy(s, dr, q).wait_send()

        for j in range(2, NCH):
            @pl.when(n == first["w%d" % j])
            def _():
                for b in BOTH:
                    r_copy(j - 2, b).wait_send()
                    for i in BOTH:
                        d_copy(j - 2, b, i).wait_send()

        base = (n % TWO) * 2

        @pl.when(n < n_body)
        def _():
            for u in BOTH:
                zcp(n, u, base + u).wait()

            @pl.when(n + 1 < n_body)
            def _():
                for u in BOTH:
                    zcp(n + 1, u, 2 - base + u).start()

            kind = body_at(n)[0]

            @pl.when(kind == 0)
            def _():
                x_body(n, base)

            @pl.when(kind == 1)
            def _():
                w_body(n, base)

            @pl.when(kind == TWO)
            def _():
                l_body(n, base)

        return 0

    lax.fori_loop(0, n_all, body, 0)
    loss[...] = l_sum(2, TWO, c)

    for q in range(nq):
        if q >= nq - 2:
            f_out(q).wait()
        far_copy(q).wait_send()
        for dr in BOTH:
            x_copy(2, dr, q).wait_send()
    for b in BOTH:
        for j in range(NCH - 2, NCH):
            for i in BOTH:
                d_copy(j, b, i).wait_send()
            r_copy(j, b).wait_send()

        @pl.when(is_here(b))
        def _():
            o_here(NCH - 1, b).wait()

        @pl.when(jnp.logical_not(is_here(b)))
        def _():
            o_copy(NCH - 1, b).wait_send()

    q0 = half_of(y, c, ny)
    for f in BOTH:
        kept = (f == q0) & ((q0 + c) % TWO == c)

        @pl.when(jnp.logical_not(kept))
        def _():
            for j in range(NCH):
                dst = dwo.at[:, pl.ds(f * slot + j * sb, sb)]
                remote(fin.at[0], dst, osend.at[j, 0], orecv.at[f, j], at.dev(c=at.pc)).wait_recv()

    for k in range(1, nx):
        l_copy(0, k).wait_send()
    for k in range(1, ny):
        l_copy(1, k).wait_send()
    l_copy(2, 0).wait_send()


def grads(nx, ny, inv, z, w, xt, st8, hk):
    h = w.shape[1]
    ch = w.shape[2]
    tr = z.shape[3]
    nq = 4
    shape = jax.ShapeDtypeStruct
    dma = pltpu.SemaphoreType.DMA
    vm = pltpu.VMEM
    vspec = pl.BlockSpec(memory_space=pltpu.VMEM)
    sb, qr = ch // TWO, tr // nq
    return pl.pallas_call(
        functools.partial(grads_kernel, nx, ny, inv),
        out_shape=(
            shape((tr, h), BF16), shape((hk, NCH * ch), BF16), shape((SUB, LANES), F32),
            shape((nx - 1, TWO, nq, qr, h), F32), shape((nq, qr, h), F32),
            shape((NCH, TWO, TWO, hk, sb), F32), shape((NCH, TWO, hk, sb), F32),
        ),
        in_specs=[ANY, ANY, ANY, vspec],
        out_specs=(ANY, ANY, vspec, ANY, ANY, ANY, ANY),
        scratch_shapes=[
            vm((NCH, h, ch), BF16), vm((nx, h, TWO * tr), BF16), vm((4, tr, ch), F32), vm((TWO, tr, ch), BF16),
            vm((TWO, h, ch), F32), vm((TWO, TWO, tr, h), F32), vm((TWO * nx, tr, LANES), F32), vm((SUB, LANES), F32),
            vm((TWO, TWO, qr, h), F32), vm((TWO, TWO, hk, sb), F32), vm((TWO, TWO, hk, sb), F32),
            vm((TWO, hk, sb), BF16), vm((TWO, qr, h), BF16), vm((3, max(nx, ny), SUB, LANES), F32),
            dma((NCH,)), dma, dma((4,)), dma((nx - 1, TWO, nq)), dma((nx - 1, TWO, nq)), dma((nq,)), dma((nq,)),
            dma((NCH, TWO, TWO)), dma((NCH, TWO, TWO)), dma((NCH, TWO)), dma((NCH, TWO)), dma((NCH, TWO)), dma((TWO, NCH)),
            dma((TWO, TWO)), dma((TWO, TWO)), dma((3, max(nx, ny))), dma((3, max(nx, ny))), dma((nq,)),
        ],
        compiler_params=pltpu.CompilerParams(
            collective_id=1, has_side_effects=True, vmem_limit_bytes=67_000_000
        ),
        name="grads",
    )(z, w, xt, st8)


def solution(mesh):
    ny = mesh.shape["fsdp"]
    tp_size = mesh.shape["tp"]
    nx = tp_size // TWO
    token_spec = P(("dp", "fsdp", "tp"), None)
    label_spec = P(("dp", "fsdp", "tp"))

    def local_step(hidden, w_head, labels):
        tr, h = hidden.shape
        hk, vocab = w_head.shape
        inv = 1.0 / (tr * tp_size * ny)
        vp = -(-vocab // (256 * NCH)) * (256 * NCH)
        ch = vp // NCH
        sb = ch // TWO
        slot = NCH * sb
        tp = lax.axis_index("tp")
        x, y = tp // TWO, lax.axis_index("fsdp")
        w_pad = jnp.pad(w_head, ((0, 0), (0, vp - vocab)))
        lab8 = jnp.pad(labels.reshape(-1, LANES), ((0, SUB - tr // LANES), (0, 0)))
        xg, wg, z, sta, laba, xt = gather_logits(nx, ny, vocab, hidden, w_pad, lab8)

        ms = sta[..., 0, :].reshape(TWO * nx, TWO, nx, tr)
        ss = sta[..., 1, :].reshape(TWO * nx, TWO, nx, tr)
        top = jnp.max(ms, axis=0)
        tot = jnp.sum(ss * jnp.exp(ms - top), axis=0)
        lab = laba[:, :, 0 : tr // LANES, :].reshape(2, nx, tr)
        shard, off = lab // vocab, lab % vocab
        b, f = shard % TWO, off // slot
        pos = off - f * slot
        mine = (shard // TWO == x) & (half_of(y, b, ny) == f)
        col = jnp.where(mine, (pos // sb) * ch + b * sb + pos % sb, -1)
        rows = [top + jnp.log(tot) - jnp.log(inv), col.astype(F32)]
        st8 = jnp.stack(rows + [jnp.zeros_like(top)] * 6, axis=2)
        d_hidden, d_w, loss = grads(nx, ny, inv, z, wg, xt, st8, hk)[:3]
        mean_loss = jnp.sum(loss) * inv + jnp.log(inv)
        return mean_loss.reshape(1), d_hidden, d_w[:, :vocab]

    return jax.shard_map(
        local_step,
        mesh=mesh,
        in_specs=(token_spec, P("fsdp", "tp"), label_spec),
        out_specs=(P("dp"), token_spec, P(("dp", "fsdp"), "tp")),
        check_vma=False,
    )
```

```python
import functools
import math

import jax
import jax.numpy as jnp
from jax import lax
from jax.experimental import pallas as pl
from jax.experimental.pallas import tpu as pltpu
from jax.sharding import PartitionSpec as P

MESH = pl.DeviceIdType.MESH
F32 = jnp.float32
BF16 = jnp.bfloat16
NCH = 5
LOW = -1e30
ANY = pl.BlockSpec(memory_space=pl.ANY)
LANES = 128
SUB = 8
TWO = 2
BOTH = range(TWO)
RIGHT, LEFT = True, False


class Place:
    def __init__(self, nx, ny):
        tp = lax.axis_index("tp")
        self.nx, self.ny = nx, ny
        self.x, self.c, self.y = tp // TWO, tp % TWO, lax.axis_index("fsdp")
        up, down = (self.y + 1) % ny, (self.y + ny - 1) % ny
        even = (self.y + self.c) % TWO == 0
        self.up, self.down = up, down
        self.pc = 1 - self.c
        self.p = jnp.where(even, up, down)
        self.a = jnp.where(even, down, up)
        self.far = (self.y + 2) % ny
        self.half = ((self.y - self.c + ny) % ny) // TWO

    def dev(self, x=None, y=None, c=None):
        x = self.x if x is None else x
        y = self.y if y is None else y
        c = self.c if c is None else c
        return {"fsdp": y, "tp": x * 2 + c}


def half_of(y, b, ny):
    return ((y - b + ny) % ny) // TWO


def pick(n, table):
    out = 0
    for i, v in enumerate(table):
        if v:
            out = out + jnp.where(n == i, v, 0)
    return out


def remote(src, dst, ssem, rsem, dev):
    return pltpu.make_async_remote_copy(
        src_ref=src, dst_ref=dst, send_sem=ssem, recv_sem=rsem, device_id=dev, device_id_type=MESH
    )


def local(src, dst, sem):
    return pltpu.make_async_copy(src, dst, sem)


def gather_logits_kernel(
    nx, ny, vocab,
    x_hbm, w_hbm, lab_hbm, xg, wo, z, sta, laba, xt,
    w, wsrc, xown, xb, zb, bias, m, s, stm, xtb,
    xsend, xrecv, ysend, yrecv, wsend, wrecv, dsend, drecv, ssend, srecv, lsend, lrecv, loc, wloc, xsem, zsem, tsem, wload,
):
    at = Place(nx, ny)
    x, y, c = at.x, at.y, at.c
    tr = xown.shape[0]
    hk = w_hbm.shape[1]
    sb = w.shape[1] // TWO
    slot = NCH * sb
    left, right = (x + nx - 1) % nx, (x + 1) % nx
    top, bot = pl.ds(0, tr // TWO), pl.ds(tr // TWO, tr // TWO)

    def rows_in(f, q):
        return min(sb, vocab - f * slot - q * sb)

    def w_load(f, q):
        n = rows_in(f, q)
        src = w_hbm.at[pl.ds(f * slot + q * sb, n)]
        return local(src, wsrc.at[f * NCH + q, pl.ds(0, n)], wload.at[f * NCH + q])

    def preload():
        for q in range(NCH):
            for f in BOTH:
                w_load(f, q).start()

    barrier = pltpu.get_barrier_semaphore()
    for k in range(1, nx):
        pl.semaphore_signal(barrier, inc=1, device_id=at.dev(x=(x + k) % nx), device_id_type=MESH)
    for k in range(nx):
        pl.semaphore_signal(barrier, inc=1, device_id=at.dev(x=(x + k) % nx, y=at.far), device_id_type=MESH)
    pl.semaphore_signal(barrier, inc=1, device_id=at.dev(y=at.up), device_id_type=MESH)
    pl.semaphore_signal(barrier, inc=1, device_id=at.dev(y=at.down), device_id_type=MESH)
    pl.semaphore_signal(barrier, inc=1, device_id=at.dev(c=at.pc), device_id_type=MESH)
    load_x = local(x_hbm, xown, loc.at[0])
    load_x.start()
    preload()
    pl.semaphore_wait(barrier, TWO * nx + 2)
    load_x.wait()

    def x_send(r, to_right):
        i = 0 if to_right else 1
        src = xown if r == 0 else xg.at[1, x]
        return remote(src, xg.at[r, x], xsend.at[r, i], xrecv.at[r, i], at.dev(x=right if to_right else left))

    def x_relay(r, to_right):
        if to_right:
            part = xg.at[r, left, top]
            return remote(part, part, xsend.at[r, 2], xrecv.at[r, 2], at.dev(x=right))
        part = xg.at[r, right, bot]
        return remote(part, part, xsend.at[r, 3], xrecv.at[r, 3], at.dev(x=left))

    x_far = remote(xown, xg.at[1, x], ysend, yrecv, at.dev(y=at.far))
    keep_x = local(xown, xg.at[0, x], loc.at[1])

    blocks = [(f, q) for f in BOTH for q in range(NCH)]

    def w_src(f, q):
        return wsrc.at[f * NCH + q]

    def w_dst(k, q):
        return w.at[q, pl.ds(pl.multiple_of(c * sb, SUB), sb), pl.ds(pl.multiple_of(k * hk, LANES), hk)]

    def w_own(q):
        return remote(w_src(at.half, q), w_dst(y, q), wsend.at[0, q], wrecv.at[0, q], at.dev(y=at.p))

    def w_other(q):
        return remote(w_src(1 - at.half, q), w_dst(y, q), wsend.at[1, q], wrecv.at[1, q], at.dev(y=at.a))

    def w_far(q):
        return remote(w_src(1 - at.half, q), w_dst(y, q), wsend.at[2, q], wrecv.at[2, q], at.dev(y=at.far))

    def w_core(q):
        part = w.at[q, pl.ds(pl.multiple_of(c * sb, SUB), sb)]
        return remote(part, part, dsend.at[q], drecv.at[q], at.dev(c=at.pc))

    def w_local(f, q):
        n = rows_in(f, q)
        dst = w.at[q, pl.ds(pl.multiple_of(c * sb, SUB), n), pl.ds(pl.multiple_of(y * hk, LANES), hk)]
        return local(w_hbm.at[pl.ds(f * slot + q * sb, n)], dst, wloc.at[q])

    def w_out(q):
        w_own(q).start()
        w_other(q).start()
        w_far(q).start()

    x_send(0, RIGHT).start()
    x_send(0, LEFT).start()
    for q in range(NCH):
        for f in BOTH:
            w_load(f, q).wait()
            if rows_in(f, q) < sb:
                pad = sb - rows_in(f, q)
                wsrc[f * NCH + q, sb - pad :, :] = jnp.zeros((pad, hk), BF16)
        w_out(q)
        if q == 0:
            x_far.start()
    keep_x.start()
    for f, q in blocks:
        @pl.when(at.half == f)
        def _():
            w_local(f, q).start()
            if rows_in(f, q) < sb:
                pad = sb - rows_in(f, q)
                at_row = pl.multiple_of(c * sb + sb - pad, SUB)
                w[q, pl.ds(at_row, pad), pl.ds(pl.multiple_of(y * hk, LANES), hk)] = jnp.zeros((pad, hk), BF16)

    peers = [(0, k) for k in range(1, nx)] + [(1, k) for k in range(nx)]

    def lab_copy(i):
        sy, k = peers[i]
        return remote(
            lab_hbm, laba.at[sy, x], lsend.at[i], lrecv.at[sy, x],
            at.dev(x=(x + k) % nx, y=at.far if sy else y),
        )

    for i in range(len(peers)):
        lab_copy(i).start()
    lab_own = local(lab_hbm, laba.at[0, x], loc.at[2])
    lab_own.start()

    tail = lax.broadcasted_iota(jnp.int32, bias.shape[1:], 1)
    slot_of = tail // LANES
    pos = slot - LANES + tail - slot_of * LANES
    half_b = jnp.where(slot_of == 0, half_of(y, 0, ny), half_of(y, 1, ny))
    bias[...] = jnp.zeros_like(bias)
    bias[NCH - 1] = jnp.where((half_b == 1) & (pos >= vocab - slot), LOW, 0.0)
    m[...] = jnp.full_like(m, -3e38)
    s[...] = jnp.zeros_like(s)

    def xt_out(run, u):
        return local(
            xtb.at[u], xt.at[run // TWO, :, pl.ds(pl.multiple_of((run % TWO) * tr, LANES), tr)], tsem.at[u]
        )

    keep_x.wait()
    x_send(0, RIGHT).wait_recv()
    x_relay(0, RIGHT).start()
    x_send(0, LEFT).wait_recv()
    x_relay(0, LEFT).start()

    n_steps = TWO * nx * NCH

    near = (0, 3, 1, 2)
    order = [(0, k, 0) for k in near] + [(1, 0, 0)]
    order += [(0, k, 1) for k in near] + [(1, 0, 1)]
    order += [(1, k, j) for j in BOTH for k in (3, 1)]
    order += [(0, k, 2) for k in near] + [(1, k, 2) for k in (0, 3, 1)] + [(1, 2, j) for j in range(3)]
    order += [(r, k, j) for j in (3, 4) for r in BOTH for k in near]
    codes = [(r * 4 + k) * 8 + j for r, k, j in order]

    def code_of(t):
        return tuple(pick(t, codes[u::TWO]) for u in BOTH)

    def place_of(code):
        run = code // 8
        return run // 4, code % 8, (x + run % 4) % nx

    def xcp(i, u):
        r, j, k = place_of(i)
        return local(xg.at[r, k], xb.at[u], xsem.at[u])

    def zcp(i, u):
        r, j, k = place_of(i)
        return local(zb.at[u], z.at[j, r, k], zsem.at[u])

    def step(i, u):
        r, j, k = place_of(i)
        run = r * nx + k
        c0 = 0
        for width in (sb * 4 // 5, TWO * sb - sb * 4 // 5) if sb % 640 == 0 else (2 * sb,):
            cols = slice(c0, c0 + width)
            zz = lax.dot_general(xb[u], w[j, cols, :], (((1,), (1,)), ((), ())), preferred_element_type=F32)
            zb[u, :, cols] = zz
            blk = min(64, tr)
            for o in range(0, tr, blk):
                rows = slice(o, o + blk)
                m_old = m[run, rows, :]
                parts = [zz[rows, LANES * e : LANES * e + LANES] for e in range(width // LANES)]
                for e in range(width // LANES):
                    at_e = slice(c0 + LANES * e, c0 + LANES * e + LANES)
                    if at_e.stop % sb == 0:
                        end = at_e.stop // sb
                        parts[e] = parts[e] + bias[j, 0:1, LANES * end - LANES : LANES * end]
                        zb[u, rows, at_e] = parts[e]
                mx = m_old
                for part in parts:
                    mx = jnp.maximum(mx, part)
                acc = s[run, rows, :] * jnp.exp(m_old - mx)
                for part in parts:
                    acc = acc + jnp.exp(part - mx)
                m[run, rows, :] = mx
                s[run, rows, :] = acc
            c0 += width

    def stat_copy(r, i):
        sy, k = peers[i]
        rr = 1 - r if sy else r
        return remote(
            stm.at[r], sta.at[sy, x, rr], ssend.at[r, i], srecv.at[sy, x, rr],
            at.dev(x=(x + k) % nx, y=at.far if sy else y),
        )

    def stat_own(r):
        return local(stm.at[r], sta.at[0, x, r], loc.at[3 + r])

    def finish_stats(r):
        lane = lax.broadcasted_iota(jnp.int32, m.shape[1:], 1)
        blk = jnp.zeros(m.shape[1:], F32)
        for d in range(nx):
            mm = m[r * nx + d]
            top_m = jnp.max(mm, axis=1, keepdims=True)
            tot = jnp.sum(s[r * nx + d] * jnp.exp(mm - top_m), axis=1, keepdims=True)
            blk = jnp.where(lane == d, top_m, jnp.where(lane == nx + d, tot, blk))
        stm[r] = blk.T[0:SUB, :]
        for i in range(len(peers)):
            stat_copy(r, i).start()
        stat_own(r).start()

    def w_here(j):
        for f in BOTH:
            pl.when(at.half == f)(w_local(f, j).wait)

        w_own(j).wait_recv()
        w_other(j).wait_recv()
        w_far(j).wait_recv()
        w_core(j).start()

    here_at = (0, 2, 6, 11, 15)
    both_at = (0, 2, 7, 12, 16)

    def body(t, held):
        older, old, now = held
        later = code_of(t + 1)

        @pl.when(t == 0)
        def _():
            for u in BOTH:
                xcp(now[u], u).start()
            x_relay(0, RIGHT).wait_recv()
            x_relay(0, LEFT).wait_recv()

        for j in range(NCH):
            pl.when(t == here_at[j])(functools.partial(w_here, j))
            pl.when(t == both_at[j])(w_core(j).wait_recv)

        @pl.when(t == 1)
        def _():
            x_far.wait_recv()
            x_send(1, RIGHT).start()
            x_send(1, LEFT).start()

        @pl.when(t == 4)
        def _():
            x_send(1, RIGHT).wait_recv()
            x_relay(1, RIGHT).start()
            x_send(1, LEFT).wait_recv()
            x_relay(1, LEFT).start()

        @pl.when(t == 9)
        def _():
            x_relay(1, RIGHT).wait_recv()
            x_relay(1, LEFT).wait_recv()

        @pl.when(t == 16)
        def _():
            local(w, wo, loc.at[5]).start()

        @pl.when(t == 18)
        def _():
            finish_stats(0)

        base = (t % TWO) * 2
        for u in BOTH:
            xcp(now[u], base + u).wait()

        for u in BOTH:
            r, j, k = place_of(now[u])

            @pl.when(j == 0)
            def _():
                cp = xt_out(r * nx + k, u)
                xtb[u] = xb[base + u].T
                cp.start()

        @pl.when(TWO * t + 2 < n_steps)
        def _():
            for u in BOTH:
                xcp(later[u], 2 - base + u).start()

        @pl.when(t > 1)
        def _():
            for u in BOTH:
                zcp(older[u], base + u).wait()

        for u in BOTH:
            step(now[u], base + u)
        for u in BOTH:
            zcp(now[u], base + u).start()
            r, j, k = place_of(now[u])

            @pl.when(j == 0)
            def _():
                xt_out(r * nx + k, u).wait()

        return old, now, later

    none = (jnp.int32(0),) * TWO
    older, old, _ = lax.fori_loop(0, n_steps // TWO, body, (none, none, code_of(jnp.int32(0))))
    finish_stats(1)
    for u in BOTH:
        zcp(older[u], u).wait()
        zcp(old[u], TWO + u).wait()
    local(w, wo, loc.at[5]).wait()
    lab_own.wait()
    stat_own(0).wait()
    stat_own(1).wait()
    for r in BOTH:
        for right_way in (RIGHT, LEFT):
            x_send(r, right_way).wait_send()
            x_relay(r, right_way).wait_send()
    x_far.wait_send()
    for q in range(NCH):
        w_own(q).wait_send()
        w_other(q).wait_send()
        w_far(q).wait_send()
        w_core(q).wait_send()
    for i in range(len(peers)):
        lab_copy(i).wait_send()
        stat_copy(0, i).wait_send()
        stat_copy(1, i).wait_send()
    for sy in BOTH:
        for k in range(nx):
            def arrived():
                remote(lab_hbm, laba.at[sy, k], lsend.at[0], lrecv.at[sy, k], at.dev(c=at.pc)).wait_recv()
                for rr in BOTH:
                    remote(stm.at[rr], sta.at[sy, k, rr], ssend.at[0, 0], srecv.at[sy, k, rr], at.dev(c=at.pc)).wait_recv()

            if sy == 0:
                pl.when(k != x)(arrived)
            else:
                arrived()


def gather_logits(nx, ny, vocab, x, w, lab):
    tr, h = x.shape
    hk = w.shape[1]
    vp = -(-vocab // (TWO * LANES * NCH)) * TWO * LANES * NCH
    ch = vp // NCH
    shape = jax.ShapeDtypeStruct
    dma = pltpu.SemaphoreType.DMA
    vm = pltpu.VMEM
    flops = TWO * TWO * nx * tr * h * vp
    return pl.pallas_call(
        functools.partial(gather_logits_kernel, nx, ny, vocab),
        out_shape=(
            shape((TWO, nx, tr, h), BF16),
            shape((NCH, ch, h), BF16),
            shape((NCH, TWO, nx, tr, ch), F32),
            shape((TWO, nx, TWO, SUB, tr), F32),
            shape((TWO, nx) + lab.shape, jnp.int32),
            shape((nx, h, TWO * tr), BF16),
        ),
        in_specs=[ANY] * 3,
        out_specs=(ANY,) * 6,
        scratch_shapes=[
            vm((NCH, ch, h), BF16), vm((TWO * NCH, ch // TWO, hk), BF16), vm((tr, h), BF16),
            vm((4, tr, h), BF16), vm((4, tr, ch), F32), vm((NCH, SUB, TWO * LANES), F32),
            vm((TWO * nx, tr, LANES), F32), vm((TWO * nx, tr, LANES), F32), vm((TWO, SUB, tr), F32), vm((TWO, h, tr), BF16),
            dma((TWO, 4)), dma((TWO, 4)), dma, dma, dma((3, NCH)), dma((3, NCH)), dma((NCH,)), dma((NCH,)),
            dma((TWO, TWO * nx - 1)), dma((TWO, nx, TWO)), dma((TWO * nx - 1,)), dma((TWO, nx)),
            dma((6,)), dma((NCH,)), dma((4,)), dma((4,)), dma((TWO,)), dma((TWO * NCH,)),
        ],
        compiler_params=pltpu.CompilerParams(
            collective_id=0, has_side_effects=True, vmem_limit_bytes=60 * 2**20
        ),
        cost_estimate=pl.CostEstimate(flops=flops, bytes_accessed=4 * TWO * nx * tr * vp, transcendentals=0),
        name="gather_logits",
    )(x, w, lab)


def grads_kernel(
    nx, ny, inv, vocab, z, w_hbm, xt_hbm, sta_hbm, lab_hbm, dxo, dwo, loss, rx, fx, dd, rr,
    w, xt, zb, gb, acc, dx, st, sta, laba, lacc, tmpa, tmpb, keep, fin, fdx, lbuf,
    wsem, tsem, zsem, xsend, xrecv, fsend, frecv, dsend, drecv, rsend, rrecv, osend, orecv, asem, bsem, lsend, lrecv,
    out_sem, ssem,
):
    at = Place(nx, ny)
    x, y, c = at.x, at.y, at.c
    tr, h = dxo.shape
    ch = zb.shape[2]
    sb = ch // TWO
    slot = NCH * sb
    hk = dwo.shape[1]
    nq = rx.shape[2]
    qr = tr // nq
    left, right = (x + nx - 1) % nx, (x + 1) % nx

    def par(yy, b):
        return jnp.where((yy + b) % TWO == 0, (yy + 1) % ny, (yy + ny - 1) % ny)

    def adj(yy, b):
        return jnp.where((yy + b) % TWO == 0, (yy + ny - 1) % ny, (yy + 1) % ny)

    stats = [local(sta_hbm, sta, ssem.at[0]), local(lab_hbm, laba, ssem.at[1])]
    for cp in stats:
        cp.start()
    local(w_hbm.at[0], w.at[0], wsem.at[0]).start()
    barrier = pltpu.get_barrier_semaphore()
    for k in range(1, nx):
        pl.semaphore_signal(barrier, inc=1, device_id=at.dev(x=(x + k) % nx), device_id_type=MESH)
    for k in range(1, ny):
        pl.semaphore_signal(barrier, inc=1, device_id=at.dev(y=(y + k) % ny), device_id_type=MESH)
        pl.semaphore_signal(barrier, inc=1, device_id=at.dev(y=(y + k) % ny, c=at.pc), device_id_type=MESH)
    pl.semaphore_signal(barrier, inc=1, device_id=at.dev(c=at.pc), device_id_type=MESH)

    segments = ["x0", "w0", "w1", "x1", "w2", "w3", "x2", "w4", "x3"]
    first, after, n_body = {}, {}, 0
    for seg in segments:
        first[seg] = n_body
        n_body += NCH if seg.startswith("x") else nx
        after[seg] = n_body

    def body_at(n):
        code, start = 0, 0
        for seg in segments[1:]:
            here = n >= first[seg]
            code = jnp.where(here, int(seg.startswith("w")) * 8 + int(seg[-1]), code)
            start = jnp.where(here, first[seg], start)
        return code // 8, code % 8, n - start

    def tile(n, u):
        kind, i, k = body_at(n)
        mine = jnp.where(u == 0, (x + TWO * nx - 1 - i) % nx, (x + 1 + i) % nx)
        run = TWO * k + u
        is_x = kind == 0
        return jnp.where(is_x, k, i), jnp.where(is_x, u, run // nx), jnp.where(is_x, mine, run % nx)

    def zcp(n, u, buf):
        j, r, d = tile(n, u)
        return local(z.at[j, r, d], zb.at[buf], zsem.at[buf])

    for u in BOTH:
        zcp(0, u, u).start()
    for j in range(1, NCH):
        local(w_hbm.at[j], w.at[j], wsem.at[j]).start()
    local(xt_hbm, xt, tsem).start()

    for cp in stats:
        cp.wait()
    for r in BOTH:
        parts = [sta[sy, k, r] for sy in BOTH for k in range(nx)]
        top = functools.reduce(jnp.maximum, [part[0:nx] for part in parts])
        tot = sum(part[nx : TWO * nx] * jnp.exp(part[0:nx] - top) for part in parts)
        shift = top + jnp.log(tot) - math.log(inv)
        for d in range(nx):
            col = jnp.full(laba.shape[TWO:], -1, jnp.int32)
            for b in BOTH:
                base = (x * TWO + b) * vocab + half_of(y, b, ny) * slot
                pos = laba[r, d] - base
                room = jnp.where(half_of(y, b, ny) == 0, slot, vocab - slot)
                chunk = sum((pos >= q * sb).astype(jnp.int32) for q in range(1, NCH))
                col = jnp.where((pos >= 0) & (pos < room), chunk * ch + b * sb + pos - chunk * sb, col)
            line = jnp.concatenate([col[o : o + 1].astype(F32) for o in range(tr // LANES)], axis=1)
            rows = jnp.concatenate([shift[d : d + 1], line, jnp.zeros((SUB - TWO, tr), F32)], axis=0)
            st[r * nx + d] = jnp.concatenate([rows] * 16, axis=0).T
    lacc[...] = jnp.zeros_like(lacc)
    pl.semaphore_wait(barrier, nx - 1 + TWO * (ny - 1) + 1)

    def x_copy(s, dr, q):
        return remote(
            dx.at[s % TWO, dr, pl.ds(pl.multiple_of(q * qr, SUB), qr)], rx.at[s, dr, q],
            xsend.at[s, dr, q], xrecv.at[s, dr, q], at.dev(x=left if dr else right),
        )

    def far_copy(q):
        return remote(
            dx.at[1, 1, pl.ds(pl.multiple_of(q * qr, SUB), qr)], fx.at[q], fsend.at[q], frecv.at[q], at.dev(y=at.far)
        )

    def a_load(s, q, dr):
        return local(rx.at[s - 1, dr, q], tmpa.at[q % TWO, dr], asem.at[q % TWO, dr])

    def a_pre(s, q):
        for dr in BOTH:
            x_copy(s - 1, dr, q).wait_recv()
            a_load(s, q, dr).start()

    def a_use(s, q):
        rows = pl.ds(pl.multiple_of(q * qr, SUB), qr)
        for dr in BOTH:
            a_load(s, q, dr).wait()
            dx[s % TWO, dr, rows, :] += tmpa[q % TWO, dr]

        @pl.when(s < nx - 1)
        def _():
            for dr in BOTH:
                x_copy(s, dr, q).start()

        @pl.when(s == nx - 1)
        def _():
            far_copy(q).start()

    def f_load(q):
        return local(fx.at[q], tmpa.at[q % TWO, 0], asem.at[q % TWO, 0])

    def f_out(q):
        return local(fdx.at[q % TWO], dxo.at[pl.ds(pl.multiple_of(q * qr, 16), qr)], out_sem.at[q])

    def f_pre(q):
        far_copy(q).wait_recv()
        f_load(q).start()

    def f_use(q):
        f_load(q).wait()

        @pl.when(q > 1)
        def _():
            f_out(q - 2).wait()

        rows = pl.ds(pl.multiple_of(q * qr, SUB), qr)
        fdx[q % TWO] = (dx[1, 0, rows] + tmpa[q % TWO, 0]).astype(BF16)
        f_out(q).start()

    def lot(b):
        q = (c + b) % TWO
        slices = [(b + TWO * q) % ny, (b + 1 + TWO * q) % ny]
        other = [(b + TWO * (1 - q)) % ny, (b + 1 + TWO * (1 - q)) % ny]
        home = half_of(y, b, ny) == q
        kt = jnp.where(home, y, adj(y, b))
        it = jnp.where(slices[0] == kt, 0, 1)
        return slices, other, kt, it, home

    def rows_of(k):
        return pl.ds(pl.multiple_of(k * hk, 16), hk)

    def d_copy(j, b, i):
        other = lot(b)[1]
        return remote(
            acc.at[j % TWO, rows_of(other[i]), pl.ds(b * sb, sb)], dd.at[j, b, i],
            dsend.at[j, b, i], drecv.at[j, b, i], at.dev(c=at.pc),
        )

    def d_send(j):
        for b in BOTH:
            for i in BOTH:
                d_copy(j, b, i).start()

    def r_load(j, b, i):
        return local(dd.at[j, b, i], tmpb.at[b, i], bsem.at[b, i])

    def r_pre(j):
        for b in BOTH:
            for i in BOTH:
                d_copy(j, b, i).wait_recv()
                r_load(j, b, i).start()

    def r_copy(j, b):
        slices, _, _, it, _ = lot(b)
        kg = jnp.where(it == 0, slices[1], slices[0])
        src = acc.at[j % TWO, rows_of(kg), pl.ds(b * sb, sb)]
        return remote(src, rr.at[j, b], rsend.at[j, b], rrecv.at[j, b], at.dev(y=par(y, b)))

    def r_use(j):
        for b in BOTH:
            slices, _, kt, it, _ = lot(b)
            kg = jnp.where(it == 0, slices[1], slices[0])
            for i in BOTH:
                r_load(j, b, i).wait()

            acc[j % TWO, rows_of(kg), pl.ds(b * sb, sb)] += tmpb[b, 1 - it]
            r_copy(j, b).start()
            keep[j % TWO, b] = acc[j % TWO, rows_of(kt), pl.ds(b * sb, sb)] + tmpb[b, it]

    def s_load(j, b):
        return local(rr.at[j, b], tmpb.at[b, 0], bsem.at[b, 0])

    def s_pre(j):
        for b in BOTH:
            r_copy(j, b).wait_recv()
            s_load(j, b).start()

    def o_copy(j, b):
        kt = lot(b)[2]
        f = half_of(y, b, ny)
        dst = dwo.at[pl.ds(pl.multiple_of(f * slot + j * sb, SUB), sb)]
        return remote(fin.at[b], dst, osend.at[j, b], orecv.at[f, j], at.dev(y=kt, c=b))

    def o_here(j, b):
        f = half_of(y, b, ny)
        dst = dwo.at[pl.ds(pl.multiple_of(f * slot + j * sb, SUB), sb)]
        return local(fin.at[b], dst, orecv.at[f, j])

    def is_here(b):
        return lot(b)[4] & (c == b)

    def s_use(j):
        for b in BOTH:
            s_load(j, b).wait()

            @pl.when((j > 0) & jnp.logical_not(is_here(b)))
            def _():
                o_copy(j - 1, b).wait_send()

            @pl.when((j > 0) & is_here(b))
            def _():
                o_here(j - 1, b).wait()

            fin[b] = (keep[j % TWO, b] + tmpb[b, 0]).T.astype(BF16)

            @pl.when(is_here(b))
            def _():
                o_here(j, b).start()

            @pl.when(jnp.logical_not(is_here(b)))
            def _():
                o_copy(j, b).start()

    def l_copy(stage, k):
        if stage == 0:
            return remote(lbuf.at[0, x], lbuf.at[0, x], lsend.at[0, k], lrecv.at[0, x], at.dev(x=(x + k) % nx))
        if stage == 1:
            return remote(lbuf.at[1, y], lbuf.at[1, y], lsend.at[1, k], lrecv.at[1, y], at.dev(y=(y + k) % ny))
        return remote(lbuf.at[2, c], lbuf.at[2, c], lsend.at[2, 0], lrecv.at[2, c], at.dev(c=at.pc))

    def l_sum(stage, size, me):
        for k in range(size):
            @pl.when(k != me)
            def _():
                remote(
                    lbuf.at[stage, k], lbuf.at[stage, k], lsend.at[stage, 0], lrecv.at[stage, k], at.dev(c=at.pc)
                ).wait_recv()

        total = lbuf[stage, 0]
        for k in range(1, size):
            total = total + lbuf[stage, k]
        return total

    def l_start():
        lbuf[0, x] = -lacc[...]
        for k in range(1, nx):
            l_copy(0, k).start()

    def l_mid():
        lbuf[1, y] = l_sum(0, nx, x)
        for k in range(1, ny):
            l_copy(1, k).start()

    def l_late():
        lbuf[2, c] = l_sum(1, ny, y)
        l_copy(2, 0).start()

    lane = lax.broadcasted_iota(jnp.int32, (min(64, tr), LANES), 1).astype(F32)

    def each_tile(n, u, buf, c0, c1, fn):
        j, r, d = tile(n, u)
        blk = min(64, tr)
        for o in range(0, tr, blk):
            rows = slice(o, o + blk)
            t = st[r * nx + d, rows, :]
            shift = jnp.broadcast_to(t[:, 0:1], (blk, LANES))
            lab = jnp.broadcast_to(t[:, 1:TWO], (blk, LANES)) - (j * ch).astype(F32)
            for e in range(c0 // LANES, c1 // LANES):
                cols = slice(LANES * e, LANES * e + LANES)
                fn(rows, cols, zb[buf, rows, cols] - shift, lane + float(LANES * e) == lab)

    def make_g(n, u, buf, c0, c1, loss_sum=None):
        def one(rows, cols, dist, hit):
            g = jnp.exp(dist)
            gb[u, rows, cols] = jnp.where(hit, g - inv, g).astype(BF16)
            if loss_sum is not None:
                loss_sum.append(jnp.where(hit, dist, 0.0) + (loss_sum.pop() if loss_sum else 0.0))

        each_tile(n, u, buf, c0, c1, one)

    big = ch % (10 * LANES) == 0
    x_cuts = [(ch * e // 5, ch * (e + 1) // 5) for e in range(5)] if big else [(0, ch)]
    w_cuts = [(0, ch // 5), (ch // 5, ch * 3 // 5), (ch * 3 // 5, ch)] if big else [(0, ch)]

    def x_body(n, base):
        _, s, j = body_at(n)
        half = s % TWO

        @pl.when(j == 0)
        def _():
            dx[half] = jnp.zeros(dx.shape[1:], F32)

        for u in BOTH:
            for c0, c1 in x_cuts:
                loss_sum = []
                make_g(n, u, base + u, c0, c1, loss_sum)
                lacc[...] += jnp.sum(loss_sum[0].reshape(-1, SUB, LANES), axis=0)
                dx[half, u] += lax.dot_general(
                    gb[u, :, c0:c1], w[j, c0:c1, :], (((1,), (0,)), ((), ())), preferred_element_type=F32
                )

    def w_body(n, base):
        _, j, k = body_at(n)
        half = j % TWO

        @pl.when(k == 0)
        def _():
            acc[half] = jnp.zeros(acc.shape[1:], F32)

        for c0, c1 in w_cuts:
            for u in BOTH:
                make_g(n, u, base + u, c0, c1)
            acc[half, :, c0:c1] += jnp.dot(
                xt[k], gb[:, :, c0:c1].reshape(TWO * tr, c1 - c0), preferred_element_type=F32
            )

    plan_a = [(after["x1"] + q, 1, q) for q in range(nq)]
    plan_a += [(after["x2"] + q + q // 3 * 2, 2, q) for q in range(nq)] + [(n_body + q, 3, q) for q in range(nq)]
    plan_r = [(11, 12, 0), (15, 17, 1), (24, 25, 2), (28, 30, 3), (37, 38, 4)]
    plan_s = [(18, 19, 0), (23, 24, 1), (31, 32, 2), (36, 37, 3), (n_body + 1, n_body + 2, 4)]
    pre_r, use_r = [(p, j) for p, _, j in plan_r], [(u, j) for _, u, j in plan_r]
    pre_s, use_s = [(p, j) for p, _, j in plan_s], [(u, j) for _, u, j in plan_s]
    plan_f = [(n_body + nq + q, q) for q in range(nq)]
    n_all = n_body + TWO * nq

    def when(n, table, fn):
        table = [(e[0], e[1:]) for e in table]
        hit = functools.reduce(lambda p, q: p | q, [n == e for e, _ in table])

        @pl.when(hit)
        def _():
            args = []
            for i in range(len(table[0][1])):
                val = 0
                for e, vals in table:
                    if vals[i]:
                        val = val + jnp.where(n == e, vals[i], 0)
                args.append(val + jnp.int32(0))
            fn(*args)

    def body(n, _):
        @pl.when(n < NCH)
        def _():
            local(w_hbm.at[n], w.at[n], wsem.at[n]).wait()

        @pl.when(n == first["w0"])
        def _():
            local(xt_hbm, xt, tsem).wait()
            for q in range(nq):
                for dr in BOTH:
                    x_copy(0, dr, q).start()

        when(n, [(after["w%d" % j], j) for j in range(NCH)], d_send)
        when(n, plan_a, a_use)
        when(n, plan_f, f_use)
        when(n, use_r, r_use)
        when(n, use_s, s_use)
        when(n, [(e[0] - 1,) + e[1:] for e in plan_a], a_pre)
        when(n, [(e[0] - 1,) + e[1:] for e in plan_f], f_pre)
        when(n, pre_r, r_pre)
        when(n, pre_s, s_pre)

        for at_n, fn in ((n_body, l_start), (n_body + TWO, l_mid), (n_body + nq, l_late)):
            pl.when(n == at_n)(fn)

        @pl.when((n == first["x2"]) | (n == first["x3"]))
        def _():
            s = jnp.where(n == first["x2"], 0, 1)
            for q in range(nq):
                for dr in BOTH:
                    x_copy(s, dr, q).wait_send()

        for j in range(2, NCH):
            @pl.when(n == first["w%d" % j])
            def _():
                for b in BOTH:
                    r_copy(j - 2, b).wait_send()
                    for i in BOTH:
                        d_copy(j - 2, b, i).wait_send()

        base = (n % TWO) * 2

        @pl.when(n < n_body)
        def _():
            for u in BOTH:
                zcp(n, u, base + u).wait()

            @pl.when(n + 1 < n_body)
            def _():
                for u in BOTH:
                    zcp(n + 1, u, 2 - base + u).start()

            kind = body_at(n)[0]

            @pl.when(kind == 0)
            def _():
                x_body(n, base)

            @pl.when(kind == 1)
            def _():
                w_body(n, base)

        return 0

    lax.fori_loop(0, n_all, body, 0)
    loss[...] = l_sum(2, TWO, c)

    for q in range(nq):
        if q >= nq - 2:
            f_out(q).wait()
        far_copy(q).wait_send()
        for dr in BOTH:
            x_copy(2, dr, q).wait_send()
    for b in BOTH:
        for j in range(NCH - 2, NCH):
            for i in BOTH:
                d_copy(j, b, i).wait_send()
            r_copy(j, b).wait_send()

        @pl.when(is_here(b))
        def _():
            o_here(NCH - 1, b).wait()

        @pl.when(jnp.logical_not(is_here(b)))
        def _():
            o_copy(NCH - 1, b).wait_send()

    q0 = half_of(y, c, ny)
    for f in BOTH:
        kept = (f == q0) & ((q0 + c) % TWO == c)

        @pl.when(jnp.logical_not(kept))
        def _():
            for j in range(NCH):
                dst = dwo.at[pl.ds(f * slot + j * sb, sb)]
                remote(fin.at[0], dst, osend.at[j, 0], orecv.at[f, j], at.dev(c=at.pc)).wait_recv()

    for k in range(1, nx):
        l_copy(0, k).wait_send()
    for k in range(1, ny):
        l_copy(1, k).wait_send()
    l_copy(2, 0).wait_send()


def grads(nx, ny, inv, vocab, z, w, xt, sta, laba, hk):
    ch, h = w.shape[1:]
    tr = z.shape[3]
    nq = 4
    shape = jax.ShapeDtypeStruct
    dma = pltpu.SemaphoreType.DMA
    vm = pltpu.VMEM
    vspec = pl.BlockSpec(memory_space=pltpu.VMEM)
    sb, qr = ch // TWO, tr // nq
    return pl.pallas_call(
        functools.partial(grads_kernel, nx, ny, inv, vocab),
        out_shape=(
            shape((tr, h), BF16), shape((NCH * ch, hk), BF16), shape((SUB, LANES), F32),
            shape((nx - 1, TWO, nq, qr, h), F32), shape((nq, qr, h), F32),
            shape((NCH, TWO, TWO, hk, sb), F32), shape((NCH, TWO, hk, sb), F32),
        ),
        in_specs=[ANY] * 5,
        out_specs=(ANY, ANY, vspec, ANY, ANY, ANY, ANY),
        scratch_shapes=[
            vm((NCH, ch, h), BF16), vm((nx, h, TWO * tr), BF16), vm((4, tr, ch), F32), vm((TWO, tr, ch), BF16),
            vm((TWO, h, ch), F32), vm((TWO, TWO, tr, h), F32), vm((TWO * nx, tr, LANES), F32), vm(sta.shape, F32), vm(laba.shape, jnp.int32), vm((SUB, LANES), F32),
            vm((TWO, TWO, qr, h), F32), vm((TWO, TWO, hk, sb), F32), vm((TWO, TWO, hk, sb), F32),
            vm((TWO, sb, hk), BF16), vm((TWO, qr, h), BF16), vm((3, max(nx, ny), SUB, LANES), F32),
            dma((NCH,)), dma, dma((4,)), dma((nx - 1, TWO, nq)), dma((nx - 1, TWO, nq)), dma((nq,)), dma((nq,)),
            dma((NCH, TWO, TWO)), dma((NCH, TWO, TWO)), dma((NCH, TWO)), dma((NCH, TWO)), dma((NCH, TWO)), dma((TWO, NCH)),
            dma((TWO, TWO)), dma((TWO, TWO)), dma((3, max(nx, ny))), dma((3, max(nx, ny))), dma((nq,)), dma((TWO,)),
        ],
        compiler_params=pltpu.CompilerParams(
            collective_id=1, has_side_effects=True, vmem_limit_bytes=67_000_000
        ),
        name="grads",
    )(z, w, xt, sta, laba)


def solution(mesh):
    ny = mesh.shape["fsdp"]
    tp_size = mesh.shape["tp"]
    nx = tp_size // TWO
    token_spec = P(("dp", "fsdp", "tp"), None)
    label_spec = P(("dp", "fsdp", "tp"))

    def local_step(hidden, w_head, labels):
        tr, h = hidden.shape
        hk, vocab = w_head.shape
        inv = 1.0 / (tr * tp_size * ny)
        lab = labels.reshape(-1, LANES)
        xg, wg, z, sta, laba, xt = gather_logits(nx, ny, vocab, hidden, w_head.T, lab)
        d_hidden, d_w, loss = grads(nx, ny, inv, vocab, z, wg, xt, sta, laba, hk)[:3]
        mean_loss = jnp.sum(loss) * inv + math.log(inv)
        return mean_loss.reshape(1), d_hidden, d_w[:vocab].T

    return jax.shard_map(
        local_step,
        mesh=mesh,
        in_specs=(token_spec, P("fsdp", "tp"), label_spec),
        out_specs=(P("dp"), token_spec, P(("dp", "fsdp"), "tp")),
        check_vma=False,
    )
```

```python
import functools
import math

import jax
import jax.numpy as jnp
from jax import lax
from jax.experimental import pallas as pl
from jax.experimental.pallas import tpu as pltpu
from jax.sharding import PartitionSpec as P

MESH = pl.DeviceIdType.MESH
F32 = jnp.float32
BF16 = jnp.bfloat16
NCH = 5
LOW = -1e30
ANY = pl.BlockSpec(memory_space=pl.ANY)
LANES = 128
SUB = 8
TWO = 2
BOTH = range(TWO)
RIGHT, LEFT = True, False


class Place:
    def __init__(self, nx, ny):
        tp = lax.axis_index("tp")
        self.nx, self.ny = nx, ny
        self.x, self.c, self.y = tp // TWO, tp % TWO, lax.axis_index("fsdp")
        up, down = (self.y + 1) % ny, (self.y + ny - 1) % ny
        even = (self.y + self.c) % TWO == 0
        self.up, self.down = up, down
        self.pc = 1 - self.c
        self.p = jnp.where(even, up, down)
        self.a = jnp.where(even, down, up)
        self.far = (self.y + 2) % ny
        self.half = ((self.y - self.c + ny) % ny) // TWO

    def dev(self, x=None, y=None, c=None):
        x = self.x if x is None else x
        y = self.y if y is None else y
        c = self.c if c is None else c
        return {"fsdp": y, "tp": x * 2 + c}


def half_of(y, b, ny):
    return ((y - b + ny) % ny) // TWO


def pick(n, table):
    out = 0
    for i, v in enumerate(table):
        if v:
            out = out + jnp.where(n == i, v, 0)
    return out


def remote(src, dst, ssem, rsem, dev):
    return pltpu.make_async_remote_copy(
        src_ref=src, dst_ref=dst, send_sem=ssem, recv_sem=rsem, device_id=dev, device_id_type=MESH
    )


def local(src, dst, sem):
    return pltpu.make_async_copy(src, dst, sem)


def gather_logits_kernel(
    nx, ny, vocab,
    x_hbm, w_hbm, lab_hbm, xg, wo, z, sta, laba, xt,
    w, wsrc, xown, xb, zb, bias, m, s, stm, xtb,
    xsend, xrecv, ysend, yrecv, wsend, wrecv, dsend, drecv, ssend, srecv, lsend, lrecv, loc, wloc, xsem, zsem, tsem, wload,
):
    at = Place(nx, ny)
    x, y, c = at.x, at.y, at.c
    tr = xown.shape[0]
    hk = w_hbm.shape[1]
    sb = w.shape[1] // TWO
    slot = NCH * sb
    left, right = (x + nx - 1) % nx, (x + 1) % nx
    top, bot = pl.ds(0, tr // TWO), pl.ds(tr // TWO, tr // TWO)

    def rows_in(f, q):
        return min(sb, vocab - f * slot - q * sb)

    def w_load(f, q):
        n = rows_in(f, q)
        src = w_hbm.at[pl.ds(f * slot + q * sb, n)]
        return local(src, wsrc.at[f * NCH + q, pl.ds(0, n)], wload.at[f * NCH + q])

    def preload():
        for q in range(NCH):
            for f in BOTH:
                w_load(f, q).start()

    barrier = pltpu.get_barrier_semaphore()
    for k in range(1, nx):
        pl.semaphore_signal(barrier, inc=1, device_id=at.dev(x=(x + k) % nx), device_id_type=MESH)
    for k in range(nx):
        pl.semaphore_signal(barrier, inc=1, device_id=at.dev(x=(x + k) % nx, y=at.far), device_id_type=MESH)
    pl.semaphore_signal(barrier, inc=1, device_id=at.dev(y=at.up), device_id_type=MESH)
    pl.semaphore_signal(barrier, inc=1, device_id=at.dev(y=at.down), device_id_type=MESH)
    pl.semaphore_signal(barrier, inc=1, device_id=at.dev(c=at.pc), device_id_type=MESH)
    load_x = local(x_hbm, xown, loc.at[0])
    load_x.start()
    preload()
    pl.semaphore_wait(barrier, TWO * nx + 2)
    load_x.wait()

    def x_send(r, to_right):
        i = 0 if to_right else 1
        src = xown if r == 0 else xg.at[1, x]
        return remote(src, xg.at[r, x], xsend.at[r, i], xrecv.at[r, i], at.dev(x=right if to_right else left))

    def x_relay(r, to_right):
        if to_right:
            part = xg.at[r, left, top]
            return remote(part, part, xsend.at[r, 2], xrecv.at[r, 2], at.dev(x=right))
        part = xg.at[r, right, bot]
        return remote(part, part, xsend.at[r, 3], xrecv.at[r, 3], at.dev(x=left))

    x_far = remote(xown, xg.at[1, x], ysend, yrecv, at.dev(y=at.far))
    keep_x = local(xown, xg.at[0, x], loc.at[1])

    blocks = [(f, q) for f in BOTH for q in range(NCH)]

    def w_src(f, q):
        return wsrc.at[f * NCH + q]

    def w_dst(k, q):
        return w.at[q, pl.ds(pl.multiple_of(c * sb, SUB), sb), pl.ds(pl.multiple_of(k * hk, LANES), hk)]

    def w_own(q):
        return remote(w_src(at.half, q), w_dst(y, q), wsend.at[0, q], wrecv.at[0, q], at.dev(y=at.p))

    def w_other(q):
        return remote(w_src(1 - at.half, q), w_dst(y, q), wsend.at[1, q], wrecv.at[1, q], at.dev(y=at.a))

    def w_far(q):
        if q < TWO:
            return remote(w_dst(at.a, q), w_dst(at.a, q), wsend.at[2, q], wrecv.at[2, q], at.dev(y=at.p))
        return remote(w_src(1 - at.half, q), w_dst(y, q), wsend.at[2, q], wrecv.at[2, q], at.dev(y=at.far))

    def w_core(q):
        part = w.at[q, pl.ds(pl.multiple_of(c * sb, SUB), sb)]
        return remote(part, part, dsend.at[q], drecv.at[q], at.dev(c=at.pc))

    def w_local(f, q):
        n = rows_in(f, q)
        dst = w.at[q, pl.ds(pl.multiple_of(c * sb, SUB), n), pl.ds(pl.multiple_of(y * hk, LANES), hk)]
        return local(w_hbm.at[pl.ds(f * slot + q * sb, n)], dst, wloc.at[q])

    def w_out(q):
        w_own(q).start()
        w_other(q).start()
        if q >= TWO:
            w_far(q).start()

    x_send(0, RIGHT).start()
    x_send(0, LEFT).start()
    for q in range(NCH):
        for f in BOTH:
            w_load(f, q).wait()
            if rows_in(f, q) < sb:
                pad = sb - rows_in(f, q)
                wsrc[f * NCH + q, sb - pad :, :] = jnp.zeros((pad, hk), BF16)
        if q < TWO:
            w_out(q)
    keep_x.start()
    for f, q in blocks:
        @pl.when(at.half == f)
        def _():
            w_local(f, q).start()
            if rows_in(f, q) < sb:
                pad = sb - rows_in(f, q)
                at_row = pl.multiple_of(c * sb + sb - pad, SUB)
                w[q, pl.ds(at_row, pad), pl.ds(pl.multiple_of(y * hk, LANES), hk)] = jnp.zeros((pad, hk), BF16)

    peers = [(0, k) for k in range(1, nx)] + [(1, k) for k in range(nx)]

    def lab_copy(i):
        sy, k = peers[i]
        return remote(
            lab_hbm, laba.at[sy, x], lsend.at[i], lrecv.at[sy, x],
            at.dev(x=(x + k) % nx, y=at.far if sy else y),
        )

    for i in range(len(peers)):
        lab_copy(i).start()
    lab_own = local(lab_hbm, laba.at[0, x], loc.at[2])
    lab_own.start()

    tail = lax.broadcasted_iota(jnp.int32, bias.shape[1:], 1)
    slot_of = tail // LANES
    pos = slot - LANES + tail - slot_of * LANES
    half_b = jnp.where(slot_of == 0, half_of(y, 0, ny), half_of(y, 1, ny))
    bias[...] = jnp.zeros_like(bias)
    bias[NCH - 1] = jnp.where((half_b == 1) & (pos >= vocab - slot), LOW, 0.0)
    m[...] = jnp.full_like(m, -3e38)
    s[...] = jnp.zeros_like(s)

    def xt_out(run, u):
        return local(
            xtb.at[u], xt.at[run // TWO, :, pl.ds(pl.multiple_of((run % TWO) * tr, LANES), tr)], tsem.at[u]
        )

    for q in BOTH:
        w_other(q).wait_recv()
        w_far(q).start()
    x_far.start()
    for q in range(TWO, NCH):
        w_out(q)
    keep_x.wait()
    x_send(0, RIGHT).wait_recv()
    x_relay(0, RIGHT).start()
    x_send(0, LEFT).wait_recv()
    x_relay(0, LEFT).start()

    n_steps = TWO * nx * NCH

    near = (0, 3, 1, 2)
    order = [(0, k, j) for k in near for j in BOTH] + [(1, 0, 0), (1, 0, 1)]
    order += [(0, k, 2) for k in near] + [(1, 0, 2), (1, 3, 0), (1, 3, 1), (1, 1, 0), (1, 1, 1), (1, 3, 2)]
    order += [(0, k, 3) for k in near] + [(1, 1, 2)] + [(1, 2, j) for j in range(3)] + [(1, k, 3) for k in (0, 3, 1, 2)]
    order += [(r, k, 4) for r in BOTH for k in near]
    codes = [(r * 4 + k) * 8 + j for r, k, j in order]

    def code_of(t):
        return tuple(pick(t, codes[u::TWO]) for u in BOTH)

    def place_of(code):
        run = code // 8
        return run // 4, code % 8, (x + run % 4) % nx

    def xcp(i, u):
        r, j, k = place_of(i)
        return local(xg.at[r, k], xb.at[u], xsem.at[u])

    def zcp(i, u):
        r, j, k = place_of(i)
        return local(zb.at[u], z.at[j, r, k], zsem.at[u])

    def step(i, u):
        r, j, k = place_of(i)
        run = r * nx + k
        c0 = 0
        for width in (sb * 4 // 5, TWO * sb - sb * 4 // 5) if sb % 640 == 0 else (2 * sb,):
            cols = slice(c0, c0 + width)
            zz = lax.dot_general(xb[u], w[j, cols, :], (((1,), (1,)), ((), ())), preferred_element_type=F32)
            zb[u, :, cols] = zz
            blk = min(64, tr)
            for o in range(0, tr, blk):
                rows = slice(o, o + blk)
                m_old = m[run, rows, :]
                parts = [zz[rows, LANES * e : LANES * e + LANES] for e in range(width // LANES)]
                for e in range(width // LANES):
                    at_e = slice(c0 + LANES * e, c0 + LANES * e + LANES)
                    if at_e.stop % sb == 0:
                        end = at_e.stop // sb
                        parts[e] = parts[e] + bias[j, 0:1, LANES * end - LANES : LANES * end]
                        zb[u, rows, at_e] = parts[e]
                mx = m_old
                for part in parts:
                    mx = jnp.maximum(mx, part)
                acc = s[run, rows, :] * jnp.exp(m_old - mx)
                for part in parts:
                    acc = acc + jnp.exp(part - mx)
                m[run, rows, :] = mx
                s[run, rows, :] = acc
            c0 += width

    def stat_copy(r, i):
        sy, k = peers[i]
        rr = 1 - r if sy else r
        return remote(
            stm.at[r], sta.at[sy, x, rr], ssend.at[r, i], srecv.at[sy, x, rr],
            at.dev(x=(x + k) % nx, y=at.far if sy else y),
        )

    def stat_own(r):
        return local(stm.at[r], sta.at[0, x, r], loc.at[3 + r])

    def finish_stats(r):
        lane = lax.broadcasted_iota(jnp.int32, m.shape[1:], 1)
        blk = jnp.zeros(m.shape[1:], F32)
        for d in range(nx):
            mm = m[r * nx + d]
            top_m = jnp.max(mm, axis=1, keepdims=True)
            tot = jnp.sum(s[r * nx + d] * jnp.exp(mm - top_m), axis=1, keepdims=True)
            blk = jnp.where(lane == d, top_m, jnp.where(lane == nx + d, tot, blk))
        stm[r] = blk.T[0:SUB, :]
        for i in range(len(peers)):
            stat_copy(r, i).start()
        stat_own(r).start()

    def w_here(j):
        for f in BOTH:
            pl.when(at.half == f)(w_local(f, j).wait)

        w_own(j).wait_recv()
        if j >= TWO:
            w_other(j).wait_recv()
        w_far(j).wait_recv()
        w_core(j).start()

    here_at = (0, 0, 5, 9, 15)
    both_at = (0, 0, 5, 10, 16)

    def body(t, held):
        older, old, now = held
        later = code_of(t + 1)

        @pl.when((t == 0) | (t == 4) | (t == 7))
        def _():
            @pl.when(t == 4)
            def _():
                x_far.wait_recv()
                x_send(1, RIGHT).start()
                x_send(1, LEFT).start()

            @pl.when(t == 7)
            def _():
                x_send(1, RIGHT).wait_recv()
                x_relay(1, RIGHT).start()
                x_send(1, LEFT).wait_recv()
                x_relay(1, LEFT).start()

            for u in BOTH:
                xcp(now[u], (t % TWO) * TWO + u).start()

        for j in range(NCH):
            pl.when(t == here_at[j])(functools.partial(w_here, j))
            pl.when(t == both_at[j])(w_core(j).wait_recv)

        @pl.when(t == 2)
        def _():
            x_relay(0, RIGHT).wait_recv()
            x_relay(0, LEFT).wait_recv()

        @pl.when(t == 11)
        def _():
            x_relay(1, RIGHT).wait_recv()
            x_relay(1, LEFT).wait_recv()

        @pl.when(t == 16)
        def _():
            local(w, wo, loc.at[5]).start()

        @pl.when(t == 18)
        def _():
            finish_stats(0)

        base = (t % TWO) * 2
        for u in BOTH:
            xcp(now[u], base + u).wait()

        for u in BOTH:
            r, j, k = place_of(now[u])

            @pl.when(j == 0)
            def _():
                cp = xt_out(r * nx + k, u)
                xtb[u] = xb[base + u].T
                cp.start()

        @pl.when((TWO * t + 2 < n_steps) & (t != 3) & (t != 6))
        def _():
            for u in BOTH:
                xcp(later[u], 2 - base + u).start()

        @pl.when(t > 1)
        def _():
            for u in BOTH:
                zcp(older[u], base + u).wait()

        for u in BOTH:
            step(now[u], base + u)
        for u in BOTH:
            zcp(now[u], base + u).start()
            r, j, k = place_of(now[u])

            @pl.when(j == 0)
            def _():
                xt_out(r * nx + k, u).wait()

        return old, now, later

    none = (jnp.int32(0),) * TWO
    older, old, _ = lax.fori_loop(0, n_steps // TWO, body, (none, none, code_of(jnp.int32(0))))
    finish_stats(1)
    for u in BOTH:
        zcp(older[u], u).wait()
        zcp(old[u], TWO + u).wait()
    local(w, wo, loc.at[5]).wait()
    lab_own.wait()
    stat_own(0).wait()
    stat_own(1).wait()
    for r in BOTH:
        for right_way in (RIGHT, LEFT):
            x_send(r, right_way).wait_send()
            x_relay(r, right_way).wait_send()
    x_far.wait_send()
    for q in range(NCH):
        w_own(q).wait_send()
        w_other(q).wait_send()
        w_far(q).wait_send()
        w_core(q).wait_send()
    for i in range(len(peers)):
        lab_copy(i).wait_send()
        stat_copy(0, i).wait_send()
        stat_copy(1, i).wait_send()
    for sy in BOTH:
        for k in range(nx):
            def arrived():
                remote(lab_hbm, laba.at[sy, k], lsend.at[0], lrecv.at[sy, k], at.dev(c=at.pc)).wait_recv()
                for rr in BOTH:
                    remote(stm.at[rr], sta.at[sy, k, rr], ssend.at[0, 0], srecv.at[sy, k, rr], at.dev(c=at.pc)).wait_recv()

            if sy == 0:
                pl.when(k != x)(arrived)
            else:
                arrived()


def gather_logits(nx, ny, vocab, x, w, lab):
    tr, h = x.shape
    hk = w.shape[1]
    vp = -(-vocab // (TWO * LANES * NCH)) * TWO * LANES * NCH
    ch = vp // NCH
    shape = jax.ShapeDtypeStruct
    dma = pltpu.SemaphoreType.DMA
    vm = pltpu.VMEM
    flops = TWO * TWO * nx * tr * h * vp
    return pl.pallas_call(
        functools.partial(gather_logits_kernel, nx, ny, vocab),
        out_shape=(
            shape((TWO, nx, tr, h), BF16),
            shape((NCH, ch, h), BF16),
            shape((NCH, TWO, nx, tr, ch), F32),
            shape((TWO, nx, TWO, SUB, tr), F32),
            shape((TWO, nx) + lab.shape, jnp.int32),
            shape((nx, h, TWO * tr), BF16),
        ),
        in_specs=[ANY] * 3,
        out_specs=(ANY,) * 6,
        scratch_shapes=[
            vm((NCH, ch, h), BF16), vm((TWO * NCH, ch // TWO, hk), BF16), vm((tr, h), BF16),
            vm((4, tr, h), BF16), vm((4, tr, ch), F32), vm((NCH, SUB, TWO * LANES), F32),
            vm((TWO * nx, tr, LANES), F32), vm((TWO * nx, tr, LANES), F32), vm((TWO, SUB, tr), F32), vm((TWO, h, tr), BF16),
            dma((TWO, 4)), dma((TWO, 4)), dma, dma, dma((3, NCH)), dma((3, NCH)), dma((NCH,)), dma((NCH,)),
            dma((TWO, TWO * nx - 1)), dma((TWO, nx, TWO)), dma((TWO * nx - 1,)), dma((TWO, nx)),
            dma((6,)), dma((NCH,)), dma((4,)), dma((4,)), dma((TWO,)), dma((TWO * NCH,)),
        ],
        compiler_params=pltpu.CompilerParams(
            collective_id=0, has_side_effects=True, vmem_limit_bytes=60 * 2**20
        ),
        cost_estimate=pl.CostEstimate(flops=flops, bytes_accessed=4 * TWO * nx * tr * vp, transcendentals=0),
        name="gather_logits",
    )(x, w, lab)


def grads_kernel(
    nx, ny, inv, vocab, z, w_hbm, xt_hbm, sta_hbm, lab_hbm, dxo, dwo, loss, rx, fx, dd, rr,
    w, xt, zb, gb, acc, dx, st, sta, laba, lacc, tmpa, tmpb, keep, fin, fdx, lbuf,
    wsem, tsem, zsem, xsend, xrecv, fsend, frecv, dsend, drecv, rsend, rrecv, osend, orecv, asem, bsem, lsend, lrecv,
    out_sem, ssem,
):
    at = Place(nx, ny)
    x, y, c = at.x, at.y, at.c
    tr, h = dxo.shape
    ch = zb.shape[2]
    sb = ch // TWO
    slot = NCH * sb
    hk = dwo.shape[1]
    nq = rx.shape[2]
    qr = tr // nq
    left, right = (x + nx - 1) % nx, (x + 1) % nx

    def par(yy, b):
        return jnp.where((yy + b) % TWO == 0, (yy + 1) % ny, (yy + ny - 1) % ny)

    def adj(yy, b):
        return jnp.where((yy + b) % TWO == 0, (yy + ny - 1) % ny, (yy + 1) % ny)

    stats = [local(sta_hbm, sta, ssem.at[0]), local(lab_hbm, laba, ssem.at[1])]
    for cp in stats:
        cp.start()
    local(w_hbm.at[0], w.at[0], wsem.at[0]).start()
    barrier = pltpu.get_barrier_semaphore()
    for k in range(1, nx):
        pl.semaphore_signal(barrier, inc=1, device_id=at.dev(x=(x + k) % nx), device_id_type=MESH)
    for k in range(1, ny):
        pl.semaphore_signal(barrier, inc=1, device_id=at.dev(y=(y + k) % ny), device_id_type=MESH)
        pl.semaphore_signal(barrier, inc=1, device_id=at.dev(y=(y + k) % ny, c=at.pc), device_id_type=MESH)
    pl.semaphore_signal(barrier, inc=1, device_id=at.dev(c=at.pc), device_id_type=MESH)

    segments = ["x0", "w0", "w1", "x1", "w2", "w3", "x2", "x3", "w4"]
    first, after, n_body = {}, {}, 0
    for seg in segments:
        first[seg] = n_body
        n_body += NCH if seg.startswith("x") else nx
        after[seg] = n_body

    def body_at(n):
        code, start = 0, 0
        for seg in segments[1:]:
            here = n >= first[seg]
            code = jnp.where(here, int(seg.startswith("w")) * 8 + int(seg[-1]), code)
            start = jnp.where(here, first[seg], start)
        return code // 8, code % 8, n - start

    def tile(n, u):
        kind, i, k = body_at(n)
        mine = jnp.where(u == 0, (x + TWO * nx - 1 - i) % nx, (x + 1 + i) % nx)
        run = TWO * k + u
        is_x = kind == 0
        return jnp.where(is_x, k, i), jnp.where(is_x, u, run // nx), jnp.where(is_x, mine, run % nx)

    def zcp(n, u, buf):
        j, r, d = tile(n, u)
        return local(z.at[j, r, d], zb.at[buf], zsem.at[buf])

    for u in BOTH:
        zcp(0, u, u).start()
    for j in range(1, NCH):
        local(w_hbm.at[j], w.at[j], wsem.at[j]).start()
    local(xt_hbm, xt, tsem).start()

    for cp in stats:
        cp.wait()
    for r in BOTH:
        parts = [sta[sy, k, r] for sy in BOTH for k in range(nx)]
        top = functools.reduce(jnp.maximum, [part[0:nx] for part in parts])
        tot = sum(part[nx : TWO * nx] * jnp.exp(part[0:nx] - top) for part in parts)
        shift = top + jnp.log(tot) - math.log(inv)
        for d in range(nx):
            col = jnp.full(laba.shape[TWO:], -1, jnp.int32)
            for b in BOTH:
                base = (x * TWO + b) * vocab + half_of(y, b, ny) * slot
                pos = laba[r, d] - base
                room = jnp.where(half_of(y, b, ny) == 0, slot, vocab - slot)
                chunk = sum((pos >= q * sb).astype(jnp.int32) for q in range(1, NCH))
                col = jnp.where((pos >= 0) & (pos < room), chunk * ch + b * sb + pos - chunk * sb, col)
            line = jnp.concatenate([col[o : o + 1].astype(F32) for o in range(tr // LANES)], axis=1)
            rows = jnp.concatenate([shift[d : d + 1], line, jnp.zeros((SUB - TWO, tr), F32)], axis=0)
            st[r * nx + d] = jnp.concatenate([rows] * 16, axis=0).T
    lacc[...] = jnp.zeros_like(lacc)
    pl.semaphore_wait(barrier, nx - 1 + TWO * (ny - 1) + 1)

    def x_copy(s, dr, q):
        return remote(
            dx.at[s % TWO, dr, pl.ds(pl.multiple_of(q * qr, SUB), qr)], rx.at[s, dr, q],
            xsend.at[s, dr, q], xrecv.at[s, dr, q], at.dev(x=left if dr else right),
        )

    def far_copy(q):
        return remote(
            dx.at[1, 1, pl.ds(pl.multiple_of(q * qr, SUB), qr)], fx.at[q], fsend.at[q], frecv.at[q], at.dev(y=at.far)
        )

    def a_load(s, q, dr):
        return local(rx.at[s - 1, dr, q], tmpa.at[q % TWO, dr], asem.at[q % TWO, dr])

    def a_pre(s, q):
        for dr in BOTH:
            x_copy(s - 1, dr, q).wait_recv()
            a_load(s, q, dr).start()

    def a_use(s, q):
        rows = pl.ds(pl.multiple_of(q * qr, SUB), qr)
        for dr in BOTH:
            a_load(s, q, dr).wait()
            dx[s % TWO, dr, rows, :] += tmpa[q % TWO, dr]

        @pl.when(s < nx - 1)
        def _():
            for dr in BOTH:
                x_copy(s, dr, q).start()

        @pl.when(s == nx - 1)
        def _():
            far_copy(q).start()

    def f_load(q):
        return local(fx.at[q], tmpa.at[q % TWO, 0], asem.at[q % TWO, 0])

    def f_out(q):
        return local(fdx.at[q % TWO], dxo.at[pl.ds(pl.multiple_of(q * qr, 16), qr)], out_sem.at[q])

    def f_pre(q):
        far_copy(q).wait_recv()
        f_load(q).start()

    def f_use(q):
        f_load(q).wait()

        @pl.when(q > 1)
        def _():
            f_out(q - 2).wait()

        rows = pl.ds(pl.multiple_of(q * qr, SUB), qr)
        fdx[q % TWO] = (dx[1, 0, rows] + tmpa[q % TWO, 0]).astype(BF16)
        f_out(q).start()

    def lot(b):
        q = (c + b) % TWO
        slices = [(b + TWO * q) % ny, (b + 1 + TWO * q) % ny]
        other = [(b + TWO * (1 - q)) % ny, (b + 1 + TWO * (1 - q)) % ny]
        home = half_of(y, b, ny) == q
        kt = jnp.where(home, y, adj(y, b))
        it = jnp.where(slices[0] == kt, 0, 1)
        return slices, other, kt, it, home

    def rows_of(k):
        return pl.ds(pl.multiple_of(k * hk, 16), hk)

    def d_copy(j, b, i):
        other = lot(b)[1]
        return remote(
            acc.at[j % TWO, rows_of(other[i]), pl.ds(b * sb, sb)], dd.at[j, b, i],
            dsend.at[j, b, i], drecv.at[j, b, i], at.dev(c=at.pc),
        )

    def d_send(j):
        for b in BOTH:
            for i in BOTH:
                d_copy(j, b, i).start()

    def r_load(j, b, i):
        return local(dd.at[j, b, i], tmpb.at[b, i], bsem.at[b, i])

    def r_pre(j):
        for b in BOTH:
            for i in BOTH:
                d_copy(j, b, i).wait_recv()
                r_load(j, b, i).start()

    def r_copy(j, b):
        slices, _, _, it, _ = lot(b)
        kg = jnp.where(it == 0, slices[1], slices[0])
        src = acc.at[j % TWO, rows_of(kg), pl.ds(b * sb, sb)]
        return remote(src, rr.at[j, b], rsend.at[j, b], rrecv.at[j, b], at.dev(y=par(y, b)))

    def r_use(j):
        for b in BOTH:
            slices, _, kt, it, _ = lot(b)
            kg = jnp.where(it == 0, slices[1], slices[0])
            for i in BOTH:
                r_load(j, b, i).wait()

            acc[j % TWO, rows_of(kg), pl.ds(b * sb, sb)] += tmpb[b, 1 - it]
            r_copy(j, b).start()
            keep[j % TWO, b] = acc[j % TWO, rows_of(kt), pl.ds(b * sb, sb)] + tmpb[b, it]

    def s_load(j, b):
        return local(rr.at[j, b], tmpb.at[b, 0], bsem.at[b, 0])

    def s_pre(j):
        for b in BOTH:
            r_copy(j, b).wait_recv()
            s_load(j, b).start()

    def o_copy(j, b):
        kt = lot(b)[2]
        f = half_of(y, b, ny)
        dst = dwo.at[pl.ds(pl.multiple_of(f * slot + j * sb, SUB), sb)]
        return remote(fin.at[b], dst, osend.at[j, b], orecv.at[f, j], at.dev(y=kt, c=b))

    def o_here(j, b):
        f = half_of(y, b, ny)
        dst = dwo.at[pl.ds(pl.multiple_of(f * slot + j * sb, SUB), sb)]
        return local(fin.at[b], dst, orecv.at[f, j])

    def is_here(b):
        return lot(b)[4] & (c == b)

    def s_use(j):
        for b in BOTH:
            s_load(j, b).wait()

            @pl.when((j > 0) & jnp.logical_not(is_here(b)))
            def _():
                o_copy(j - 1, b).wait_send()

            @pl.when((j > 0) & is_here(b))
            def _():
                o_here(j - 1, b).wait()

            fin[b] = (keep[j % TWO, b] + tmpb[b, 0]).T.astype(BF16)

            @pl.when(is_here(b))
            def _():
                o_here(j, b).start()

            @pl.when(jnp.logical_not(is_here(b)))
            def _():
                o_copy(j, b).start()

    def l_copy(stage, k):
        if stage == 0:
            return remote(lbuf.at[0, x], lbuf.at[0, x], lsend.at[0, k], lrecv.at[0, x], at.dev(x=(x + k) % nx))
        if stage == 1:
            return remote(lbuf.at[1, y], lbuf.at[1, y], lsend.at[1, k], lrecv.at[1, y], at.dev(y=(y + k) % ny))
        return remote(lbuf.at[2, c], lbuf.at[2, c], lsend.at[2, 0], lrecv.at[2, c], at.dev(c=at.pc))

    def l_sum(stage, size, me):
        for k in range(size):
            @pl.when(k != me)
            def _():
                remote(
                    lbuf.at[stage, k], lbuf.at[stage, k], lsend.at[stage, 0], lrecv.at[stage, k], at.dev(c=at.pc)
                ).wait_recv()

        total = lbuf[stage, 0]
        for k in range(1, size):
            total = total + lbuf[stage, k]
        return total

    def l_start():
        lbuf[0, x] = -lacc[...]
        for k in range(1, nx):
            l_copy(0, k).start()

    def l_mid():
        lbuf[1, y] = l_sum(0, nx, x)
        for k in range(1, ny):
            l_copy(1, k).start()

    def l_late():
        lbuf[2, c] = l_sum(1, ny, y)
        l_copy(2, 0).start()

    lane = lax.broadcasted_iota(jnp.int32, (min(64, tr), LANES), 1).astype(F32)

    def each_tile(n, u, buf, c0, c1, fn):
        j, r, d = tile(n, u)
        blk = min(64, tr)
        for o in range(0, tr, blk):
            rows = slice(o, o + blk)
            t = st[r * nx + d, rows, :]
            shift = jnp.broadcast_to(t[:, 0:1], (blk, LANES))
            lab = jnp.broadcast_to(t[:, 1:TWO], (blk, LANES)) - (j * ch).astype(F32)
            for e in range(c0 // LANES, c1 // LANES):
                cols = slice(LANES * e, LANES * e + LANES)
                fn(rows, cols, zb[buf, rows, cols] - shift, lane + float(LANES * e) == lab)

    def make_g(n, u, buf, c0, c1, loss_sum=None):
        def one(rows, cols, dist, hit):
            g = jnp.exp(dist)
            gb[u, rows, cols] = jnp.where(hit, g - inv, g).astype(BF16)
            if loss_sum is not None:
                loss_sum.append(jnp.where(hit, dist, 0.0) + (loss_sum.pop() if loss_sum else 0.0))

        each_tile(n, u, buf, c0, c1, one)

    big = ch % (10 * LANES) == 0
    x_cuts = [(ch * e // 5, ch * (e + 1) // 5) for e in range(5)] if big else [(0, ch)]
    w_cuts = [(0, ch // 5), (ch // 5, ch * 3 // 5), (ch * 3 // 5, ch)] if big else [(0, ch)]

    def x_body(n, base):
        _, s, j = body_at(n)
        half = s % TWO

        @pl.when(j == 0)
        def _():
            dx[half] = jnp.zeros(dx.shape[1:], F32)

        for u in BOTH:
            for c0, c1 in x_cuts:
                loss_sum = []
                make_g(n, u, base + u, c0, c1, loss_sum)
                lacc[...] += jnp.sum(loss_sum[0].reshape(-1, SUB, LANES), axis=0)
                dx[half, u] += lax.dot_general(
                    gb[u, :, c0:c1], w[j, c0:c1, :], (((1,), (0,)), ((), ())), preferred_element_type=F32
                )

    def w_body(n, base):
        _, j, k = body_at(n)
        half = j % TWO

        @pl.when(k == 0)
        def _():
            acc[half] = jnp.zeros(acc.shape[1:], F32)

        for c0, c1 in w_cuts:
            for u in BOTH:
                make_g(n, u, base + u, c0, c1)
            acc[half, :, c0:c1] += jnp.dot(
                xt[k], gb[:, :, c0:c1].reshape(TWO * tr, c1 - c0), preferred_element_type=F32
            )

    plan_a = [(after["x1"] + q, 1, q) for q in range(nq)] + [(after["x2"] + q, 2, q) for q in range(nq)]
    plan_a += [(after["x3"] + 3 * q, 3, q) for q in range(nq)]
    plan_r = [(11, 12, 0), (15, 16, 1), (24, 25, 2), (28, 29, 3), (42, 43, 4)]
    plan_s = [(17, 18, 0), (21, 22, 1), (30, 31, 2), (34, 35, 3), (46, 47, 4)]
    pre_r, use_r = [(p, j) for p, _, j in plan_r], [(u, j) for _, u, j in plan_r]
    pre_s, use_s = [(p, j) for p, _, j in plan_s], [(u, j) for _, u, j in plan_s]
    plan_f = [(41, 0), (44, 1), (46, 2), (48, 3)]
    n_all = n_body + TWO * nq + 1

    def when(n, table, fn):
        table = [(e[0], e[1:]) for e in table]
        hit = functools.reduce(lambda p, q: p | q, [n == e for e, _ in table])

        @pl.when(hit)
        def _():
            args = []
            for i in range(len(table[0][1])):
                val = 0
                for e, vals in table:
                    if vals[i]:
                        val = val + jnp.where(n == e, vals[i], 0)
                args.append(val + jnp.int32(0))
            fn(*args)

    def body(n, _):
        @pl.when(n < NCH)
        def _():
            local(w_hbm.at[n], w.at[n], wsem.at[n]).wait()

        @pl.when(n == first["w0"])
        def _():
            local(xt_hbm, xt, tsem).wait()
            for q in range(nq):
                for dr in BOTH:
                    x_copy(0, dr, q).start()

        when(n, [(after["w%d" % j], j) for j in range(NCH)], d_send)
        when(n, plan_a, a_use)
        when(n, plan_f, f_use)
        when(n, use_r, r_use)
        when(n, use_s, s_use)
        when(n, [(e[0] - 1,) + e[1:] for e in plan_a], a_pre)
        when(n, [(e[0] - 1,) + e[1:] for e in plan_f], f_pre)
        when(n, pre_r, r_pre)
        when(n, pre_s, s_pre)

        for at_n, fn in ((n_body, l_start), (n_body + TWO, l_mid), (n_body + nq, l_late)):
            pl.when(n == at_n)(fn)

        @pl.when((n == first["x2"]) | (n == first["x3"]))
        def _():
            s = jnp.where(n == first["x2"], 0, 1)
            for q in range(nq):
                for dr in BOTH:
                    x_copy(s, dr, q).wait_send()

        for j in range(2, NCH):
            @pl.when(n == first["w%d" % j])
            def _():
                for b in BOTH:
                    r_copy(j - 2, b).wait_send()
                    for i in BOTH:
                        d_copy(j - 2, b, i).wait_send()

        base = (n % TWO) * 2

        @pl.when(n < n_body)
        def _():
            for u in BOTH:
                zcp(n, u, base + u).wait()

            @pl.when(n + 1 < n_body)
            def _():
                for u in BOTH:
                    zcp(n + 1, u, 2 - base + u).start()

            kind = body_at(n)[0]

            @pl.when(kind == 0)
            def _():
                x_body(n, base)

            @pl.when(kind == 1)
            def _():
                w_body(n, base)

        return 0

    lax.fori_loop(0, n_all, body, 0)
    loss[...] = l_sum(2, TWO, c)

    for q in range(nq):
        if q >= nq - 2:
            f_out(q).wait()
        far_copy(q).wait_send()
        for dr in BOTH:
            x_copy(2, dr, q).wait_send()
    for b in BOTH:
        for j in range(NCH - 2, NCH):
            for i in BOTH:
                d_copy(j, b, i).wait_send()
            r_copy(j, b).wait_send()

        @pl.when(is_here(b))
        def _():
            o_here(NCH - 1, b).wait()

        @pl.when(jnp.logical_not(is_here(b)))
        def _():
            o_copy(NCH - 1, b).wait_send()

    q0 = half_of(y, c, ny)
    for f in BOTH:
        kept = (f == q0) & ((q0 + c) % TWO == c)

        @pl.when(jnp.logical_not(kept))
        def _():
            for j in range(NCH):
                dst = dwo.at[pl.ds(f * slot + j * sb, sb)]
                remote(fin.at[0], dst, osend.at[j, 0], orecv.at[f, j], at.dev(c=at.pc)).wait_recv()

    for k in range(1, nx):
        l_copy(0, k).wait_send()
    for k in range(1, ny):
        l_copy(1, k).wait_send()
    l_copy(2, 0).wait_send()


def grads(nx, ny, inv, vocab, z, w, xt, sta, laba, hk):
    ch, h = w.shape[1:]
    tr = z.shape[3]
    nq = 4
    shape = jax.ShapeDtypeStruct
    dma = pltpu.SemaphoreType.DMA
    vm = pltpu.VMEM
    vspec = pl.BlockSpec(memory_space=pltpu.VMEM)
    sb, qr = ch // TWO, tr // nq
    return pl.pallas_call(
        functools.partial(grads_kernel, nx, ny, inv, vocab),
        out_shape=(
            shape((tr, h), BF16), shape((NCH * ch, hk), BF16), shape((SUB, LANES), F32),
            shape((nx - 1, TWO, nq, qr, h), F32), shape((nq, qr, h), F32),
            shape((NCH, TWO, TWO, hk, sb), F32), shape((NCH, TWO, hk, sb), F32),
        ),
        in_specs=[ANY] * 5,
        out_specs=(ANY, ANY, vspec, ANY, ANY, ANY, ANY),
        scratch_shapes=[
            vm((NCH, ch, h), BF16), vm((nx, h, TWO * tr), BF16), vm((4, tr, ch), F32), vm((TWO, tr, ch), BF16),
            vm((TWO, h, ch), F32), vm((TWO, TWO, tr, h), F32), vm((TWO * nx, tr, LANES), F32), vm(sta.shape, F32), vm(laba.shape, jnp.int32), vm((SUB, LANES), F32),
            vm((TWO, TWO, qr, h), F32), vm((TWO, TWO, hk, sb), F32), vm((TWO, TWO, hk, sb), F32),
            vm((TWO, sb, hk), BF16), vm((TWO, qr, h), BF16), vm((3, max(nx, ny), SUB, LANES), F32),
            dma((NCH,)), dma, dma((4,)), dma((nx - 1, TWO, nq)), dma((nx - 1, TWO, nq)), dma((nq,)), dma((nq,)),
            dma((NCH, TWO, TWO)), dma((NCH, TWO, TWO)), dma((NCH, TWO)), dma((NCH, TWO)), dma((NCH, TWO)), dma((TWO, NCH)),
            dma((TWO, TWO)), dma((TWO, TWO)), dma((3, max(nx, ny))), dma((3, max(nx, ny))), dma((nq,)), dma((TWO,)),
        ],
        compiler_params=pltpu.CompilerParams(
            collective_id=1, has_side_effects=True, vmem_limit_bytes=67_000_000
        ),
        name="grads",
    )(z, w, xt, sta, laba)


def solution(mesh):
    ny = mesh.shape["fsdp"]
    tp_size = mesh.shape["tp"]
    nx = tp_size // TWO
    token_spec = P(("dp", "fsdp", "tp"), None)
    label_spec = P(("dp", "fsdp", "tp"))

    def local_step(hidden, w_head, labels):
        tr, h = hidden.shape
        hk, vocab = w_head.shape
        inv = 1.0 / (tr * tp_size * ny)
        lab = labels.reshape(-1, LANES)
        xg, wg, z, sta, laba, xt = gather_logits(nx, ny, vocab, hidden, w_head.T, lab)
        d_hidden, d_w, loss = grads(nx, ny, inv, vocab, z, wg, xt, sta, laba, hk)[:3]
        mean_loss = jnp.sum(loss) * inv + math.log(inv)
        return mean_loss.reshape(1), d_hidden, d_w[:vocab].T

    return jax.shard_map(
        local_step,
        mesh=mesh,
        in_specs=(token_spec, P("fsdp", "tp"), label_spec),
        out_specs=(P("dp"), token_spec, P(("dp", "fsdp"), "tp")),
        check_vma=False,
    )
```

```python
import functools
import math

import jax
import jax.numpy as jnp
from jax import lax
from jax.experimental import pallas as pl
from jax.experimental.pallas import tpu as pltpu
from jax.sharding import PartitionSpec as P

MESH = pl.DeviceIdType.MESH
F32 = jnp.float32
BF16 = jnp.bfloat16
NCH = 5
LOW = -1e30
ANY = pl.BlockSpec(memory_space=pl.ANY)
LANES = 128
SUB = 8
TWO = 2
BOTH = range(TWO)
RIGHT, LEFT = True, False


class Place:
    def __init__(self, nx, ny):
        tp = lax.axis_index("tp")
        self.nx, self.ny = nx, ny
        self.x, self.c, self.y = tp // TWO, tp % TWO, lax.axis_index("fsdp")
        up, down = (self.y + 1) % ny, (self.y + ny - 1) % ny
        even = (self.y + self.c) % TWO == 0
        self.up, self.down = up, down
        self.pc = 1 - self.c
        self.p = jnp.where(even, up, down)
        self.a = jnp.where(even, down, up)
        self.far = (self.y + 2) % ny
        self.half = ((self.y - self.c + ny) % ny) // TWO

    def dev(self, x=None, y=None, c=None):
        x = self.x if x is None else x
        y = self.y if y is None else y
        c = self.c if c is None else c
        return {"fsdp": y, "tp": x * 2 + c}


def half_of(y, b, ny):
    return ((y - b + ny) % ny) // TWO


def pick(n, table):
    out = 0
    for i, v in enumerate(table):
        if v:
            out = out + jnp.where(n == i, v, 0)
    return out


def remote(src, dst, ssem, rsem, dev):
    return pltpu.make_async_remote_copy(
        src_ref=src, dst_ref=dst, send_sem=ssem, recv_sem=rsem, device_id=dev, device_id_type=MESH
    )


def local(src, dst, sem):
    return pltpu.make_async_copy(src, dst, sem)


def gather_logits_kernel(
    nx, ny, vocab,
    x_hbm, w_hbm, lab_hbm, xg, wo, z, sta, laba, xt,
    w, wsrc, xown, xb, zb, bias, m, s, stm, xtb,
    xsend, xrecv, ysend, yrecv, wsend, wrecv, dsend, drecv, ssend, srecv, lsend, lrecv, loc, wloc, xsem, zsem, tsem, wload,
):
    at = Place(nx, ny)
    x, y, c = at.x, at.y, at.c
    tr = xown.shape[0]
    hk = w_hbm.shape[1]
    sb = w.shape[1] // TWO
    slot = NCH * sb
    left, right = (x + nx - 1) % nx, (x + 1) % nx
    top, bot = pl.ds(0, tr // TWO), pl.ds(tr // TWO, tr // TWO)

    def rows_in(f, q):
        return min(sb, vocab - f * slot - q * sb)

    def w_load(f, q):
        n = rows_in(f, q)
        src = w_hbm.at[pl.ds(f * slot + q * sb, n)]
        return local(src, wsrc.at[f * NCH + q, pl.ds(0, n)], wload.at[f * NCH + q])

    def preload():
        for q in range(NCH):
            for f in BOTH:
                w_load(f, q).start()

    barrier = pltpu.get_barrier_semaphore()
    for k in range(1, nx):
        pl.semaphore_signal(barrier, inc=1, device_id=at.dev(x=(x + k) % nx), device_id_type=MESH)
    for k in range(nx):
        pl.semaphore_signal(barrier, inc=1, device_id=at.dev(x=(x + k) % nx, y=at.far), device_id_type=MESH)
    pl.semaphore_signal(barrier, inc=1, device_id=at.dev(y=at.up), device_id_type=MESH)
    pl.semaphore_signal(barrier, inc=1, device_id=at.dev(y=at.down), device_id_type=MESH)
    pl.semaphore_signal(barrier, inc=1, device_id=at.dev(c=at.pc), device_id_type=MESH)
    load_x = local(x_hbm, xown, loc.at[0])
    load_x.start()
    preload()
    pl.semaphore_wait(barrier, TWO * nx + 2)
    load_x.wait()

    def x_send(r, to_right):
        i = 0 if to_right else 1
        src = xown if r == 0 else xg.at[1, x]
        return remote(src, xg.at[r, x], xsend.at[r, i], xrecv.at[r, i], at.dev(x=right if to_right else left))

    def x_relay(r, to_right):
        if to_right:
            part = xg.at[r, left, top]
            return remote(part, part, xsend.at[r, 2], xrecv.at[r, 2], at.dev(x=right))
        part = xg.at[r, right, bot]
        return remote(part, part, xsend.at[r, 3], xrecv.at[r, 3], at.dev(x=left))

    x_far = remote(xown, xg.at[1, x], ysend, yrecv, at.dev(y=at.far))
    keep_x = local(xown, xg.at[0, x], loc.at[1])

    blocks = [(f, q) for f in BOTH for q in range(NCH)]

    def w_src(f, q):
        return wsrc.at[f * NCH + q]

    def w_dst(k, q):
        return w.at[q, pl.ds(pl.multiple_of(c * sb, SUB), sb), pl.ds(pl.multiple_of(k * hk, LANES), hk)]

    def w_own(q):
        return remote(w_src(at.half, q), w_dst(y, q), wsend.at[0, q], wrecv.at[0, q], at.dev(y=at.p))

    def w_other(q):
        return remote(w_src(1 - at.half, q), w_dst(y, q), wsend.at[1, q], wrecv.at[1, q], at.dev(y=at.a))

    def w_far(q):
        return remote(w_src(1 - at.half, q), w_dst(y, q), wsend.at[2, q], wrecv.at[2, q], at.dev(y=at.far))

    def w_core(q):
        part = w.at[q, pl.ds(pl.multiple_of(c * sb, SUB), sb)]
        return remote(part, part, dsend.at[q], drecv.at[q], at.dev(c=at.pc))

    def w_local(f, q):
        n = rows_in(f, q)
        dst = w.at[q, pl.ds(pl.multiple_of(c * sb, SUB), n), pl.ds(pl.multiple_of(y * hk, LANES), hk)]
        return local(w_hbm.at[pl.ds(f * slot + q * sb, n)], dst, wloc.at[q])

    def w_out(q):
        w_own(q).start()
        w_other(q).start()
        w_far(q).start()

    x_send(0, RIGHT).start()
    x_send(0, LEFT).start()
    for q in range(NCH):
        for f in BOTH:
            w_load(f, q).wait()
            if rows_in(f, q) < sb:
                pad = sb - rows_in(f, q)
                wsrc[f * NCH + q, sb - pad :, :] = jnp.zeros((pad, hk), BF16)
        w_out(q)
        if q == 0:
            x_far.start()
    keep_x.start()
    for f, q in blocks:
        @pl.when(at.half == f)
        def _():
            w_local(f, q).start()
            if rows_in(f, q) < sb:
                pad = sb - rows_in(f, q)
                at_row = pl.multiple_of(c * sb + sb - pad, SUB)
                w[q, pl.ds(at_row, pad), pl.ds(pl.multiple_of(y * hk, LANES), hk)] = jnp.zeros((pad, hk), BF16)

    peers = [(0, k) for k in range(1, nx)] + [(1, k) for k in range(nx)]

    def lab_copy(i):
        sy, k = peers[i]
        return remote(
            lab_hbm, laba.at[sy, x], lsend.at[i], lrecv.at[sy, x],
            at.dev(x=(x + k) % nx, y=at.far if sy else y),
        )

    for i in range(len(peers)):
        lab_copy(i).start()
    lab_own = local(lab_hbm, laba.at[0, x], loc.at[2])
    lab_own.start()

    tail = lax.broadcasted_iota(jnp.int32, bias.shape[1:], 1)
    slot_of = tail // LANES
    pos = slot - LANES + tail - slot_of * LANES
    half_b = jnp.where(slot_of == 0, half_of(y, 0, ny), half_of(y, 1, ny))
    bias[...] = jnp.zeros_like(bias)
    bias[NCH - 1] = jnp.where((half_b == 1) & (pos >= vocab - slot), LOW, 0.0)
    m[...] = jnp.full_like(m, -3e38)
    s[...] = jnp.zeros_like(s)

    def xt_out(run, u):
        return local(
            xtb.at[u], xt.at[run // TWO, :, pl.ds(pl.multiple_of((run % TWO) * tr, LANES), tr)], tsem.at[u]
        )

    keep_x.wait()
    x_send(0, RIGHT).wait_recv()
    x_relay(0, RIGHT).start()
    x_send(0, LEFT).wait_recv()
    x_relay(0, LEFT).start()

    n_steps = TWO * nx * NCH

    near = (0, 3, 1, 2)
    order = [(0, k, 0) for k in near] + [(1, 0, 0)]
    order += [(0, k, 1) for k in near] + [(1, 0, 1)]
    order += [(1, k, j) for j in BOTH for k in (3, 1)]
    order += [(0, k, 2) for k in near] + [(1, k, 2) for k in (0, 3, 1)] + [(1, 2, j) for j in range(3)]
    order += [(r, k, j) for j in (3, 4) for r in BOTH for k in near]
    codes = [(r * 4 + k) * 8 + j for r, k, j in order]

    def code_of(t):
        return tuple(pick(t, codes[u::TWO]) for u in BOTH)

    def place_of(code):
        run = code // 8
        return run // 4, code % 8, (x + run % 4) % nx

    def xcp(i, u):
        r, j, k = place_of(i)
        return local(xg.at[r, k], xb.at[u], xsem.at[u])

    def zcp(i, u):
        r, j, k = place_of(i)
        return local(zb.at[u], z.at[j, r, k], zsem.at[u])

    def step(i, u):
        r, j, k = place_of(i)
        run = r * nx + k
        c0 = 0
        for width in (sb * 4 // 5, TWO * sb - sb * 4 // 5) if sb % 640 == 0 else (2 * sb,):
            cols = slice(c0, c0 + width)
            zz = lax.dot_general(xb[u], w[j, cols, :], (((1,), (1,)), ((), ())), preferred_element_type=F32)
            zb[u, :, cols] = zz
            blk = min(64, tr)
            for o in range(0, tr, blk):
                rows = slice(o, o + blk)
                m_old = m[run, rows, :]
                parts = [zz[rows, LANES * e : LANES * e + LANES] for e in range(width // LANES)]
                for e in range(width // LANES):
                    at_e = slice(c0 + LANES * e, c0 + LANES * e + LANES)
                    if at_e.stop % sb == 0:
                        end = at_e.stop // sb
                        parts[e] = parts[e] + bias[j, 0:1, LANES * end - LANES : LANES * end]
                        zb[u, rows, at_e] = parts[e]
                mx = m_old
                for part in parts:
                    mx = jnp.maximum(mx, part)
                acc = s[run, rows, :] * jnp.exp(m_old - mx)
                for part in parts:
                    acc = acc + jnp.exp(part - mx)
                m[run, rows, :] = mx
                s[run, rows, :] = acc
            c0 += width

    def stat_copy(r, i):
        sy, k = peers[i]
        rr = 1 - r if sy else r
        return remote(
            stm.at[r], sta.at[sy, x, rr], ssend.at[r, i], srecv.at[sy, x, rr],
            at.dev(x=(x + k) % nx, y=at.far if sy else y),
        )

    def stat_own(r):
        return local(stm.at[r], sta.at[0, x, r], loc.at[3 + r])

    def finish_stats(r):
        lane = lax.broadcasted_iota(jnp.int32, m.shape[1:], 1)
        blk = jnp.zeros(m.shape[1:], F32)
        for d in range(nx):
            mm = m[r * nx + d]
            top_m = jnp.max(mm, axis=1, keepdims=True)
            tot = jnp.sum(s[r * nx + d] * jnp.exp(mm - top_m), axis=1, keepdims=True)
            blk = jnp.where(lane == d, top_m, jnp.where(lane == nx + d, tot, blk))
        stm[r] = blk.T[0:SUB, :]
        for i in range(len(peers)):
            stat_copy(r, i).start()
        stat_own(r).start()

    def w_here(j):
        for f in BOTH:
            pl.when(at.half == f)(w_local(f, j).wait)

        w_own(j).wait_recv()
        w_other(j).wait_recv()
        w_far(j).wait_recv()
        w_core(j).start()

    here_at = (0, 2, 6, 11, 15)
    both_at = (0, 2, 7, 12, 16)

    def body(t, held):
        older, old, now = held
        later = code_of(t + 1)

        @pl.when(t == 0)
        def _():
            for u in BOTH:
                xcp(now[u], u).start()
            x_relay(0, RIGHT).wait_recv()
            x_relay(0, LEFT).wait_recv()

        for j in range(NCH):
            pl.when(t == here_at[j])(functools.partial(w_here, j))
            pl.when(t == both_at[j])(w_core(j).wait_recv)

        @pl.when(t == 1)
        def _():
            x_far.wait_recv()
            x_send(1, RIGHT).start()
            x_send(1, LEFT).start()

        @pl.when(t == 4)
        def _():
            x_send(1, RIGHT).wait_recv()
            x_relay(1, RIGHT).start()
            x_send(1, LEFT).wait_recv()
            x_relay(1, LEFT).start()

        @pl.when(t == 9)
        def _():
            x_relay(1, RIGHT).wait_recv()
            x_relay(1, LEFT).wait_recv()

        @pl.when(t == 16)
        def _():
            local(w, wo, loc.at[5]).start()

        @pl.when(t == 18)
        def _():
            finish_stats(0)

        base = (t % TWO) * 2
        for u in BOTH:
            xcp(now[u], base + u).wait()

        for u in BOTH:
            r, j, k = place_of(now[u])

            @pl.when(j == 0)
            def _():
                cp = xt_out(r * nx + k, u)
                xtb[u] = xb[base + u].T
                cp.start()

        @pl.when(TWO * t + 2 < n_steps)
        def _():
            for u in BOTH:
                xcp(later[u], 2 - base + u).start()

        @pl.when(t > 1)
        def _():
            for u in BOTH:
                zcp(older[u], base + u).wait()

        for u in BOTH:
            step(now[u], base + u)
        for u in BOTH:
            zcp(now[u], base + u).start()
            r, j, k = place_of(now[u])

            @pl.when(j == 0)
            def _():
                xt_out(r * nx + k, u).wait()

        return old, now, later

    none = (jnp.int32(0),) * TWO
    older, old, _ = lax.fori_loop(0, n_steps // TWO, body, (none, none, code_of(jnp.int32(0))))
    finish_stats(1)
    for u in BOTH:
        zcp(older[u], u).wait()
        zcp(old[u], TWO + u).wait()
    local(w, wo, loc.at[5]).wait()
    lab_own.wait()
    stat_own(0).wait()
    stat_own(1).wait()
    for r in BOTH:
        for right_way in (RIGHT, LEFT):
            x_send(r, right_way).wait_send()
            x_relay(r, right_way).wait_send()
    x_far.wait_send()
    for q in range(NCH):
        w_own(q).wait_send()
        w_other(q).wait_send()
        w_far(q).wait_send()
        w_core(q).wait_send()
    for i in range(len(peers)):
        lab_copy(i).wait_send()
        stat_copy(0, i).wait_send()
        stat_copy(1, i).wait_send()
    for sy in BOTH:
        for k in range(nx):
            def arrived():
                remote(lab_hbm, laba.at[sy, k], lsend.at[0], lrecv.at[sy, k], at.dev(c=at.pc)).wait_recv()
                for rr in BOTH:
                    remote(stm.at[rr], sta.at[sy, k, rr], ssend.at[0, 0], srecv.at[sy, k, rr], at.dev(c=at.pc)).wait_recv()

            if sy == 0:
                pl.when(k != x)(arrived)
            else:
                arrived()


def gather_logits(nx, ny, vocab, x, w, lab):
    tr, h = x.shape
    hk = w.shape[1]
    vp = -(-vocab // (TWO * LANES * NCH)) * TWO * LANES * NCH
    ch = vp // NCH
    shape = jax.ShapeDtypeStruct
    dma = pltpu.SemaphoreType.DMA
    vm = pltpu.VMEM
    flops = TWO * TWO * nx * tr * h * vp
    return pl.pallas_call(
        functools.partial(gather_logits_kernel, nx, ny, vocab),
        out_shape=(
            shape((TWO, nx, tr, h), BF16),
            shape((NCH, ch, h), BF16),
            shape((NCH, TWO, nx, tr, ch), F32),
            shape((TWO, nx, TWO, SUB, tr), F32),
            shape((TWO, nx) + lab.shape, jnp.int32),
            shape((nx, h, TWO * tr), BF16),
        ),
        in_specs=[ANY] * 3,
        out_specs=(ANY,) * 6,
        scratch_shapes=[
            vm((NCH, ch, h), BF16), vm((TWO * NCH, ch // TWO, hk), BF16), vm((tr, h), BF16),
            vm((4, tr, h), BF16), vm((4, tr, ch), F32), vm((NCH, SUB, TWO * LANES), F32),
            vm((TWO * nx, tr, LANES), F32), vm((TWO * nx, tr, LANES), F32), vm((TWO, SUB, tr), F32), vm((TWO, h, tr), BF16),
            dma((TWO, 4)), dma((TWO, 4)), dma, dma, dma((3, NCH)), dma((3, NCH)), dma((NCH,)), dma((NCH,)),
            dma((TWO, TWO * nx - 1)), dma((TWO, nx, TWO)), dma((TWO * nx - 1,)), dma((TWO, nx)),
            dma((6,)), dma((NCH,)), dma((4,)), dma((4,)), dma((TWO,)), dma((TWO * NCH,)),
        ],
        compiler_params=pltpu.CompilerParams(
            collective_id=0, has_side_effects=True, vmem_limit_bytes=60 * 2**20
        ),
        cost_estimate=pl.CostEstimate(flops=flops, bytes_accessed=4 * TWO * nx * tr * vp, transcendentals=0),
        name="gather_logits",
    )(x, w, lab)


def grads_kernel(
    nx, ny, inv, vocab, z, w_hbm, xt_hbm, sta_hbm, lab_hbm, dxo, dwo, loss, rx, fx, dd, rr,
    w, xt, zb, gb, acc, dx, st, sta, laba, lacc, tmpa, tmpb, keep, fin, fdx, lbuf,
    wsem, tsem, zsem, xsend, xrecv, fsend, frecv, dsend, drecv, rsend, rrecv, osend, orecv, asem, bsem, lsend, lrecv,
    out_sem, ssem,
):
    at = Place(nx, ny)
    x, y, c = at.x, at.y, at.c
    tr, h = dxo.shape
    ch = zb.shape[2]
    sb = ch // TWO
    slot = NCH * sb
    hk = dwo.shape[1]
    nq = rx.shape[2]
    qr = tr // nq
    left, right = (x + nx - 1) % nx, (x + 1) % nx

    def par(yy, b):
        return jnp.where((yy + b) % TWO == 0, (yy + 1) % ny, (yy + ny - 1) % ny)

    def adj(yy, b):
        return jnp.where((yy + b) % TWO == 0, (yy + ny - 1) % ny, (yy + 1) % ny)

    stats = [local(sta_hbm, sta, ssem.at[0]), local(lab_hbm, laba, ssem.at[1])]
    for cp in stats:
        cp.start()
    local(w_hbm.at[0], w.at[0], wsem.at[0]).start()
    barrier = pltpu.get_barrier_semaphore()
    for k in range(1, nx):
        pl.semaphore_signal(barrier, inc=1, device_id=at.dev(x=(x + k) % nx), device_id_type=MESH)
    for k in range(1, ny):
        pl.semaphore_signal(barrier, inc=1, device_id=at.dev(y=(y + k) % ny), device_id_type=MESH)
        pl.semaphore_signal(barrier, inc=1, device_id=at.dev(y=(y + k) % ny, c=at.pc), device_id_type=MESH)
    pl.semaphore_signal(barrier, inc=1, device_id=at.dev(c=at.pc), device_id_type=MESH)

    segments = ["x0", "w0", "w1", "x1", "w2", "w3", "x2", "x3", "w4"]
    first, after, n_body = {}, {}, 0
    for seg in segments:
        first[seg] = n_body
        n_body += NCH if seg.startswith("x") else nx
        after[seg] = n_body

    def body_at(n):
        code, start = 0, 0
        for seg in segments[1:]:
            here = n >= first[seg]
            code = jnp.where(here, int(seg.startswith("w")) * 8 + int(seg[-1]), code)
            start = jnp.where(here, first[seg], start)
        return code // 8, code % 8, n - start

    def tile(n, u):
        kind, i, k = body_at(n)
        mine = jnp.where(u == 0, (x + TWO * nx - 1 - i) % nx, (x + 1 + i) % nx)
        run = TWO * k + u
        is_x = kind == 0
        return jnp.where(is_x, k, i), jnp.where(is_x, u, run // nx), jnp.where(is_x, mine, run % nx)

    def zcp(n, u, buf):
        j, r, d = tile(n, u)
        return local(z.at[j, r, d], zb.at[buf], zsem.at[buf])

    for u in BOTH:
        zcp(0, u, u).start()
    for j in range(1, NCH):
        local(w_hbm.at[j], w.at[j], wsem.at[j]).start()
    local(xt_hbm, xt, tsem).start()

    for cp in stats:
        cp.wait()
    for r in BOTH:
        parts = [sta[sy, k, r] for sy in BOTH for k in range(nx)]
        top = functools.reduce(jnp.maximum, [part[0:nx] for part in parts])
        tot = sum(part[nx : TWO * nx] * jnp.exp(part[0:nx] - top) for part in parts)
        shift = top + jnp.log(tot) - math.log(inv)
        for d in range(nx):
            col = jnp.full(laba.shape[TWO:], -1, jnp.int32)
            for b in BOTH:
                base = (x * TWO + b) * vocab + half_of(y, b, ny) * slot
                pos = laba[r, d] - base
                room = jnp.where(half_of(y, b, ny) == 0, slot, vocab - slot)
                chunk = sum((pos >= q * sb).astype(jnp.int32) for q in range(1, NCH))
                col = jnp.where((pos >= 0) & (pos < room), chunk * ch + b * sb + pos - chunk * sb, col)
            line = jnp.concatenate([col[o : o + 1].astype(F32) for o in range(tr // LANES)], axis=1)
            rows = jnp.concatenate([shift[d : d + 1], line, jnp.zeros((SUB - TWO, tr), F32)], axis=0)
            st[r * nx + d] = jnp.concatenate([rows] * 16, axis=0).T
    lacc[...] = jnp.zeros_like(lacc)
    pl.semaphore_wait(barrier, nx - 1 + TWO * (ny - 1) + 1)

    def x_copy(s, dr, q):
        return remote(
            dx.at[s % TWO, dr, pl.ds(pl.multiple_of(q * qr, SUB), qr)], rx.at[s, dr, q],
            xsend.at[s, dr, q], xrecv.at[s, dr, q], at.dev(x=left if dr else right),
        )

    def far_copy(q):
        return remote(
            dx.at[1, 1, pl.ds(pl.multiple_of(q * qr, SUB), qr)], fx.at[q], fsend.at[q], frecv.at[q], at.dev(y=at.far)
        )

    def a_load(s, q, dr):
        return local(rx.at[s - 1, dr, q], tmpa.at[q % TWO, dr], asem.at[q % TWO, dr])

    def a_pre(s, q):
        for dr in BOTH:
            x_copy(s - 1, dr, q).wait_recv()
            a_load(s, q, dr).start()

    def a_use(s, q):
        rows = pl.ds(pl.multiple_of(q * qr, SUB), qr)
        for dr in BOTH:
            a_load(s, q, dr).wait()
            dx[s % TWO, dr, rows, :] += tmpa[q % TWO, dr]

        @pl.when(s < nx - 1)
        def _():
            for dr in BOTH:
                x_copy(s, dr, q).start()

        @pl.when(s == nx - 1)
        def _():
            far_copy(q).start()

    def f_load(q):
        return local(fx.at[q], tmpa.at[q % TWO, 0], asem.at[q % TWO, 0])

    def f_out(q):
        return local(fdx.at[q % TWO], dxo.at[pl.ds(pl.multiple_of(q * qr, 16), qr)], out_sem.at[q])

    def f_pre(q):
        far_copy(q).wait_recv()
        f_load(q).start()

    def f_use(q):
        f_load(q).wait()

        @pl.when(q > 1)
        def _():
            f_out(q - 2).wait()

        rows = pl.ds(pl.multiple_of(q * qr, SUB), qr)
        fdx[q % TWO] = (dx[1, 0, rows] + tmpa[q % TWO, 0]).astype(BF16)
        f_out(q).start()

    def lot(b):
        q = (c + b) % TWO
        slices = [(b + TWO * q) % ny, (b + 1 + TWO * q) % ny]
        other = [(b + TWO * (1 - q)) % ny, (b + 1 + TWO * (1 - q)) % ny]
        home = half_of(y, b, ny) == q
        kt = jnp.where(home, y, adj(y, b))
        it = jnp.where(slices[0] == kt, 0, 1)
        return slices, other, kt, it, home

    def rows_of(k):
        return pl.ds(pl.multiple_of(k * hk, 16), hk)

    def d_copy(j, b, i):
        other = lot(b)[1]
        return remote(
            acc.at[j % TWO, rows_of(other[i]), pl.ds(b * sb, sb)], dd.at[j, b, i],
            dsend.at[j, b, i], drecv.at[j, b, i], at.dev(c=at.pc),
        )

    def d_send(j):
        for b in BOTH:
            for i in BOTH:
                d_copy(j, b, i).start()

    def r_load(j, b, i):
        return local(dd.at[j, b, i], tmpb.at[b, i], bsem.at[b, i])

    def r_pre(j):
        for b in BOTH:
            for i in BOTH:
                d_copy(j, b, i).wait_recv()
                r_load(j, b, i).start()

    def r_copy(j, b):
        slices, _, _, it, _ = lot(b)
        kg = jnp.where(it == 0, slices[1], slices[0])
        src = acc.at[j % TWO, rows_of(kg), pl.ds(b * sb, sb)]
        return remote(src, rr.at[j, b], rsend.at[j, b], rrecv.at[j, b], at.dev(y=par(y, b)))

    def r_use(j):
        for b in BOTH:
            slices, _, kt, it, _ = lot(b)
            kg = jnp.where(it == 0, slices[1], slices[0])
            for i in BOTH:
                r_load(j, b, i).wait()

            acc[j % TWO, rows_of(kg), pl.ds(b * sb, sb)] += tmpb[b, 1 - it]
            r_copy(j, b).start()
            keep[j % TWO, b] = acc[j % TWO, rows_of(kt), pl.ds(b * sb, sb)] + tmpb[b, it]

    def s_load(j, b):
        return local(rr.at[j, b], tmpb.at[b, 0], bsem.at[b, 0])

    def s_pre(j):
        for b in BOTH:
            r_copy(j, b).wait_recv()
            s_load(j, b).start()

    def o_copy(j, b):
        kt = lot(b)[2]
        f = half_of(y, b, ny)
        dst = dwo.at[pl.ds(pl.multiple_of(f * slot + j * sb, SUB), sb)]
        return remote(fin.at[b], dst, osend.at[j, b], orecv.at[f, j], at.dev(y=kt, c=b))

    def o_here(j, b):
        f = half_of(y, b, ny)
        dst = dwo.at[pl.ds(pl.multiple_of(f * slot + j * sb, SUB), sb)]
        return local(fin.at[b], dst, orecv.at[f, j])

    def is_here(b):
        return lot(b)[4] & (c == b)

    def s_use(j):
        for b in BOTH:
            s_load(j, b).wait()

            @pl.when((j > 0) & jnp.logical_not(is_here(b)))
            def _():
                o_copy(j - 1, b).wait_send()

            @pl.when((j > 0) & is_here(b))
            def _():
                o_here(j - 1, b).wait()

            fin[b] = (keep[j % TWO, b] + tmpb[b, 0]).T.astype(BF16)

            @pl.when(is_here(b))
            def _():
                o_here(j, b).start()

            @pl.when(jnp.logical_not(is_here(b)))
            def _():
                o_copy(j, b).start()

    def l_copy(stage, k):
        if stage == 0:
            return remote(lbuf.at[0, x], lbuf.at[0, x], lsend.at[0, k], lrecv.at[0, x], at.dev(x=(x + k) % nx))
        if stage == 1:
            return remote(lbuf.at[1, y], lbuf.at[1, y], lsend.at[1, k], lrecv.at[1, y], at.dev(y=(y + k) % ny))
        return remote(lbuf.at[2, c], lbuf.at[2, c], lsend.at[2, 0], lrecv.at[2, c], at.dev(c=at.pc))

    def l_sum(stage, size, me):
        for k in range(size):
            @pl.when(k != me)
            def _():
                remote(
                    lbuf.at[stage, k], lbuf.at[stage, k], lsend.at[stage, 0], lrecv.at[stage, k], at.dev(c=at.pc)
                ).wait_recv()

        total = lbuf[stage, 0]
        for k in range(1, size):
            total = total + lbuf[stage, k]
        return total

    def l_start():
        lbuf[0, x] = -lacc[...]
        for k in range(1, nx):
            l_copy(0, k).start()

    def l_mid():
        lbuf[1, y] = l_sum(0, nx, x)
        for k in range(1, ny):
            l_copy(1, k).start()

    def l_late():
        lbuf[2, c] = l_sum(1, ny, y)
        l_copy(2, 0).start()

    lane = lax.broadcasted_iota(jnp.int32, (min(64, tr), LANES), 1).astype(F32)

    def each_tile(n, u, buf, c0, c1, fn):
        j, r, d = tile(n, u)
        blk = min(64, tr)
        for o in range(0, tr, blk):
            rows = slice(o, o + blk)
            t = st[r * nx + d, rows, :]
            shift = jnp.broadcast_to(t[:, 0:1], (blk, LANES))
            lab = jnp.broadcast_to(t[:, 1:TWO], (blk, LANES)) - (j * ch).astype(F32)
            for e in range(c0 // LANES, c1 // LANES):
                cols = slice(LANES * e, LANES * e + LANES)
                fn(rows, cols, zb[buf, rows, cols] - shift, lane + float(LANES * e) == lab)

    def make_g(n, u, buf, c0, c1, loss_sum=None):
        def one(rows, cols, dist, hit):
            g = jnp.exp(dist)
            gb[u, rows, cols] = jnp.where(hit, g - inv, g).astype(BF16)
            if loss_sum is not None:
                loss_sum.append(jnp.where(hit, dist, 0.0) + (loss_sum.pop() if loss_sum else 0.0))

        each_tile(n, u, buf, c0, c1, one)

    big = ch % (10 * LANES) == 0
    x_cuts = [(ch * e // 5, ch * (e + 1) // 5) for e in range(5)] if big else [(0, ch)]
    w_cuts = [(0, ch // 5), (ch // 5, ch * 3 // 5), (ch * 3 // 5, ch)] if big else [(0, ch)]

    def x_body(n, base):
        _, s, j = body_at(n)
        half = s % TWO

        @pl.when(j == 0)
        def _():
            dx[half] = jnp.zeros(dx.shape[1:], F32)

        for u in BOTH:
            for c0, c1 in x_cuts:
                loss_sum = []
                make_g(n, u, base + u, c0, c1, loss_sum)
                lacc[...] += jnp.sum(loss_sum[0].reshape(-1, SUB, LANES), axis=0)
                dx[half, u] += lax.dot_general(
                    gb[u, :, c0:c1], w[j, c0:c1, :], (((1,), (0,)), ((), ())), preferred_element_type=F32
                )

    def w_body(n, base):
        _, j, k = body_at(n)
        half = j % TWO

        @pl.when(k == 0)
        def _():
            acc[half] = jnp.zeros(acc.shape[1:], F32)

        for c0, c1 in w_cuts:
            for u in BOTH:
                make_g(n, u, base + u, c0, c1)
            acc[half, :, c0:c1] += jnp.dot(
                xt[k], gb[:, :, c0:c1].reshape(TWO * tr, c1 - c0), preferred_element_type=F32
            )

    plan_a = [(after["x1"] + q, 1, q) for q in range(nq)] + [(after["x2"] + q, 2, q) for q in range(nq)]
    plan_a += [(after["x3"] + 3 * q, 3, q) for q in range(nq)]
    plan_r = [(11, 12, 0), (15, 16, 1), (24, 25, 2), (28, 29, 3), (42, 43, 4)]
    plan_s = [(17, 18, 0), (21, 22, 1), (30, 31, 2), (34, 35, 3), (46, 47, 4)]
    pre_r, use_r = [(p, j) for p, _, j in plan_r], [(u, j) for _, u, j in plan_r]
    pre_s, use_s = [(p, j) for p, _, j in plan_s], [(u, j) for _, u, j in plan_s]
    plan_f = [(41, 0), (44, 1), (46, 2), (48, 3)]
    n_all = n_body + TWO * nq + 1

    def when(n, table, fn):
        table = [(e[0], e[1:]) for e in table]
        hit = functools.reduce(lambda p, q: p | q, [n == e for e, _ in table])

        @pl.when(hit)
        def _():
            args = []
            for i in range(len(table[0][1])):
                val = 0
                for e, vals in table:
                    if vals[i]:
                        val = val + jnp.where(n == e, vals[i], 0)
                args.append(val + jnp.int32(0))
            fn(*args)

    def body(n, _):
        @pl.when(n < NCH)
        def _():
            local(w_hbm.at[n], w.at[n], wsem.at[n]).wait()

        @pl.when(n == first["w0"])
        def _():
            local(xt_hbm, xt, tsem).wait()
            for q in range(nq):
                for dr in BOTH:
                    x_copy(0, dr, q).start()

        when(n, [(after["w%d" % j], j) for j in range(NCH)], d_send)
        when(n, plan_a, a_use)
        when(n, plan_f, f_use)
        when(n, use_r, r_use)
        when(n, use_s, s_use)
        when(n, [(e[0] - 1,) + e[1:] for e in plan_a], a_pre)
        when(n, [(e[0] - 1,) + e[1:] for e in plan_f], f_pre)
        when(n, pre_r, r_pre)
        when(n, pre_s, s_pre)

        for at_n, fn in ((n_body, l_start), (n_body + TWO, l_mid), (n_body + nq, l_late)):
            pl.when(n == at_n)(fn)

        @pl.when((n == first["x2"]) | (n == first["x3"]))
        def _():
            s = jnp.where(n == first["x2"], 0, 1)
            for q in range(nq):
                for dr in BOTH:
                    x_copy(s, dr, q).wait_send()

        for j in range(2, NCH):
            @pl.when(n == first["w%d" % j])
            def _():
                for b in BOTH:
                    r_copy(j - 2, b).wait_send()
                    for i in BOTH:
                        d_copy(j - 2, b, i).wait_send()

        base = (n % TWO) * 2

        @pl.when(n < n_body)
        def _():
            for u in BOTH:
                zcp(n, u, base + u).wait()

            @pl.when(n + 1 < n_body)
            def _():
                for u in BOTH:
                    zcp(n + 1, u, 2 - base + u).start()

            kind = body_at(n)[0]

            @pl.when(kind == 0)
            def _():
                x_body(n, base)

            @pl.when(kind == 1)
            def _():
                w_body(n, base)

        return 0

    lax.fori_loop(0, n_all, body, 0)
    loss[...] = l_sum(2, TWO, c)

    for q in range(nq):
        if q >= nq - 2:
            f_out(q).wait()
        far_copy(q).wait_send()
        for dr in BOTH:
            x_copy(2, dr, q).wait_send()
    for b in BOTH:
        for j in range(NCH - 2, NCH):
            for i in BOTH:
                d_copy(j, b, i).wait_send()
            r_copy(j, b).wait_send()

        @pl.when(is_here(b))
        def _():
            o_here(NCH - 1, b).wait()

        @pl.when(jnp.logical_not(is_here(b)))
        def _():
            o_copy(NCH - 1, b).wait_send()

    q0 = half_of(y, c, ny)
    for f in BOTH:
        kept = (f == q0) & ((q0 + c) % TWO == c)

        @pl.when(jnp.logical_not(kept))
        def _():
            for j in range(NCH):
                dst = dwo.at[pl.ds(f * slot + j * sb, sb)]
                remote(fin.at[0], dst, osend.at[j, 0], orecv.at[f, j], at.dev(c=at.pc)).wait_recv()

    for k in range(1, nx):
        l_copy(0, k).wait_send()
    for k in range(1, ny):
        l_copy(1, k).wait_send()
    l_copy(2, 0).wait_send()


def grads(nx, ny, inv, vocab, z, w, xt, sta, laba, hk):
    ch, h = w.shape[1:]
    tr = z.shape[3]
    nq = 4
    shape = jax.ShapeDtypeStruct
    dma = pltpu.SemaphoreType.DMA
    vm = pltpu.VMEM
    vspec = pl.BlockSpec(memory_space=pltpu.VMEM)
    sb, qr = ch // TWO, tr // nq
    return pl.pallas_call(
        functools.partial(grads_kernel, nx, ny, inv, vocab),
        out_shape=(
            shape((tr, h), BF16), shape((NCH * ch, hk), BF16), shape((SUB, LANES), F32),
            shape((nx - 1, TWO, nq, qr, h), F32), shape((nq, qr, h), F32),
            shape((NCH, TWO, TWO, hk, sb), F32), shape((NCH, TWO, hk, sb), F32),
        ),
        in_specs=[ANY] * 5,
        out_specs=(ANY, ANY, vspec, ANY, ANY, ANY, ANY),
        scratch_shapes=[
            vm((NCH, ch, h), BF16), vm((nx, h, TWO * tr), BF16), vm((4, tr, ch), F32), vm((TWO, tr, ch), BF16),
            vm((TWO, h, ch), F32), vm((TWO, TWO, tr, h), F32), vm((TWO * nx, tr, LANES), F32), vm(sta.shape, F32), vm(laba.shape, jnp.int32), vm((SUB, LANES), F32),
            vm((TWO, TWO, qr, h), F32), vm((TWO, TWO, hk, sb), F32), vm((TWO, TWO, hk, sb), F32),
            vm((TWO, sb, hk), BF16), vm((TWO, qr, h), BF16), vm((3, max(nx, ny), SUB, LANES), F32),
            dma((NCH,)), dma, dma((4,)), dma((nx - 1, TWO, nq)), dma((nx - 1, TWO, nq)), dma((nq,)), dma((nq,)),
            dma((NCH, TWO, TWO)), dma((NCH, TWO, TWO)), dma((NCH, TWO)), dma((NCH, TWO)), dma((NCH, TWO)), dma((TWO, NCH)),
            dma((TWO, TWO)), dma((TWO, TWO)), dma((3, max(nx, ny))), dma((3, max(nx, ny))), dma((nq,)), dma((TWO,)),
        ],
        compiler_params=pltpu.CompilerParams(
            collective_id=1, has_side_effects=True, vmem_limit_bytes=67_000_000
        ),
        name="grads",
    )(z, w, xt, sta, laba)


def solution(mesh):
    ny = mesh.shape["fsdp"]
    tp_size = mesh.shape["tp"]
    nx = tp_size // TWO
    token_spec = P(("dp", "fsdp", "tp"), None)
    label_spec = P(("dp", "fsdp", "tp"))

    def local_step(hidden, w_head, labels):
        tr, h = hidden.shape
        hk, vocab = w_head.shape
        inv = 1.0 / (tr * tp_size * ny)
        lab = labels.reshape(-1, LANES)
        xg, wg, z, sta, laba, xt = gather_logits(nx, ny, vocab, hidden, w_head.T, lab)
        d_hidden, d_w, loss = grads(nx, ny, inv, vocab, z, wg, xt, sta, laba, hk)[:3]
        mean_loss = jnp.sum(loss) * inv + math.log(inv)
        return mean_loss.reshape(1), d_hidden, d_w[:vocab].T

    return jax.shard_map(
        local_step,
        mesh=mesh,
        in_specs=(token_spec, P("fsdp", "tp"), label_spec),
        out_specs=(P("dp"), token_spec, P(("dp", "fsdp"), "tp")),
        check_vma=False,
    )
```

```python
import functools
import math

import jax
import jax.numpy as jnp
from jax import lax
from jax.experimental import pallas as pl
from jax.experimental.pallas import tpu as pltpu
from jax.sharding import PartitionSpec as P

MESH = pl.DeviceIdType.MESH
F32 = jnp.float32
BF16 = jnp.bfloat16
NCH = 5
LOW = -1e30
ANY = pl.BlockSpec(memory_space=pl.ANY)
LANES = 128
SUB = 8
TWO = 2
BOTH = range(TWO)
RIGHT, LEFT = True, False


class Place:
    def __init__(self, nx, ny):
        tp = lax.axis_index("tp")
        self.nx, self.ny = nx, ny
        self.x, self.c, self.y = tp // TWO, tp % TWO, lax.axis_index("fsdp")
        up, down = (self.y + 1) % ny, (self.y + ny - 1) % ny
        even = (self.y + self.c) % TWO == 0
        self.up, self.down = up, down
        self.pc = 1 - self.c
        self.p = jnp.where(even, up, down)
        self.a = jnp.where(even, down, up)
        self.far = (self.y + 2) % ny
        self.half = ((self.y - self.c + ny) % ny) // TWO

    def dev(self, x=None, y=None, c=None):
        x = self.x if x is None else x
        y = self.y if y is None else y
        c = self.c if c is None else c
        return {"fsdp": y, "tp": x * 2 + c}


def half_of(y, b, ny):
    return ((y - b + ny) % ny) // TWO


def pick(n, table):
    out = 0
    for i, v in enumerate(table):
        if v:
            out = out + jnp.where(n == i, v, 0)
    return out


def remote(src, dst, ssem, rsem, dev):
    return pltpu.make_async_remote_copy(
        src_ref=src, dst_ref=dst, send_sem=ssem, recv_sem=rsem, device_id=dev, device_id_type=MESH
    )


def local(src, dst, sem):
    return pltpu.make_async_copy(src, dst, sem)


def gather_logits_kernel(
    nx, ny, vocab,
    x_hbm, w_hbm, lab_hbm, xg, wo, z, sta, laba, xt,
    w, wsrc, xown, xb, zb, bias, m, s, stm, xtb,
    xsend, xrecv, ysend, yrecv, wsend, wrecv, dsend, drecv, ssend, srecv, lsend, lrecv, loc, wloc, xsem, zsem, tsem, wload,
):
    at = Place(nx, ny)
    x, y, c = at.x, at.y, at.c
    tr = xown.shape[0]
    hk = w_hbm.shape[1]
    sb = w.shape[1] // TWO
    slot = NCH * sb
    left, right = (x + nx - 1) % nx, (x + 1) % nx
    top, bot = pl.ds(0, tr // TWO), pl.ds(tr // TWO, tr // TWO)

    def rows_in(f, q):
        return min(sb, vocab - f * slot - q * sb)

    def w_load(f, q):
        n = rows_in(f, q)
        src = w_hbm.at[pl.ds(f * slot + q * sb, n)]
        return local(src, wsrc.at[f * NCH + q, pl.ds(0, n)], wload.at[f * NCH + q])

    def preload():
        for q in range(NCH):
            for f in BOTH:
                w_load(f, q).start()

    barrier = pltpu.get_barrier_semaphore()
    for k in range(1, nx):
        pl.semaphore_signal(barrier, inc=1, device_id=at.dev(x=(x + k) % nx), device_id_type=MESH)
    for k in range(nx):
        pl.semaphore_signal(barrier, inc=1, device_id=at.dev(x=(x + k) % nx, y=at.far), device_id_type=MESH)
    pl.semaphore_signal(barrier, inc=1, device_id=at.dev(y=at.up), device_id_type=MESH)
    pl.semaphore_signal(barrier, inc=1, device_id=at.dev(y=at.down), device_id_type=MESH)
    pl.semaphore_signal(barrier, inc=1, device_id=at.dev(c=at.pc), device_id_type=MESH)
    load_x = local(x_hbm, xown, loc.at[0])
    load_x.start()
    preload()
    pl.semaphore_wait(barrier, TWO * nx + 2)
    load_x.wait()

    def x_send(r, to_right):
        i = 0 if to_right else 1
        src = xown if r == 0 else xg.at[1, x]
        return remote(src, xg.at[r, x], xsend.at[r, i], xrecv.at[r, i], at.dev(x=right if to_right else left))

    def x_relay(r, to_right):
        if to_right:
            part = xg.at[r, left, top]
            return remote(part, part, xsend.at[r, 2], xrecv.at[r, 2], at.dev(x=right))
        part = xg.at[r, right, bot]
        return remote(part, part, xsend.at[r, 3], xrecv.at[r, 3], at.dev(x=left))

    x_far = remote(xown, xg.at[1, x], ysend, yrecv, at.dev(y=at.far))
    keep_x = local(xown, xg.at[0, x], loc.at[1])

    blocks = [(f, q) for f in BOTH for q in range(NCH)]

    def w_src(f, q):
        return wsrc.at[f * NCH + q]

    def w_dst(k, q):
        return w.at[q, pl.ds(pl.multiple_of(c * sb, SUB), sb), pl.ds(pl.multiple_of(k * hk, LANES), hk)]

    def w_own(q):
        return remote(w_src(at.half, q), w_dst(y, q), wsend.at[0, q], wrecv.at[0, q], at.dev(y=at.p))

    def w_other(q):
        return remote(w_src(1 - at.half, q), w_dst(y, q), wsend.at[1, q], wrecv.at[1, q], at.dev(y=at.a))

    def w_far(q):
        return remote(w_src(1 - at.half, q), w_dst(y, q), wsend.at[2, q], wrecv.at[2, q], at.dev(y=at.far))

    def w_core(q):
        part = w.at[q, pl.ds(pl.multiple_of(c * sb, SUB), sb)]
        return remote(part, part, dsend.at[q], drecv.at[q], at.dev(c=at.pc))

    def w_local(f, q):
        n = rows_in(f, q)
        dst = w.at[q, pl.ds(pl.multiple_of(c * sb, SUB), n), pl.ds(pl.multiple_of(y * hk, LANES), hk)]
        return local(w_hbm.at[pl.ds(f * slot + q * sb, n)], dst, wloc.at[q])

    def w_out(q):
        w_own(q).start()
        w_other(q).start()
        w_far(q).start()

    x_send(0, RIGHT).start()
    x_send(0, LEFT).start()
    for q in range(NCH):
        for f in BOTH:
            w_load(f, q).wait()
            if rows_in(f, q) < sb:
                pad = sb - rows_in(f, q)
                wsrc[f * NCH + q, sb - pad :, :] = jnp.zeros((pad, hk), BF16)
        w_out(q)
        if q == 0:
            x_far.start()
    keep_x.start()
    for f, q in blocks:
        @pl.when(at.half == f)
        def _():
            w_local(f, q).start()
            if rows_in(f, q) < sb:
                pad = sb - rows_in(f, q)
                at_row = pl.multiple_of(c * sb + sb - pad, SUB)
                w[q, pl.ds(at_row, pad), pl.ds(pl.multiple_of(y * hk, LANES), hk)] = jnp.zeros((pad, hk), BF16)

    peers = [(0, k) for k in range(1, nx)] + [(1, k) for k in range(nx)]

    def lab_copy(i):
        sy, k = peers[i]
        return remote(
            lab_hbm, laba.at[sy, x], lsend.at[i], lrecv.at[sy, x],
            at.dev(x=(x + k) % nx, y=at.far if sy else y),
        )

    for i in range(len(peers)):
        lab_copy(i).start()
    lab_own = local(lab_hbm, laba.at[0, x], loc.at[2])
    lab_own.start()

    tail = lax.broadcasted_iota(jnp.int32, bias.shape[1:], 1)
    slot_of = tail // LANES
    pos = slot - LANES + tail - slot_of * LANES
    half_b = jnp.where(slot_of == 0, half_of(y, 0, ny), half_of(y, 1, ny))
    bias[...] = jnp.zeros_like(bias)
    bias[NCH - 1] = jnp.where((half_b == 1) & (pos >= vocab - slot), LOW, 0.0)
    m[...] = jnp.full_like(m, -3e38)
    s[...] = jnp.zeros_like(s)

    def xt_out(run, u):
        return local(
            xtb.at[u], xt.at[run // TWO, :, pl.ds(pl.multiple_of((run % TWO) * tr, LANES), tr)], tsem.at[u]
        )

    keep_x.wait()
    x_send(0, RIGHT).wait_recv()
    x_relay(0, RIGHT).start()
    x_send(0, LEFT).wait_recv()
    x_relay(0, LEFT).start()

    n_steps = TWO * nx * NCH

    near = (0, 3, 1, 2)
    order = [(0, k, 0) for k in near] + [(1, 0, 0)]
    order += [(0, k, 1) for k in near] + [(1, 0, 1)]
    order += [(1, k, j) for j in BOTH for k in (3, 1)]
    order += [(0, k, 2) for k in near] + [(1, k, 2) for k in (0, 3, 1)] + [(1, 2, j) for j in range(3)]
    order += [(r, k, j) for j in (3, 4) for r in BOTH for k in near]
    codes = [(r * 4 + k) * 8 + j for r, k, j in order]

    def code_of(t):
        return tuple(pick(t, codes[u::TWO]) for u in BOTH)

    def place_of(code):
        run = code // 8
        return run // 4, code % 8, (x + run % 4) % nx

    def xcp(i, u):
        r, j, k = place_of(i)
        return local(xg.at[r, k], xb.at[u], xsem.at[u])

    def zcp(i, u):
        r, j, k = place_of(i)
        return local(zb.at[u], z.at[j, r, k], zsem.at[u])

    def step(i, u):
        r, j, k = place_of(i)
        run = r * nx + k
        c0 = 0
        for width in (sb * 2 // 5, sb * 4 // 5, sb * 4 // 5) if sb % 640 == 0 else (2 * sb,):
            cols = slice(c0, c0 + width)
            zz = lax.dot_general(xb[u], w[j, cols, :], (((1,), (1,)), ((), ())), preferred_element_type=F32)
            zb[u, :, cols] = zz
            blk = min(64, tr)
            for o in range(0, tr, blk):
                rows = slice(o, o + blk)
                m_old = m[run, rows, :]
                parts = [zz[rows, LANES * e : LANES * e + LANES] for e in range(width // LANES)]
                for e in range(width // LANES):
                    at_e = slice(c0 + LANES * e, c0 + LANES * e + LANES)
                    if at_e.stop % sb == 0:
                        end = at_e.stop // sb
                        parts[e] = parts[e] + bias[j, 0:1, LANES * end - LANES : LANES * end]
                        zb[u, rows, at_e] = parts[e]
                mx = m_old
                for part in parts:
                    mx = jnp.maximum(mx, part)
                acc = s[run, rows, :] * jnp.exp(m_old - mx)
                for part in parts:
                    acc = acc + jnp.exp(part - mx)
                m[run, rows, :] = mx
                s[run, rows, :] = acc
            c0 += width

    def stat_copy(r, i):
        sy, k = peers[i]
        rr = 1 - r if sy else r
        return remote(
            stm.at[r], sta.at[sy, x, rr], ssend.at[r, i], srecv.at[sy, x, rr],
            at.dev(x=(x + k) % nx, y=at.far if sy else y),
        )

    def stat_own(r):
        return local(stm.at[r], sta.at[0, x, r], loc.at[3 + r])

    def finish_stats(r):
        lane = lax.broadcasted_iota(jnp.int32, m.shape[1:], 1)
        blk = jnp.zeros(m.shape[1:], F32)
        for d in range(nx):
            mm = m[r * nx + d]
            top_m = jnp.max(mm, axis=1, keepdims=True)
            tot = jnp.sum(s[r * nx + d] * jnp.exp(mm - top_m), axis=1, keepdims=True)
            blk = jnp.where(lane == d, top_m, jnp.where(lane == nx + d, tot, blk))
        stm[r] = blk.T[0:SUB, :]
        for i in range(len(peers)):
            stat_copy(r, i).start()
        stat_own(r).start()

    def w_here(j):
        for f in BOTH:
            pl.when(at.half == f)(w_local(f, j).wait)

        w_own(j).wait_recv()
        w_other(j).wait_recv()
        w_far(j).wait_recv()
        w_core(j).start()

    here_at = (0, 2, 6, 11, 15)
    both_at = (0, 2, 7, 12, 16)

    def body(t, held):
        older, old, now = held
        later = code_of(t + 1)

        @pl.when(t == 0)
        def _():
            for u in BOTH:
                xcp(now[u], u).start()
            x_relay(0, RIGHT).wait_recv()
            x_relay(0, LEFT).wait_recv()

        for j in range(NCH):
            pl.when(t == here_at[j])(functools.partial(w_here, j))
            pl.when(t == both_at[j])(w_core(j).wait_recv)

        @pl.when(t == 1)
        def _():
            x_far.wait_recv()
            x_send(1, RIGHT).start()
            x_send(1, LEFT).start()

        @pl.when(t == 4)
        def _():
            x_send(1, RIGHT).wait_recv()
            x_relay(1, RIGHT).start()
            x_send(1, LEFT).wait_recv()
            x_relay(1, LEFT).start()

        @pl.when(t == 9)
        def _():
            x_relay(1, RIGHT).wait_recv()
            x_relay(1, LEFT).wait_recv()

        @pl.when(t == 16)
        def _():
            local(w, wo, loc.at[5]).start()

        @pl.when(t == 18)
        def _():
            finish_stats(0)

        base = (t % TWO) * 2
        for u in BOTH:
            xcp(now[u], base + u).wait()

        for u in BOTH:
            r, j, k = place_of(now[u])

            @pl.when(j == 0)
            def _():
                cp = xt_out(r * nx + k, u)
                xtb[u] = xb[base + u].T
                cp.start()

        @pl.when(TWO * t + 2 < n_steps)
        def _():
            for u in BOTH:
                xcp(later[u], 2 - base + u).start()

        @pl.when(t > 1)
        def _():
            for u in BOTH:
                zcp(older[u], base + u).wait()

        for u in BOTH:
            step(now[u], base + u)
        for u in BOTH:
            zcp(now[u], base + u).start()
            r, j, k = place_of(now[u])

            @pl.when(j == 0)
            def _():
                xt_out(r * nx + k, u).wait()

        return old, now, later

    none = (jnp.int32(0),) * TWO
    older, old, _ = lax.fori_loop(0, n_steps // TWO, body, (none, none, code_of(jnp.int32(0))))
    finish_stats(1)
    for u in BOTH:
        zcp(older[u], u).wait()
        zcp(old[u], TWO + u).wait()
    local(w, wo, loc.at[5]).wait()
    lab_own.wait()
    stat_own(0).wait()
    stat_own(1).wait()
    for r in BOTH:
        for right_way in (RIGHT, LEFT):
            x_send(r, right_way).wait_send()
            x_relay(r, right_way).wait_send()
    x_far.wait_send()
    for q in range(NCH):
        w_own(q).wait_send()
        w_other(q).wait_send()
        w_far(q).wait_send()
        w_core(q).wait_send()
    for i in range(len(peers)):
        lab_copy(i).wait_send()
        stat_copy(0, i).wait_send()
        stat_copy(1, i).wait_send()
    for sy in BOTH:
        for k in range(nx):
            def arrived():
                remote(lab_hbm, laba.at[sy, k], lsend.at[0], lrecv.at[sy, k], at.dev(c=at.pc)).wait_recv()
                for rr in BOTH:
                    remote(stm.at[rr], sta.at[sy, k, rr], ssend.at[0, 0], srecv.at[sy, k, rr], at.dev(c=at.pc)).wait_recv()

            if sy == 0:
                pl.when(k != x)(arrived)
            else:
                arrived()


def gather_logits(nx, ny, vocab, x, w, lab):
    tr, h = x.shape
    hk = w.shape[1]
    vp = -(-vocab // (TWO * LANES * NCH)) * TWO * LANES * NCH
    ch = vp // NCH
    shape = jax.ShapeDtypeStruct
    dma = pltpu.SemaphoreType.DMA
    vm = pltpu.VMEM
    flops = TWO * TWO * nx * tr * h * vp
    return pl.pallas_call(
        functools.partial(gather_logits_kernel, nx, ny, vocab),
        out_shape=(
            shape((TWO, nx, tr, h), BF16),
            shape((NCH, ch, h), BF16),
            shape((NCH, TWO, nx, tr, ch), F32),
            shape((TWO, nx, TWO, SUB, tr), F32),
            shape((TWO, nx) + lab.shape, jnp.int32),
            shape((nx, h, TWO * tr), BF16),
        ),
        in_specs=[ANY] * 3,
        out_specs=(ANY,) * 6,
        scratch_shapes=[
            vm((NCH, ch, h), BF16), vm((TWO * NCH, ch // TWO, hk), BF16), vm((tr, h), BF16),
            vm((4, tr, h), BF16), vm((4, tr, ch), F32), vm((NCH, SUB, TWO * LANES), F32),
            vm((TWO * nx, tr, LANES), F32), vm((TWO * nx, tr, LANES), F32), vm((TWO, SUB, tr), F32), vm((TWO, h, tr), BF16),
            dma((TWO, 4)), dma((TWO, 4)), dma, dma, dma((3, NCH)), dma((3, NCH)), dma((NCH,)), dma((NCH,)),
            dma((TWO, TWO * nx - 1)), dma((TWO, nx, TWO)), dma((TWO * nx - 1,)), dma((TWO, nx)),
            dma((6,)), dma((NCH,)), dma((4,)), dma((4,)), dma((TWO,)), dma((TWO * NCH,)),
        ],
        compiler_params=pltpu.CompilerParams(
            collective_id=0, has_side_effects=True, vmem_limit_bytes=60 * 2**20,
        ),
        cost_estimate=pl.CostEstimate(flops=flops, bytes_accessed=4 * TWO * nx * tr * vp, transcendentals=0),
        name="gather_logits",
    )(x, w, lab)


def grads_kernel(
    nx, ny, inv, vocab, z, w_hbm, xt_hbm, sta_hbm, lab_hbm, dxo, dwo, loss, rx, fx, dd, rr,
    w, xt, zb, gb, acc, dx, st, sta, laba, lacc, tmpa, tmpb, keep, fin, fdx, lbuf,
    wsem, tsem, zsem, xsend, xrecv, fsend, frecv, dsend, drecv, rsend, rrecv, osend, orecv, asem, bsem, lsend, lrecv,
    out_sem, ssem,
):
    at = Place(nx, ny)
    x, y, c = at.x, at.y, at.c
    tr, h = dxo.shape
    ch = zb.shape[2]
    sb = ch // TWO
    slot = NCH * sb
    hk = dwo.shape[1]
    nq = rx.shape[2]
    qr = tr // nq
    left, right = (x + nx - 1) % nx, (x + 1) % nx

    def par(yy, b):
        return jnp.where((yy + b) % TWO == 0, (yy + 1) % ny, (yy + ny - 1) % ny)

    def adj(yy, b):
        return jnp.where((yy + b) % TWO == 0, (yy + ny - 1) % ny, (yy + 1) % ny)

    stats = [local(sta_hbm, sta, ssem.at[0]), local(lab_hbm, laba, ssem.at[1])]
    for cp in stats:
        cp.start()
    local(w_hbm.at[0], w.at[0], wsem.at[0]).start()
    barrier = pltpu.get_barrier_semaphore()
    for k in range(1, nx):
        pl.semaphore_signal(barrier, inc=1, device_id=at.dev(x=(x + k) % nx), device_id_type=MESH)
    for k in range(1, ny):
        pl.semaphore_signal(barrier, inc=1, device_id=at.dev(y=(y + k) % ny), device_id_type=MESH)
        pl.semaphore_signal(barrier, inc=1, device_id=at.dev(y=(y + k) % ny, c=at.pc), device_id_type=MESH)
    pl.semaphore_signal(barrier, inc=1, device_id=at.dev(c=at.pc), device_id_type=MESH)

    segments = ["x0", "w0", "w1", "x1", "w2", "w3", "x2", "x3", "w4"]
    first, after, n_body = {}, {}, 0
    for seg in segments:
        first[seg] = n_body
        n_body += NCH if seg.startswith("x") else nx
        after[seg] = n_body

    def body_at(n):
        code, start = 0, 0
        for seg in segments[1:]:
            here = n >= first[seg]
            code = jnp.where(here, int(seg.startswith("w")) * 8 + int(seg[-1]), code)
            start = jnp.where(here, first[seg], start)
        return code // 8, code % 8, n - start

    def tile(n, u):
        kind, i, k = body_at(n)
        mine = jnp.where(u == 0, (x + TWO * nx - 1 - i) % nx, (x + 1 + i) % nx)
        run = TWO * k + u
        is_x = kind == 0
        return jnp.where(is_x, k, i), jnp.where(is_x, u, run // nx), jnp.where(is_x, mine, run % nx)

    def zcp(n, u, buf):
        j, r, d = tile(n, u)
        return local(z.at[j, r, d], zb.at[buf], zsem.at[buf])

    for u in BOTH:
        zcp(0, u, u).start()
    for j in range(1, NCH):
        local(w_hbm.at[j], w.at[j], wsem.at[j]).start()
    local(xt_hbm, xt, tsem).start()

    for cp in stats:
        cp.wait()
    for r in BOTH:
        parts = [sta[sy, k, r] for sy in BOTH for k in range(nx)]
        top = functools.reduce(jnp.maximum, [part[0:nx] for part in parts])
        tot = sum(part[nx : TWO * nx] * jnp.exp(part[0:nx] - top) for part in parts)
        shift = top + jnp.log(tot) - math.log(inv)
        for d in range(nx):
            col = jnp.full(laba.shape[TWO:], -1, jnp.int32)
            for b in BOTH:
                base = (x * TWO + b) * vocab + half_of(y, b, ny) * slot
                pos = laba[r, d] - base
                room = jnp.where(half_of(y, b, ny) == 0, slot, vocab - slot)
                chunk = sum((pos >= q * sb).astype(jnp.int32) for q in range(1, NCH))
                col = jnp.where((pos >= 0) & (pos < room), chunk * ch + b * sb + pos - chunk * sb, col)
            line = jnp.concatenate([col[o : o + 1].astype(F32) for o in range(tr // LANES)], axis=1)
            rows = jnp.concatenate([shift[d : d + 1], line, jnp.zeros((SUB - TWO, tr), F32)], axis=0)
            st[r * nx + d] = jnp.concatenate([rows] * 16, axis=0).T
    lacc[...] = jnp.zeros_like(lacc)
    pl.semaphore_wait(barrier, nx - 1 + TWO * (ny - 1) + 1)

    def x_copy(s, dr, q):
        return remote(
            dx.at[s % TWO, dr, pl.ds(pl.multiple_of(q * qr, SUB), qr)], rx.at[s, dr, q],
            xsend.at[s, dr, q], xrecv.at[s, dr, q], at.dev(x=left if dr else right),
        )

    def far_copy(q):
        return remote(
            dx.at[1, 1, pl.ds(pl.multiple_of(q * qr, SUB), qr)], fx.at[q], fsend.at[q], frecv.at[q], at.dev(y=at.far)
        )

    def a_load(s, q, dr):
        return local(rx.at[s - 1, dr, q], tmpa.at[q % TWO, dr], asem.at[q % TWO, dr])

    def a_pre(s, q):
        for dr in BOTH:
            x_copy(s - 1, dr, q).wait_recv()
            a_load(s, q, dr).start()

    def a_use(s, q):
        rows = pl.ds(pl.multiple_of(q * qr, SUB), qr)
        for dr in BOTH:
            a_load(s, q, dr).wait()
            dx[s % TWO, dr, rows, :] += tmpa[q % TWO, dr]

        @pl.when(s < nx - 1)
        def _():
            for dr in BOTH:
                x_copy(s, dr, q).start()

        @pl.when(s == nx - 1)
        def _():
            far_copy(q).start()

    def f_load(q):
        return local(fx.at[q], tmpa.at[q % TWO, 0], asem.at[q % TWO, 0])

    def f_out(q):
        return local(fdx.at[q % TWO], dxo.at[pl.ds(pl.multiple_of(q * qr, 16), qr)], out_sem.at[q])

    def f_pre(q):
        far_copy(q).wait_recv()
        f_load(q).start()

    def f_use(q):
        f_load(q).wait()

        @pl.when(q > 1)
        def _():
            f_out(q - 2).wait()

        rows = pl.ds(pl.multiple_of(q * qr, SUB), qr)
        fdx[q % TWO] = (dx[1, 0, rows] + tmpa[q % TWO, 0]).astype(BF16)
        f_out(q).start()

    def lot(b):
        q = (c + b) % TWO
        slices = [(b + TWO * q) % ny, (b + 1 + TWO * q) % ny]
        other = [(b + TWO * (1 - q)) % ny, (b + 1 + TWO * (1 - q)) % ny]
        home = half_of(y, b, ny) == q
        kt = jnp.where(home, y, adj(y, b))
        it = jnp.where(slices[0] == kt, 0, 1)
        return slices, other, kt, it, home

    def rows_of(k):
        return pl.ds(pl.multiple_of(k * hk, 16), hk)

    def d_copy(j, b, i):
        other = lot(b)[1]
        return remote(
            acc.at[j % TWO, rows_of(other[i]), pl.ds(b * sb, sb)], dd.at[j, b, i],
            dsend.at[j, b, i], drecv.at[j, b, i], at.dev(c=at.pc),
        )

    def d_send(j):
        for b in BOTH:
            for i in BOTH:
                d_copy(j, b, i).start()

    def r_load(j, b, i):
        return local(dd.at[j, b, i], tmpb.at[b, i], bsem.at[b, i])

    def r_pre(j):
        for b in BOTH:
            for i in BOTH:
                d_copy(j, b, i).wait_recv()
                r_load(j, b, i).start()

    def r_copy(j, b):
        slices, _, _, it, _ = lot(b)
        kg = jnp.where(it == 0, slices[1], slices[0])
        src = acc.at[j % TWO, rows_of(kg), pl.ds(b * sb, sb)]
        return remote(src, rr.at[j, b], rsend.at[j, b], rrecv.at[j, b], at.dev(y=par(y, b)))

    def r_use(j):
        for b in BOTH:
            slices, _, kt, it, _ = lot(b)
            kg = jnp.where(it == 0, slices[1], slices[0])
            for i in BOTH:
                r_load(j, b, i).wait()

            acc[j % TWO, rows_of(kg), pl.ds(b * sb, sb)] += tmpb[b, 1 - it]
            r_copy(j, b).start()
            keep[j % TWO, b] = acc[j % TWO, rows_of(kt), pl.ds(b * sb, sb)] + tmpb[b, it]

    def s_load(j, b):
        return local(rr.at[j, b], tmpb.at[b, 0], bsem.at[b, 0])

    def s_pre(j):
        for b in BOTH:
            r_copy(j, b).wait_recv()
            s_load(j, b).start()

    def o_copy(j, b):
        kt = lot(b)[2]
        f = half_of(y, b, ny)
        dst = dwo.at[pl.ds(pl.multiple_of(f * slot + j * sb, SUB), sb)]
        return remote(fin.at[b], dst, osend.at[j, b], orecv.at[f, j], at.dev(y=kt, c=b))

    def o_here(j, b):
        f = half_of(y, b, ny)
        dst = dwo.at[pl.ds(pl.multiple_of(f * slot + j * sb, SUB), sb)]
        return local(fin.at[b], dst, orecv.at[f, j])

    def is_here(b):
        return lot(b)[4] & (c == b)

    def s_use(j):
        for b in BOTH:
            s_load(j, b).wait()

            @pl.when((j > 0) & jnp.logical_not(is_here(b)))
            def _():
                o_copy(j - 1, b).wait_send()

            @pl.when((j > 0) & is_here(b))
            def _():
                o_here(j - 1, b).wait()

            fin[b] = (keep[j % TWO, b] + tmpb[b, 0]).T.astype(BF16)

            @pl.when(is_here(b))
            def _():
                o_here(j, b).start()

            @pl.when(jnp.logical_not(is_here(b)))
            def _():
                o_copy(j, b).start()

    def l_copy(stage, k):
        if stage == 0:
            return remote(lbuf.at[0, x], lbuf.at[0, x], lsend.at[0, k], lrecv.at[0, x], at.dev(x=(x + k) % nx))
        if stage == 1:
            return remote(lbuf.at[1, y], lbuf.at[1, y], lsend.at[1, k], lrecv.at[1, y], at.dev(y=(y + k) % ny))
        return remote(lbuf.at[2, c], lbuf.at[2, c], lsend.at[2, 0], lrecv.at[2, c], at.dev(c=at.pc))

    def l_sum(stage, size, me):
        for k in range(size):
            @pl.when(k != me)
            def _():
                remote(
                    lbuf.at[stage, k], lbuf.at[stage, k], lsend.at[stage, 0], lrecv.at[stage, k], at.dev(c=at.pc)
                ).wait_recv()

        total = lbuf[stage, 0]
        for k in range(1, size):
            total = total + lbuf[stage, k]
        return total

    def l_start():
        lbuf[0, x] = -lacc[...]
        for k in range(1, nx):
            l_copy(0, k).start()

    def l_mid():
        lbuf[1, y] = l_sum(0, nx, x)
        for k in range(1, ny):
            l_copy(1, k).start()

    def l_late():
        lbuf[2, c] = l_sum(1, ny, y)
        l_copy(2, 0).start()

    lane = lax.broadcasted_iota(jnp.int32, (min(64, tr), LANES), 1).astype(F32)

    def each_tile(n, u, buf, c0, c1, fn):
        j, r, d = tile(n, u)
        blk = min(64, tr)
        for o in range(0, tr, blk):
            rows = slice(o, o + blk)
            t = st[r * nx + d, rows, :]
            shift = jnp.broadcast_to(t[:, 0:1], (blk, LANES))
            lab = jnp.broadcast_to(t[:, 1:TWO], (blk, LANES)) - (j * ch).astype(F32)
            for e in range(c0 // LANES, c1 // LANES):
                cols = slice(LANES * e, LANES * e + LANES)
                fn(rows, cols, zb[buf, rows, cols] - shift, lane + float(LANES * e) == lab)

    def make_g(n, u, buf, c0, c1, loss_sum=None):
        def one(rows, cols, dist, hit):
            g = jnp.exp(dist)
            gb[u, rows, cols] = jnp.where(hit, g - inv, g).astype(BF16)
            if loss_sum is not None:
                loss_sum.append(jnp.where(hit, dist, 0.0) + (loss_sum.pop() if loss_sum else 0.0))

        each_tile(n, u, buf, c0, c1, one)

    big = ch % (10 * LANES) == 0
    x_cuts = [(ch * e // 5, ch * (e + 1) // 5) for e in range(5)] if big else [(0, ch)]
    w_cuts = [(0, ch // 5), (ch // 5, ch * 3 // 5), (ch * 3 // 5, ch)] if big else [(0, ch)]

    def x_body(n, base):
        _, s, j = body_at(n)
        half = s % TWO

        @pl.when(j == 0)
        def _():
            dx[half] = jnp.zeros(dx.shape[1:], F32)

        for u in BOTH:
            for c0, c1 in x_cuts:
                loss_sum = []
                make_g(n, u, base + u, c0, c1, loss_sum)
                lacc[...] += jnp.sum(loss_sum[0].reshape(-1, SUB, LANES), axis=0)
                dx[half, u] += lax.dot_general(
                    gb[u, :, c0:c1], w[j, c0:c1, :], (((1,), (0,)), ((), ())), preferred_element_type=F32
                )

    def w_body(n, base):
        _, j, k = body_at(n)
        half = j % TWO

        @pl.when(k == 0)
        def _():
            acc[half] = jnp.zeros(acc.shape[1:], F32)

        for c0, c1 in w_cuts:
            for u in BOTH:
                make_g(n, u, base + u, c0, c1)
            acc[half, :, c0:c1] += jnp.dot(
                xt[k], gb[:, :, c0:c1].reshape(TWO * tr, c1 - c0), preferred_element_type=F32
            )

    plan_a = [(after["x1"] + q, 1, q) for q in range(nq)] + [(after["x2"] + q, 2, q) for q in range(nq)]
    plan_a += [(after["x3"] + 3 * q, 3, q) for q in range(nq)]
    plan_r = [(11, 12, 0), (15, 16, 1), (24, 25, 2), (28, 29, 3), (42, 43, 4)]
    plan_s = [(17, 18, 0), (21, 22, 1), (30, 31, 2), (34, 35, 3), (46, 47, 4)]
    pre_r, use_r = [(p, j) for p, _, j in plan_r], [(u, j) for _, u, j in plan_r]
    pre_s, use_s = [(p, j) for p, _, j in plan_s], [(u, j) for _, u, j in plan_s]
    plan_f = [(41, 0), (44, 1), (46, 2), (48, 3)]
    n_all = n_body + TWO * nq + 1

    def when(n, table, fn):
        table = [(e[0], e[1:]) for e in table]
        hit = functools.reduce(lambda p, q: p | q, [n == e for e, _ in table])

        @pl.when(hit)
        def _():
            args = []
            for i in range(len(table[0][1])):
                val = 0
                for e, vals in table:
                    if vals[i]:
                        val = val + jnp.where(n == e, vals[i], 0)
                args.append(val + jnp.int32(0))
            fn(*args)

    def body(n, _):
        @pl.when(n < NCH)
        def _():
            local(w_hbm.at[n], w.at[n], wsem.at[n]).wait()

        @pl.when(n == first["w0"])
        def _():
            local(xt_hbm, xt, tsem).wait()
            for q in range(nq):
                for dr in BOTH:
                    x_copy(0, dr, q).start()

        when(n, [(after["w%d" % j], j) for j in range(NCH)], d_send)
        when(n, plan_a, a_use)
        when(n, plan_f, f_use)
        when(n, use_r, r_use)
        when(n, use_s, s_use)
        when(n, [(e[0] - 1,) + e[1:] for e in plan_a], a_pre)
        when(n, [(e[0] - 1,) + e[1:] for e in plan_f], f_pre)
        when(n, pre_r, r_pre)
        when(n, pre_s, s_pre)

        for at_n, fn in ((n_body, l_start), (n_body + TWO, l_mid), (n_body + nq, l_late)):
            pl.when(n == at_n)(fn)

        @pl.when((n == first["x2"]) | (n == first["x3"]))
        def _():
            s = jnp.where(n == first["x2"], 0, 1)
            for q in range(nq):
                for dr in BOTH:
                    x_copy(s, dr, q).wait_send()

        for j in range(2, NCH):
            @pl.when(n == first["w%d" % j])
            def _():
                for b in BOTH:
                    r_copy(j - 2, b).wait_send()
                    for i in BOTH:
                        d_copy(j - 2, b, i).wait_send()

        base = (n % TWO) * 2

        @pl.when(n < n_body)
        def _():
            for u in BOTH:
                zcp(n, u, base + u).wait()

            @pl.when(n + 1 < n_body)
            def _():
                for u in BOTH:
                    zcp(n + 1, u, 2 - base + u).start()

            kind = body_at(n)[0]

            @pl.when(kind == 0)
            def _():
                x_body(n, base)

            @pl.when(kind == 1)
            def _():
                w_body(n, base)

        return 0

    lax.fori_loop(0, n_all, body, 0)
    loss[...] = l_sum(2, TWO, c)

    for q in range(nq):
        if q >= nq - 2:
            f_out(q).wait()
        far_copy(q).wait_send()
        for dr in BOTH:
            x_copy(2, dr, q).wait_send()
    for b in BOTH:
        for j in range(NCH - 2, NCH):
            for i in BOTH:
                d_copy(j, b, i).wait_send()
            r_copy(j, b).wait_send()

        @pl.when(is_here(b))
        def _():
            o_here(NCH - 1, b).wait()

        @pl.when(jnp.logical_not(is_here(b)))
        def _():
            o_copy(NCH - 1, b).wait_send()

    q0 = half_of(y, c, ny)
    for f in BOTH:
        kept = (f == q0) & ((q0 + c) % TWO == c)

        @pl.when(jnp.logical_not(kept))
        def _():
            for j in range(NCH):
                dst = dwo.at[pl.ds(f * slot + j * sb, sb)]
                remote(fin.at[0], dst, osend.at[j, 0], orecv.at[f, j], at.dev(c=at.pc)).wait_recv()

    for k in range(1, nx):
        l_copy(0, k).wait_send()
    for k in range(1, ny):
        l_copy(1, k).wait_send()
    l_copy(2, 0).wait_send()


def grads(nx, ny, inv, vocab, z, w, xt, sta, laba, hk):
    ch, h = w.shape[1:]
    tr = z.shape[3]
    nq = 4
    shape = jax.ShapeDtypeStruct
    dma = pltpu.SemaphoreType.DMA
    vm = pltpu.VMEM
    vspec = pl.BlockSpec(memory_space=pltpu.VMEM)
    sb, qr = ch // TWO, tr // nq
    return pl.pallas_call(
        functools.partial(grads_kernel, nx, ny, inv, vocab),
        out_shape=(
            shape((tr, h), BF16), shape((NCH * ch, hk), BF16), shape((SUB, LANES), F32),
            shape((nx - 1, TWO, nq, qr, h), F32), shape((nq, qr, h), F32),
            shape((NCH, TWO, TWO, hk, sb), F32), shape((NCH, TWO, hk, sb), F32),
        ),
        in_specs=[ANY] * 5,
        out_specs=(ANY, ANY, vspec, ANY, ANY, ANY, ANY),
        scratch_shapes=[
            vm((NCH, ch, h), BF16), vm((nx, h, TWO * tr), BF16), vm((4, tr, ch), F32), vm((TWO, tr, ch), BF16),
            vm((TWO, h, ch), F32), vm((TWO, TWO, tr, h), F32), vm((TWO * nx, tr, LANES), F32), vm(sta.shape, F32), vm(laba.shape, jnp.int32), vm((SUB, LANES), F32),
            vm((TWO, TWO, qr, h), F32), vm((TWO, TWO, hk, sb), F32), vm((TWO, TWO, hk, sb), F32),
            vm((TWO, sb, hk), BF16), vm((TWO, qr, h), BF16), vm((3, max(nx, ny), SUB, LANES), F32),
            dma((NCH,)), dma, dma((4,)), dma((nx - 1, TWO, nq)), dma((nx - 1, TWO, nq)), dma((nq,)), dma((nq,)),
            dma((NCH, TWO, TWO)), dma((NCH, TWO, TWO)), dma((NCH, TWO)), dma((NCH, TWO)), dma((NCH, TWO)), dma((TWO, NCH)),
            dma((TWO, TWO)), dma((TWO, TWO)), dma((3, max(nx, ny))), dma((3, max(nx, ny))), dma((nq,)), dma((TWO,)),
        ],
        compiler_params=pltpu.CompilerParams(
            collective_id=1, has_side_effects=True, vmem_limit_bytes=67_000_000,
        ),
        name="grads",
    )(z, w, xt, sta, laba)


def solution(mesh):
    ny = mesh.shape["fsdp"]
    tp_size = mesh.shape["tp"]
    nx = tp_size // TWO
    token_spec = P(("dp", "fsdp", "tp"), None)
    label_spec = P(("dp", "fsdp", "tp"))

    def local_step(hidden, w_head, labels):
        tr, h = hidden.shape
        hk, vocab = w_head.shape
        inv = 1.0 / (tr * tp_size * ny)
        lab = labels.reshape(-1, LANES)
        xg, wg, z, sta, laba, xt = gather_logits(nx, ny, vocab, hidden, w_head.T, lab)
        d_hidden, d_w, loss = grads(nx, ny, inv, vocab, z, wg, xt, sta, laba, hk)[:3]
        mean_loss = jnp.sum(loss) * inv + math.log(inv)
        return mean_loss.reshape(1), d_hidden, d_w[:vocab].T

    return jax.shard_map(
        local_step,
        mesh=mesh,
        in_specs=(token_spec, P("fsdp", "tp"), label_spec),
        out_specs=(P("dp"), token_spec, P(("dp", "fsdp"), "tp")),
        check_vma=False,
    )
```
